32 devices in a mesh: blk: 16 (over z, y, core), head: 2 (over x).
Axes of the slice: x: 2, y: 2, z: 4, core: 2. Of those that a mesh axis runs over, the one named last changes fastest.
Arguments:
- tokens: bfloat16 [2048, 3584], P(('blk', 'head')), may hold values from -100 to 100
- norm_gain: float32 [3584], replicated, may hold values from 0.1 to 1.9
- w_query: bfloat16 [3584, 3072], P('blk', 'head'), may hold values from -0.09375 to 0.09375
- w_key: bfloat16 [3584, 512], P('blk'), may hold values from -0.09375 to 0.09375
- w_value: bfloat16 [3584, 512], P('blk'), may hold values from -0.09375 to 0.09375
- q_bias: float32 [3072], P('head'), may hold values from -200 to 200
- k_bias: float32 [512], replicated, may hold values from -25 to 25
- v_bias: float32 [512], replicated, may hold values from -2.5 to 2.5
- w_out: bfloat16 [3072, 3584], P('head', 'blk'), may hold values from -0.109375 to 0.109375
Outputs:
- attention_out: bfloat16 [2048, 3584], P(('blk', 'head'))
The draws below stay inside these ranges and needn't reach their ends.
All inputs are finite; a program needn't handle non-finite values.
Results may differ from the reference program's by a relative error of at most 0.04.
The reference program's roundings to bfloat16 on the way count: a program that leaves them out, or rounds other values in their place, can miss the bound.
Values may be sent and summed in bfloat16 or wider, within the bound.
A program may use at most 64 MiB of HBM per device.

```python
import jax
import jax.numpy as jnp
from jax import lax

D = 3584
HD = 128
H = 24
G = 6
KVH = 4
SEQ = 2048


def draw_tokens(key, part):
    first, second, third = jax.random.split(jax.random.fold_in(key, 5), 3)
    row_scale = jnp.exp(jax.random.uniform(second, (SEQ, 1), minval=0.0, maxval=jnp.log(10.0)))
    col_scale = jnp.exp(jax.random.uniform(third, (1, D), minval=jnp.log(0.3), maxval=jnp.log(3.0)))
    base = jax.random.normal(first, (SEQ, D))
    return jnp.clip(base * row_scale * col_scale, -100.0, 100.0).astype(jnp.bfloat16)


def draw_q_bias(key, part):
    values = 0.5 * jax.random.normal(jax.random.fold_in(key, 3), (H * HD,))
    return jnp.clip(values, -2.0, 2.0).astype(jnp.float32)


def draw_k_bias(key, part):
    values = 0.5 * jax.random.normal(jax.random.fold_in(key, 4), (KVH * HD,))
    return jnp.clip(values, -2.0, 2.0).astype(jnp.float32)


def shard_levels(key, extent, cuts, least, largest):
    def one(axis_at, shards_of):
        steps = jax.random.uniform(jax.random.fold_in(jax.random.fold_in(key, 6), axis_at), (shards_of,), jnp.float32, least / len(cuts), largest / len(cuts))
        return jnp.repeat(jnp.exp(steps), extent[axis_at] // shards_of).reshape((-1,) + (1,) * (len(extent) - axis_at - 1))

    gain = one(*cuts[0])
    for cut in cuts[1:]:
        gain = gain * one(*cut)
    return gain


def normal_values(key, dims, scale, limit, cuts=(), kind=jnp.bfloat16):
    level = shard_levels(key, dims, cuts, -0.22, 0.18) if cuts else 1.0
    values = jax.random.normal(key, dims, jnp.float32) * scale * level
    return jnp.minimum(jnp.maximum(values, -limit), limit).astype(kind)


def setup_inputs(seed: int = 0) -> dict:
    key_list = jax.random.split(jax.random.key(seed), 10)
    tokens = draw_tokens(jax.random.fold_in(key_list[9], 71), 0)
    norm_gain = jnp.clip(1.0 + 0.18 * jax.random.normal(key_list[1], (D,), jnp.float32), 0.1, 1.9)
    w_query = normal_values(key_list[2], (D, H * HD), D ** -0.5, 0.09375, ((0, 16), (1, 2)))
    w_key = normal_values(key_list[3], (D, KVH * HD), D ** -0.5, 0.09375, ((0, 16),))
    w_value = normal_values(key_list[4], (D, KVH * HD), D ** -0.5, 0.09375, ((0, 16),))
    q_bias = draw_q_bias(jax.random.fold_in(key_list[9], 71), 0)
    k_bias = draw_k_bias(jax.random.fold_in(key_list[9], 71), 0)
    v_bias = normal_values(key_list[7], (KVH * HD,), 0.5, 2.5, (), jnp.float32)
    w_out = normal_values(key_list[8], (H * HD, D), (H * HD) ** -0.5, 0.109375, ((0, 2), (1, 16)))
    return {"tokens": tokens, "norm_gain": norm_gain, "w_query": w_query, "w_key": w_key, "w_value": w_value, "q_bias": q_bias, "k_bias": k_bias, "v_bias": v_bias, "w_out": w_out}


theta_base = 1000000.0
eps_norm = 1e-06
masked_score = -1e+30

def rotary_tables(positions, width):
    half = width // 2
    freq = theta_base ** (-(jnp.arange(half, dtype=jnp.float32) * 2.0 / width))
    angles = positions.astype(jnp.float32)[:, None] * freq[None, :]
    angles = jnp.concatenate([angles, angles], axis=1)
    return (jnp.cos(angles), jnp.sin(angles))

def rotate(values, cosine, sine):
    half = values.shape[-1] // 2
    turned = jnp.concatenate([-values[..., half:], values[..., :half]], axis=-1)
    return values * cosine[:, None, :] + turned * sine[:, None, :]

def reference(tokens, norm_gain, w_query, w_key, w_value, q_bias, k_bias, v_bias, w_out):
    seq_len = tokens.shape[0]
    floats = tokens.astype(jnp.float32)
    normed = (floats * lax.rsqrt(lax.optimization_barrier(jnp.mean(floats * floats, axis=1, keepdims=True)) + eps_norm) * norm_gain).astype(jnp.bfloat16)
    cosine, sine = rotary_tables(jnp.arange(seq_len, dtype=jnp.int32), HD)
    query = jnp.dot(normed, w_query, preferred_element_type=jnp.float32) + q_bias
    query = rotate(query.reshape(seq_len, H, HD), cosine, sine).astype(jnp.bfloat16)
    key = jnp.dot(normed, w_key, preferred_element_type=jnp.float32) + k_bias
    key = rotate(key.reshape(seq_len, KVH, HD), cosine, sine).astype(jnp.bfloat16)
    value = (jnp.dot(normed, w_value, preferred_element_type=jnp.float32) + v_bias).astype(jnp.bfloat16)
    value = value.reshape(seq_len, KVH, HD)
    width = min(512, seq_len)
    block_total = seq_len // width
    scale = 1.0 / HD ** 0.5
    key_positions = jnp.arange(seq_len, dtype=jnp.int32)

    def one_group(group):
        query_group = lax.dynamic_slice_in_dim(query, (group * G).astype(jnp.int32), G, 1)
        key_group = lax.dynamic_index_in_dim(key, group, 1, keepdims=False).astype(jnp.float32)
        value_group = lax.dynamic_index_in_dim(value, group, 1, keepdims=False).astype(jnp.float32)

        def one_block(block):
            start = (block * width).astype(jnp.int32)
            rows_block = lax.dynamic_slice_in_dim(query_group, start, width, 0).astype(jnp.float32)
            scores = jnp.einsum('qhd,kd->hqk', rows_block, key_group) * scale
            query_positions = start + jnp.arange(width, dtype=jnp.int32)
            visible = key_positions[None, :] <= query_positions[:, None]
            scores = jnp.where(visible[None], scores, masked_score)
            top = lax.optimization_barrier(jnp.max(scores, axis=2, keepdims=True))
            weights = jnp.where(visible[None], jnp.exp(scores - top), 0.0)
            total = lax.optimization_barrier(jnp.sum(weights, axis=2))
            rounded = lax.optimization_barrier(weights.astype(jnp.bfloat16))
            mixed = jnp.einsum('hqk,kd->hqd', rounded.astype(jnp.float32), value_group)
            return (mixed / total[..., None]).astype(jnp.bfloat16)
        return lax.map(one_block, jnp.arange(block_total, dtype=jnp.int32))
    outs = lax.map(one_group, jnp.arange(KVH, dtype=jnp.int32))
    attended = outs.transpose(1, 3, 0, 2, 4).reshape(seq_len, H * HD)
    return jnp.dot(attended, w_out, preferred_element_type=jnp.float32).astype(jnp.bfloat16)
```

```python
import functools
import math

import jax
import jax.numpy as jnp
from jax import lax
from jax.experimental import pallas as pl
from jax.experimental.pallas import tpu as pltpu
from jax.sharding import PartitionSpec as P

HD = 128
G = 6
MESH = pl.DeviceIdType.MESH

theta_base = 1000000.0
eps_norm = 1e-06
masked_score = -1e30

WQ, WKV, WO, KV, WQ_TAIL, WO_TAIL = range(6)
UP, DOWN, ACROSS, CORE = range(4)


def block_width(rows, limit):
    width = min(rows, limit)
    while rows % width:
        width -= 1
    return width


def kernel(
    sizes,
    tokens_ref,
    gain_ref,
    w_query_ref,
    w_key_ref,
    w_value_ref,
    q_bias_ref,
    k_bias_ref,
    v_bias_ref,
    w_out_ref,
    cos_ref,
    sin_ref,
    out_ref,
    wq,
    wkv,
    wo,
    kv,
    normed,
    query,
    attended,
    partial,
    outgoing,
    incoming,
    local_sem,
    send_sem,
    recv_sem,
    norm_send,
    norm_recv,
    sum_send,
    sum_recv,
):
    blocks, heads = sizes
    nz = blocks // 4
    me = lax.axis_index("blk")
    head = lax.axis_index("head")
    z, y, c = me // 4, (me // 2) % 2, me % 2
    local_rows, width = tokens_ref.shape
    group_rows = local_rows * heads
    heads_here = wq.shape[1] // HD
    kv_here = wkv.shape[1] // (2 * HD)
    per_kv = heads_here // kv_here
    kv_cols = kv_here * HD
    kv_start = pl.multiple_of((head * heads_here // G) * HD, HD)
    buffers = {WQ: wq, WKV: wkv, WO: wo, KV: kv, WQ_TAIL: wq, WO_TAIL: wo}
    queries, outs = (WQ, WQ_TAIL), (WO, WO_TAIL)
    scale = 1.0 / math.sqrt(HD)

    def slot_of(zz, yy, cc):
        return (zz * 2 + yy) * 2 + cc

    def rows_of(item, slot):
        each = buffers[item].shape[0] // blocks
        first, size = 0, each
        if item in queries + outs:
            cut = each // 2 // 16 * 16
            first, size = (0, cut) if item in (WQ, WO) else (cut, each - cut)
        return buffers[item].at[pl.ds(pl.multiple_of(slot * each + first, 16), size)]

    def whole_rows(ref):
        each = ref.shape[0] // blocks
        return ref.at[pl.ds(pl.multiple_of(me * each, each), each)]

    def target(route):
        step = {UP: 4, DOWN: -4, ACROSS: 2 - 4 * y, CORE: 1 - 2 * c}[route]
        return (me + step, head)

    def copy(item, slot, route):
        part = rows_of(item, slot)
        return pltpu.make_async_remote_copy(
            src_ref=part,
            dst_ref=part,
            send_sem=send_sem.at[item, slot, route],
            recv_sem=recv_sem.at[item, slot],
            device_id=target(route),
            device_id_type=MESH,
        )

    def send(item, slot, route):
        if route == UP:
            pl.when(z < nz - 1)(lambda: copy(item, slot, route).start())
        elif route == DOWN:
            pl.when(z > 0)(lambda: copy(item, slot, route).start())
        else:
            copy(item, slot, route).start()

    def sent(item, slot, route):
        if route == UP:
            pl.when(z < nz - 1)(lambda: copy(item, slot, route).wait_send())
        elif route == DOWN:
            pl.when(z > 0)(lambda: copy(item, slot, route).wait_send())
        else:
            copy(item, slot, route).wait_send()

    def arrived(item, slot):
        copy(item, slot, CORE).wait_recv()

    def below(k, act):
        pl.when(z >= k)(lambda: act(z - k))

    def above(k, act):
        pl.when(z + k < nz)(lambda: act(z + k))

    def z_step(item, k, yy, then=()):
        def from_below(zz):
            slot = slot_of(zz, yy, c)
            arrived(item, slot)
            for route in (UP,) + then:
                send(item, slot, route)

        def from_above(zz):
            slot = slot_of(zz, yy, c)
            arrived(item, slot)
            for route in (DOWN,) + then:
                send(item, slot, route)

        below(k, from_below)
        above(k, from_above)

    def at_distance(k, act):
        if k == 0:
            act(z)
        else:
            below(k, act)
            above(k, act)

    def across(item, k):
        def act(zz):
            slot = slot_of(zz, 1 - y, c)
            arrived(item, slot)
            send(item, slot, CORE)

        at_distance(k, act)

    def finish(item):
        for zz in range(nz):
            for yy in range(2):
                arrived(item, slot_of(zz, yy, 1 - c))

    def drain(item, both):
        for yy in (y, 1 - y) if both else (y,):
            for route in (UP, DOWN):
                sent(item, slot_of(z, yy, c), route)
            for k in range(1, nz):
                below(k, lambda zz, yy=yy: sent(item, slot_of(zz, yy, c), UP))
                above(k, lambda zz, yy=yy: sent(item, slot_of(zz, yy, c), DOWN))
        if both:
            sent(item, me, ACROSS)
        for zz in range(nz):
            if not both:
                sent(item, slot_of(zz, y, c), ACROSS)
            for yy in range(2):
                sent(item, slot_of(zz, yy, c), CORE)

    own = [
        pltpu.make_async_copy(w_query_ref, whole_rows(wq), local_sem.at[0]),
        pltpu.make_async_copy(
            w_key_ref.at[:, pl.ds(kv_start, kv_cols)],
            rows_of(WKV, me).at[:, pl.ds(0, kv_cols)],
            local_sem.at[1],
        ),
        pltpu.make_async_copy(
            w_value_ref.at[:, pl.ds(kv_start, kv_cols)],
            rows_of(WKV, me).at[:, pl.ds(kv_cols, kv_cols)],
            local_sem.at[2],
        ),
        pltpu.make_async_copy(w_out_ref, whole_rows(wo), local_sem.at[3]),
    ]
    for one in own:
        one.start()

    barrier = pltpu.get_barrier_semaphore()

    def greet(blk, hd):
        pl.semaphore_signal(barrier, inc=1, device_id=(blk, hd), device_id_type=MESH)

    pl.when(z < nz - 1)(lambda: greet(me + 4, head))
    pl.when(z > 0)(lambda: greet(me - 4, head))
    greet(target(ACROSS)[0], head)
    greet(target(CORE)[0], head)
    peers = [lax.rem(head + d, heads) for d in range(1, heads)]
    for peer in peers:
        greet(me, peer)
    ends = jnp.where(z < nz - 1, 1, 0) + jnp.where(z > 0, 1, 0)
    pl.semaphore_wait(barrier, ends + 2 + len(peers))

    own[1].wait()
    own[2].wait()
    for route in (ACROSS, UP, DOWN, CORE):
        send(WKV, me, route)
    own[0].wait()
    own[3].wait()
    for item in queries + outs:
        for route in (ACROSS, CORE):
            send(item, me, route)

    my_rows = pl.ds(pl.multiple_of(head * local_rows, local_rows), local_rows)
    floats = tokens_ref[...].astype(jnp.float32)
    normed[my_rows, :] = (
        floats
        * lax.rsqrt(jnp.mean(floats * floats, axis=1, keepdims=True) + eps_norm)
        * gain_ref[...]
    ).astype(jnp.bfloat16)

    there = slot_of(z, 1 - y, c)
    arrived(WKV, there)
    for route in (UP, DOWN, CORE):
        send(WKV, there, route)

    def norm_copy(d):
        return pltpu.make_async_remote_copy(
            src_ref=normed.at[my_rows],
            dst_ref=normed.at[my_rows],
            send_sem=norm_send.at[d],
            recv_sem=norm_recv.at[d],
            device_id=(me, peers[d]),
            device_id_type=MESH,
        )

    for d in range(len(peers)):
        norm_copy(d).start()

    for k in range(1, nz):
        z_step(WKV, k, y, (CORE,))
        z_step(WKV, k, 1 - y, (CORE,))
        if k == max(1, nz - 2):
            for item in queries:
                for route in (UP, DOWN):
                    send(item, me, route)
    for d in range(len(peers)):
        norm_copy(d).wait_recv()
    finish(WKV)

    cosine, sine = cos_ref[...], sin_ref[...]

    def turn(values):
        return values * cosine + pltpu.roll(values, HD // 2, 1) * sine

    kv_rows = pl.ds(pl.multiple_of(me * group_rows, group_rows), group_rows)
    sums = jnp.dot(normed[...], wkv[...], preferred_element_type=jnp.float32)
    for g in range(kv_here):
        bias = k_bias_ref[:, pl.ds(pl.multiple_of(kv_start + g * HD, HD), HD)]
        kv[kv_rows, pl.ds(g * HD, HD)] = turn(sums[:, g * HD : (g + 1) * HD] + bias).astype(
            jnp.bfloat16
        )
        bias = v_bias_ref[:, pl.ds(pl.multiple_of(kv_start + g * HD, HD), HD)]
        at = kv_cols + g * HD
        kv[kv_rows, pl.ds(at, HD)] = (sums[:, at : at + HD] + bias).astype(jnp.bfloat16)

    for item in queries:
        across(item, 0)
    for route in (UP, DOWN, ACROSS, CORE):
        send(KV, me, route)

    for k in range(1, nz):
        for item in queries:
            z_step(item, k, y, (ACROSS, CORE))
        z_step(KV, k, y, (ACROSS, CORE))
        if k == max(1, nz - 2):
            for item in outs:
                for route in (UP, DOWN):
                    send(item, me, route)
    for k in range(1, nz):
        if k == nz - 1:
            for item in outs:
                z_step(item, 1, y, (ACROSS, CORE))
        for item in queries:
            across(item, k)
    for k in range(nz):
        across(KV, k)
    for item in queries + (KV,):
        finish(item)

    joined = 2 if heads_here % 2 == 0 else 1

    def project(n, carry):
        cols = pl.ds(pl.multiple_of(n * joined * HD, joined * HD), joined * HD)
        total = jnp.dot(normed[...], wq[:, cols], preferred_element_type=jnp.float32)
        total = total + q_bias_ref[:, cols]
        for j in range(joined):
            query[n * joined + j] = turn(total[:, j * HD : (j + 1) * HD]).astype(jnp.bfloat16)
        return carry

    lax.fori_loop(0, heads_here // joined, project, 0)

    if nz > 2:
        for item in outs:
            z_step(item, 2, y, (ACROSS, CORE))

    keys = kv.shape[0]
    span = block_width(keys, 512)
    stacked = per_kv * group_rows
    last_query = me * group_rows + group_rows - 1
    steps = last_query // span + 1

    for g in range(kv_here):
        q = query[g * per_kv : (g + 1) * per_kv].reshape(stacked, HD)

        def attend(j, state, q=q, g=g):
            top, total, acc = state
            at = pl.ds(pl.multiple_of(j * span, span), span)
            scores = (
                lax.dot_general(
                    q,
                    kv[at, pl.ds(g * HD, HD)],
                    (((1,), (1,)), ((), ())),
                    preferred_element_type=jnp.float32,
                )
                * scale
            )
            shape = (per_kv, group_rows, span)
            rows = lax.broadcasted_iota(jnp.int32, shape, 1).reshape(stacked, span)
            columns = lax.broadcasted_iota(jnp.int32, (stacked, span), 1)
            visible = columns + j * span <= rows + me * group_rows
            scores = jnp.where(visible, scores, masked_score)
            new_top = jnp.maximum(top, jnp.max(scores, axis=1, keepdims=True))
            weights = jnp.where(visible, jnp.exp(scores - new_top), 0.0)
            fade = jnp.exp(top - new_top)
            total = total * fade + jnp.sum(weights, axis=1, keepdims=True)
            acc = acc * fade + jnp.dot(
                weights.astype(jnp.bfloat16),
                kv[at, pl.ds(kv_cols + g * HD, HD)],
                preferred_element_type=jnp.float32,
            )
            return (new_top, total, acc)

        start = (
            jnp.full((stacked, 1), masked_score, jnp.float32),
            jnp.zeros((stacked, 1), jnp.float32),
            jnp.zeros((stacked, HD), jnp.float32),
        )
        top, total, acc = lax.fori_loop(0, steps, attend, start)
        result = (acc / total).astype(jnp.bfloat16)
        for r in range(per_kv):
            attended[:, pl.ds((g * per_kv + r) * HD, HD)] = result[
                r * group_rows : (r + 1) * group_rows
            ]
        for k in range(3, nz):
            if g == 0:
                z_step(WO, k, y, (ACROSS, CORE))
    for k in range(3, nz):
        z_step(WO_TAIL, k, y, (ACROSS, CORE))

    each = wo.shape[0] // blocks
    grouped = (4 * each) % HD == 0
    groups = nz if grouped else 1
    chunk = width // groups

    def sum_copy(d, i, start):
        rows = pl.ds(pl.multiple_of(peers[d] * local_rows, local_rows), local_rows)
        cols = pl.ds(pl.multiple_of(start, HD), chunk)
        return pltpu.make_async_remote_copy(
            src_ref=outgoing.at[rows, cols],
            dst_ref=incoming.at[d, :, cols],
            send_sem=sum_send.at[d, i],
            recv_sem=sum_recv.at[d, i],
            device_id=(me, peers[d]),
            device_id_type=MESH,
        )

    def produce(start, size):
        cols = pl.ds(pl.multiple_of(start, HD), size)
        result = lax.dot_general(
            attended[...],
            wo[cols, :],
            (((1,), (1,)), ((), ())),
            preferred_element_type=jnp.float32,
        )
        partial[:, cols] = result
        outgoing[:, cols] = result.astype(jnp.bfloat16)

    def place(i):
        way = 1 - 2 * (z // max(1, nz // 2)) if nz > 1 else 1
        return lax.rem(z + way * i + nz, nz)

    if grouped:

        def produce_group(i, carry):
            zz = place(i)
            slot = slot_of(zz, 1 - y, c)
            for item in outs:
                arrived(item, slot)
                send(item, slot, CORE)
            for item in outs:
                for yy in range(2):
                    arrived(item, slot_of(zz, yy, 1 - c))
            produce(zz * 4 * each, chunk)
            for d in range(len(peers)):
                sum_copy(d, i, zz * chunk).start()
            return carry

        lax.fori_loop(0, nz, produce_group, 0)
    else:
        for item in outs:
            for k in range(nz):
                across(item, k)
            finish(item)
        part = 256
        lax.fori_loop(0, width // part, lambda n, carry: (produce(n * part, part), carry)[1], 0)
        for d in range(len(peers)):
            sum_copy(d, 0, 0).start()

    for item in queries + outs + (WKV, KV):
        drain(item, item == WKV)
    for d in range(len(peers)):
        norm_copy(d).wait_send()

    def collect(i, carry):
        start = place(i) * chunk if grouped else 0
        cols = pl.ds(pl.multiple_of(start, HD), chunk)
        for d in range(len(peers)):
            sum_copy(d, i, start).wait_recv()
        result = partial[my_rows, cols]
        for d in range(len(peers)):
            result = result + incoming[d, :, cols].astype(jnp.float32)
        out_ref[:, cols] = result.astype(jnp.bfloat16)
        for d in range(len(peers)):
            sum_copy(d, i, start).wait_send()
        return carry

    lax.fori_loop(0, groups, collect, 0)


def on_device(tokens, norm_gain, w_query, w_key, w_value, q_bias, k_bias, v_bias, w_out):
    blocks, heads = lax.axis_size("blk"), lax.axis_size("head")
    local_rows, width = tokens.shape
    group_rows = local_rows * heads
    heads_here = w_query.shape[1] // HD
    kv_here = max(1, heads_here // G)
    positions = lax.axis_index("blk") * group_rows + jnp.arange(group_rows, dtype=jnp.int32)
    half = HD // 2
    freq = theta_base ** (-(jnp.arange(half, dtype=jnp.float32) * 2.0 / HD))
    angles = positions.astype(jnp.float32)[:, None] * freq[None, :]
    cosine, sine = jnp.cos(angles), jnp.sin(angles)
    cosine = jnp.concatenate([cosine, cosine], axis=1)
    sine = jnp.concatenate([-sine, sine], axis=1)
    inner = heads_here * HD
    vmem = pl.BlockSpec(memory_space=pltpu.VMEM)
    hbm = pl.BlockSpec(memory_space=pl.ANY)
    others = max(1, heads - 1)
    bf16, f32 = jnp.bfloat16, jnp.float32
    return pl.pallas_call(
        functools.partial(kernel, (blocks, heads)),
        out_shape=jax.ShapeDtypeStruct((local_rows, width), bf16),
        in_specs=[vmem, vmem, hbm, hbm, hbm, vmem, vmem, vmem, hbm, vmem, vmem],
        out_specs=vmem,
        scratch_shapes=[
            pltpu.VMEM((width, inner), bf16),
            pltpu.VMEM((width, 2 * kv_here * HD), bf16),
            pltpu.VMEM((width, inner), bf16),
            pltpu.VMEM((blocks * group_rows, 2 * kv_here * HD), bf16),
            pltpu.VMEM((group_rows, width), bf16),
            pltpu.VMEM((heads_here, group_rows, HD), bf16),
            pltpu.VMEM((group_rows, inner), bf16),
            pltpu.VMEM((group_rows, width), f32),
            pltpu.VMEM((group_rows, width), bf16),
            pltpu.VMEM((others, local_rows, width), bf16),
            pltpu.SemaphoreType.DMA((4,)),
            pltpu.SemaphoreType.DMA((6, blocks, 4)),
            pltpu.SemaphoreType.DMA((6, blocks)),
            pltpu.SemaphoreType.DMA((others,)),
            pltpu.SemaphoreType.DMA((others,)),
            pltpu.SemaphoreType.DMA((others, blocks // 4)),
            pltpu.SemaphoreType.DMA((others, blocks // 4)),
        ],
        compiler_params=pltpu.CompilerParams(
            collective_id=0, has_side_effects=True, vmem_limit_bytes=60 * 1024 * 1024
        ),
    )(
        tokens,
        norm_gain[None, :],
        w_query,
        w_key,
        w_value,
        q_bias[None, :],
        k_bias[None, :],
        v_bias[None, :],
        w_out.T,
        cosine,
        sine,
    )


def plane_kernel(
    nz,
    tokens_ref,
    gain_ref,
    w_query_ref,
    w_key_ref,
    w_value_ref,
    q_bias_ref,
    k_bias_ref,
    v_bias_ref,
    w_out_ref,
    cos_ref,
    sin_ref,
    out_ref,
    stage,
    w,
    normed,
    xs,
    part_out,
    part_in,
    own,
    biases,
    kv,
    hidden,
    att,
    att_other,
    wo,
    acc,
    outs,
    result,
    load_sem,
    wo_load_sem,
    first_send,
    w_send,
    w_recv,
    x_send,
    x_recv,
    b_send,
    b_recv,
    p_send,
    p_recv,
    kv_send,
    kv_recv,
    a_send,
    a_recv,
    wo_send,
    wo_recv,
    o_send,
    o_recv,
):
    f32, bf16 = jnp.float32, jnp.bfloat16
    me = lax.axis_index("blk")
    x = lax.axis_index("head")
    z, y, c = me // 4, (me // 2) % 2, me % 2
    rows, width = tokens_ref.shape
    each = w_query_ref.shape[0]
    depth = width // 2
    per_core = G // 2
    chunks = per_core + 1
    columns = width // nz
    zh, par = z // 2, ((z + 1) // 2) % 2
    pair, mirror = z + 1 - 2 * (z % 2), nz - 1 - z
    group = 2 * zh + par
    waiting = []

    def dev(zz, yy, cc, xx):
        return ((zz * 2 + yy) * 2 + cc, xx)

    core_peer = dev(z, y, 1 - c, x)
    x_peer = dev(z, y, c, 1 - x)
    y_peer = dev(z, 1 - y, c, x)
    diagonal = dev(z, 1 - y, c, 1 - x)

    def remote(src, dst, ssem, rsem, to):
        return pltpu.make_async_remote_copy(
            src_ref=src, dst_ref=dst, send_sem=ssem, recv_sem=rsem, device_id=to, device_id_type=MESH
        )

    def go(src, dst, ssem, rsem, to, when=None):
        one = remote(src, dst, ssem, rsem, to)
        if when is None:
            one.start()
            waiting.append(one.wait_send)
        else:
            pl.when(when)(one.start)
            waiting.append(lambda: pl.when(when)(one.wait_send))

    def got(dst, rsem, when=None):
        one = remote(dst, dst, b_send.at[0], rsem, x_peer)
        if when is None:
            one.wait_recv()
        else:
            pl.when(when)(one.wait_recv)

    def slot(zs, yy, cc):
        return (zs * 2 + yy) * 2 + cc

    zs = z % 2
    mine = slot(zs, y, c)

    def block(xx, j, rb):
        return w.at[xx, j, pl.ds(pl.multiple_of(rb * each, 16), each)]

    def source(e, f, j):
        p, cc = (par + e) % 2, (c + f) % 2
        if j == 0:
            at = pl.ds(pl.multiple_of((2 * x + p) * HD, HD), HD)
            return cc, w_key_ref.at[:, at], w_value_ref.at[:, at]
        at = pl.ds(pl.multiple_of((p * G + cc * per_core + j - 1) * HD, HD), HD)
        return None, w_query_ref.at[:, at], None

    def place(e, f, j):
        return block(x, j, mine) if (e, f) == (0, 0) else stage.at[e, f, j]

    def load(e, f, j):
        cc, first, second = source(e, f, j)
        sem = load_sem.at[e, f, j]
        if second is None:
            pltpu.make_async_copy(first, place(e, f, j), sem).start()
        else:
            pl.when(cc == 0)(pltpu.make_async_copy(first, place(e, f, j), sem).start)
            pl.when(cc == 1)(pltpu.make_async_copy(second, place(e, f, j), sem).start)

    def loaded(e, f, j):
        pltpu.make_async_copy(source(e, f, j)[1], place(e, f, j), load_sem.at[e, f, j]).wait()

    for j in range(chunks):
        for e in range(2):
            for f in range(2):
                load(e, f, j)

    barrier = pltpu.get_barrier_semaphore()
    friends = [core_peer, x_peer, y_peer, diagonal]
    for d in range(1, nz):
        for f in range(2):
            friends.append(dev((z + d) % nz, y, (c + f) % 2, x))
    for friend in friends:
        pl.semaphore_signal(barrier, inc=1, device_id=friend, device_id_type=MESH)
    pl.semaphore_wait(barrier, len(friends))

    def spread(xx, j, rb, to_x, to_y):
        if to_x:
            go(block(xx, j, rb), block(xx, j, rb), w_send.at[xx, j, rb, 0], w_recv.at[xx, j, rb], x_peer)
        if to_y:
            go(block(xx, j, rb), block(xx, j, rb), w_send.at[xx, j, rb, 1], w_recv.at[xx, j, rb], y_peer)

    def arrived(xx, j, rb):
        got(block(xx, j, rb), w_recv.at[xx, j, rb])

    def begin(j):
        loaded(0, 0, j)
        spread(x, j, mine, True, True)
        for f in range(2):
            loaded(1, f, j)
            go(
                stage.at[1, f, j],
                block(x, j, mine),
                first_send.at[1, f, j],
                w_recv.at[x, j, mine],
                dev(pair, y, (c + f) % 2, x),
            )
        loaded(0, 1, j)
        go(stage.at[0, 1, j], block(x, j, mine), first_send.at[0, 1, j], w_recv.at[x, j, mine], core_peer)

    def home(j):
        for rb in (slot(zs, y, 1 - c), slot(1 - zs, y, c), slot(1 - zs, y, 1 - c)):
            arrived(x, j, rb)
            spread(x, j, rb, True, True)

    def relay_weights(j):
        for zz in (zs, 1 - zs):
            rb = slot(zz, 1 - y, 0)
            arrived(x, j, rb)
            spread(x, j, rb, True, False)
            rb = slot(zz, y, 1)
            arrived(1 - x, j, rb)
            spread(1 - x, j, rb, False, True)

    def rest_of_weights(j):
        for zz in (zs, 1 - zs):
            arrived(x, j, slot(zz, 1 - y, 1))
            arrived(1 - x, j, slot(zz, y, 0))
            for cc in range(2):
                arrived(1 - x, j, slot(zz, 1 - y, cc))

    begin(0)

    floats = tokens_ref[...].astype(f32)
    values = (
        floats
        * lax.rsqrt(jnp.mean(floats * floats, axis=1, keepdims=True) + eps_norm)
        * gain_ref[...]
    ).astype(bf16)
    normed[0] = values[:, :depth]
    normed[1] = values[:, depth:]

    def token_rows(zz, cc):
        return xs.at[pl.ds(pl.multiple_of((zz * 2 + cc) * rows, rows), rows)]

    at_me = pl.ds(pl.multiple_of((z * 2 + c) * rows, rows), rows)
    xs[at_me, :] = jnp.where(zh == 0, values[:, :depth], values[:, depth:])
    biases[x] = q_bias_ref[...]

    near, far = 2 - zh, 3 - 3 * zh
    go(normed.at[zh], token_rows(z, c), x_send.at[0], x_recv.at[z * 2 + c], dev(pair, y, c, x))
    go(normed.at[1 - zh], token_rows(z, c), x_send.at[1], x_recv.at[z * 2 + c], dev(near, y, c, x))
    go(normed.at[zh], token_rows(z, c), x_send.at[2], x_recv.at[z * 2 + c], core_peer)
    go(biases.at[x], biases.at[x], b_send.at[0], b_recv.at[0], x_peer)

    begin(1)
    home(0)

    def pass_tokens(zz, n):
        got(token_rows(zz, c), x_recv.at[zz * 2 + c])
        if n:
            go(
                token_rows(zz, c),
                token_rows(zz, c),
                x_send.at[2 + n],
                x_recv.at[zz * 2 + c],
                dev(pair, y, c, x),
                par == 1,
            )
        go(token_rows(zz, c), token_rows(zz, c), x_send.at[5 + n], x_recv.at[zz * 2 + c], core_peer)

    pass_tokens(pair, 0)
    relay_weights(0)
    home(1)
    pass_tokens(near, 1)
    pass_tokens(far, 2)
    begin(2)
    begin(3)

    wo_cols = 2 * 2 * HD
    half_rows = each // 2

    def wo_block(h, xx, s, half):
        first = pl.multiple_of(s * each + half * half_rows, 16)
        return wo.at[h, pl.ds(first, half_rows), pl.ds(pl.multiple_of(xx * wo_cols, HD), wo_cols)]

    wo_loads = []
    for h in range(per_core):
        for gl in range(2):
            for cc in range(2):
                zz = x * (3 - gl) + (1 - x) * gl
                wo_loads.append(
                    pltpu.make_async_copy(
                        w_out_ref.at[:, pl.ds((gl * G + cc * per_core + h) * HD, HD)],
                        wo.at[
                            h,
                            pl.ds(pl.multiple_of((y * 2 + c) * each, 16), each),
                            pl.ds(pl.multiple_of((zz * 2 + cc) * HD, HD), HD),
                        ],
                        wo_load_sem.at[h, gl, cc],
                    )
                )
                wo_loads[-1].start()

    for zz in range(1, nz + 1):
        at = (z + zz) % nz
        got(token_rows(at, 1 - c), x_recv.at[at * 2 + 1 - c])

    def multiply(j):
        rest_of_weights(j)
        theirs = jnp.dot(xs[...], w[1 - zh, j], preferred_element_type=f32)
        part_out[j] = theirs.astype(bf16)
        go(part_out.at[j], part_in.at[j], p_send.at[j], p_recv.at[j], dev(mirror, y, c, x))
        own[j] = jnp.dot(xs[...], w[zh, j], preferred_element_type=f32)

    multiply(0)
    relay_weights(1)
    home(2)
    multiply(1)
    relay_weights(2)
    home(3)

    def turn(values):
        return values * cos_ref[...] + pltpu.roll(values, HD // 2, 1) * sin_ref[...]

    src = y * 2 + x
    at_group = pl.ds(pl.multiple_of(group * HD, HD), HD)
    got(part_in.at[0], p_recv.at[0])
    total = own[0] + part_in[0].astype(f32)
    kv[c, src] = jnp.where(
        c == 0, turn(total + k_bias_ref[:, at_group]), total + v_bias_ref[:, at_group]
    ).astype(bf16)

    def kv_go(kind, s, n, to):
        go(kv.at[kind, s], kv.at[kind, s], kv_send.at[n], kv_recv.at[kind, s], to)

    def kv_got(kind, s):
        got(kv.at[kind, s], kv_recv.at[kind, s])

    kv_go(c, src, 0, x_peer)
    kv_go(c, src, 1, y_peer)
    kv_go(c, src, 2, diagonal)
    kv_go(c, src, 3, core_peer)

    multiply(2)
    relay_weights(3)

    at = jax.lax.broadcasted_iota(jnp.int32, (2 * rows, 8 * rows), 1)
    within = at % (2 * rows)
    key_at = (
        (at // (4 * rows)) * 4 + (within // rows) * 2 + (at // (2 * rows)) % 2
    ) * rows + within % rows
    at = jax.lax.broadcasted_iota(jnp.int32, (2 * rows, 8 * rows), 0)
    query_at = (y * 4 + (at // rows) * 2 + x) * rows + at % rows
    hidden[...] = jnp.where(key_at <= query_at, 0.0, masked_score)

    others = [(1 - y) * 2 + x, y * 2 + 1 - x, (1 - y) * 2 + 1 - x]
    for n, s in enumerate(others):
        kv_got(c, s)
        kv_go(c, s, 4 + n, core_peer)
    got(biases.at[1 - x], b_recv.at[0])
    for s in [src] + others:
        kv_got(1 - c, s)

    factor = math.log2(math.e) / math.sqrt(HD)
    cols_of_me = pl.ds(pl.multiple_of((z * 2 + c) * HD, HD), HD)

    def att_piece(h, zz, cc):
        return att.at[h, :, pl.ds(pl.multiple_of((zz * 2 + cc) * HD, HD), HD)]

    def attend(h):
        got(part_in.at[h + 1], p_recv.at[h + 1])
        at = pl.ds(pl.multiple_of((par * G + c * per_core + h) * HD, HD), HD)
        total = own[h + 1] + part_in[h + 1].astype(f32) + biases[zh, :, at]
        query = turn(total).astype(bf16)
        for t in range(nz):
            q = query[t * 2 * rows : (t + 1) * 2 * rows]
            scores = []
            for u in range(t + 1):
                keys = kv[0, :, u * 2 * rows : (u + 1) * 2 * rows].reshape(8 * rows, HD)
                one = lax.dot_general(
                    q, keys, (((1,), (1,)), ((), ())), preferred_element_type=f32
                )
                scores.append(one + hidden[...] if u == t else one)
            top = jnp.max(functools.reduce(jnp.maximum, scores), axis=1, keepdims=True)
            mixed, sums = None, None
            for u in range(t + 1):
                weights = jnp.exp2((scores[u] - top) * factor)
                sums = weights if sums is None else sums + weights
                vals = kv[1, :, u * 2 * rows : (u + 1) * 2 * rows].reshape(8 * rows, HD)
                one = jnp.dot(weights.astype(bf16), vals, preferred_element_type=f32)
                mixed = one if mixed is None else mixed + one
            mixed = (mixed / jnp.sum(sums, axis=1, keepdims=True)).astype(bf16)
            low, high = mixed[:rows], mixed[rows:]
            att[h, t * rows : (t + 1) * rows, cols_of_me] = jnp.where(c == 0, low, high)
            att_other[h, t * rows : (t + 1) * rows, :] = jnp.where(c == 0, high, low)
        index = z * 2 + c
        for way, ok in ((1, z < nz - 1), (-1, z > 0)):
            n = 0 if way == 1 else 1
            go(att_piece(h, z, c), att_piece(h, z, c), a_send.at[h, index, n], a_recv.at[h, index], dev(z + way, y, c, x), ok)
            go(att_other.at[h], att_piece(h, z, c), a_send.at[h, index, 2 + n], a_recv.at[h, index], dev(z + way, y, 1 - c, x), ok)
        go(att_other.at[h], att_piece(h, z, c), a_send.at[h, index, 4], a_recv.at[h, index], core_peer)

    def relay_attended(h, k):
        for way, here, more in ((1, z - k >= 0, z < nz - 1), (-1, z + k < nz, z > 0)):
            zz = z - way * k
            for cc in range(2):
                def act(zz=zz, cc=cc):
                    got(att_piece(h, zz, cc), a_recv.at[h, zz * 2 + cc])

                pl.when(here)(act)
                if k < nz - 1:
                    go(
                        att_piece(h, zz, cc),
                        att_piece(h, zz, cc),
                        a_send.at[h, zz * 2 + cc, 0 if way == 1 else 1],
                        a_recv.at[h, zz * 2 + cc],
                        dev(z + way, y, c, x),
                        jnp.logical_and(here, more),
                    )

    def wo_go(h, xx, s, half, n, to):
        go(wo_block(h, xx, s, half), wo_block(h, xx, s, half), wo_send.at[h, xx, s, half, n], wo_recv.at[h, xx, s, half], to)

    def wo_got(h, xx, s, half):
        got(wo_block(h, xx, s, half), wo_recv.at[h, xx, s, half])

    def wo_begin(h):
        for one in wo_loads[4 * h : 4 * h + 4]:
            one.wait()
        for half in range(2):
            for n, to in enumerate((x_peer, y_peer, core_peer)):
                wo_go(h, x, y * 2 + c, half, n, to)

    def wo_relay(h):
        for half in (0, 1):
            wo_got(h, x, (1 - y) * 2 + c, half)
            if half == 0:
                wo_go(h, x, (1 - y) * 2 + c, half, 0, x_peer)
            wo_go(h, x, (1 - y) * 2 + c, half, 2, core_peer)
            wo_got(h, 1 - x, y * 2 + c, half)
            if half == 1:
                wo_go(h, 1 - x, y * 2 + c, half, 1, y_peer)
            wo_go(h, 1 - x, y * 2 + c, half, 2, core_peer)

    def wo_finish(h):
        for half in (0, 1):
            wo_got(h, 1 - x, (1 - y) * 2 + c, half)
            wo_go(h, 1 - x, (1 - y) * 2 + c, half, 2, core_peer)
        for half in (0, 1):
            for xx in (x, 1 - x):
                for yy in (y, 1 - y):
                    wo_got(h, xx, yy * 2 + 1 - c, half)

    def produce(h):
        got(att_piece(h, z, 1 - c), a_recv.at[h, z * 2 + 1 - c])
        for first in range(0, columns, 512):
            size = min(512, columns - first)
            part = lax.dot_general(
                att[h], wo[h, first : first + size, :], (((1,), (1,)), ((), ())), preferred_element_type=f32
            )
            if h:
                part = part + acc[:, first : first + size]
            if h < per_core - 1:
                acc[:, first : first + size] = part
            else:
                for t in range(nz):
                    outs[t, :, first : first + size] = part[t * rows : (t + 1) * rows].astype(bf16)

    wo_begin(0)
    attend(0)
    multiply(3)
    wo_begin(1)
    wo_relay(0)
    relay_attended(0, 1)
    attend(1)
    wo_begin(2)
    relay_attended(0, 2)
    wo_relay(1)
    relay_attended(1, 1)
    attend(2)
    relay_attended(0, 3)
    wo_finish(0)
    relay_attended(1, 2)
    relay_attended(2, 1)
    wo_relay(2)
    produce(0)
    relay_attended(2, 2)
    relay_attended(1, 3)
    wo_finish(1)
    produce(1)
    wo_finish(2)
    relay_attended(2, 3)
    produce(2)

    def result_cols(zz):
        return pl.ds(pl.multiple_of(zz * columns, HD), columns)

    for d in range(1, nz):
        go(outs.at[(z + d) % nz], result.at[:, result_cols(z)], o_send.at[d - 1], o_recv.at[z], dev((z + d) % nz, y, c, x))
    out_ref[:, result_cols(z)] = outs[z]
    for done in waiting:
        done()
    for d in range(1, nz):
        zz = (z + d) % nz
        got(result.at[:, result_cols(zz)], o_recv.at[zz])
        out_ref[:, result_cols(zz)] = result[:, result_cols(zz)]


def in_planes(tokens, norm_gain, w_query, w_key, w_value, q_bias, k_bias, v_bias, w_out):
    blocks = lax.axis_size("blk")
    nz = blocks // 4
    rows, width = tokens.shape
    me, x = lax.axis_index("blk"), lax.axis_index("head")
    inner, each, per_core = w_query.shape[1], w_query.shape[0], G // 2
    chunks, held, columns = per_core + 1, 2 * nz * rows, width // nz
    where = jnp.arange(held, dtype=jnp.int32)
    there = (where // (2 * rows)) * 4 + ((me // 2) % 2) * 2 + (where // rows) % 2
    positions = (there * 2 + x) * rows + where % rows
    half = HD // 2
    freq = theta_base ** (-(jnp.arange(half, dtype=jnp.float32) * 2.0 / HD))
    angles = positions.astype(jnp.float32)[:, None] * freq[None, :]
    cosine, sine = jnp.cos(angles), jnp.sin(angles)
    cosine = jnp.concatenate([cosine, cosine], axis=1)
    sine = jnp.concatenate([-sine, sine], axis=1)
    vmem = pl.BlockSpec(memory_space=pltpu.VMEM)
    hbm = pl.BlockSpec(memory_space=pl.ANY)
    bf16, f32 = jnp.bfloat16, jnp.float32
    dma = pltpu.SemaphoreType.DMA
    return pl.pallas_call(
        functools.partial(plane_kernel, nz),
        out_shape=jax.ShapeDtypeStruct((rows, width), bf16),
        in_specs=[vmem, vmem, hbm, hbm, hbm, vmem, vmem, vmem, hbm, vmem, vmem],
        out_specs=vmem,
        scratch_shapes=[
            pltpu.VMEM((2, 2, chunks, each, HD), bf16),
            pltpu.VMEM((2, chunks, 8 * each, HD), bf16),
            pltpu.VMEM((2, rows, width // 2), bf16),
            pltpu.VMEM((held, width // 2), bf16),
            pltpu.VMEM((chunks, held, HD), bf16),
            pltpu.VMEM((chunks, held, HD), bf16),
            pltpu.VMEM((chunks, held, HD), f32),
            pltpu.VMEM((2, 1, inner), f32),
            pltpu.VMEM((2, 4, held, HD), bf16),
            pltpu.VMEM((2 * rows, 8 * rows), f32),
            pltpu.VMEM((per_core, nz * rows, 2 * nz * HD), bf16),
            pltpu.VMEM((per_core, nz * rows, HD), bf16),
            pltpu.VMEM((per_core, columns, 2 * nz * HD), bf16),
            pltpu.VMEM((nz * rows, columns), f32),
            pltpu.VMEM((nz, rows, columns), bf16),
            pltpu.VMEM((rows, width), bf16),
            dma((2, 2, chunks)),
            dma((per_core, 2, 2)),
            dma((2, 2, chunks)),
            dma((2, chunks, 8, 2)),
            dma((2, chunks, 8)),
            dma((8,)),
            dma((2 * nz,)),
            dma((1,)),
            dma((1,)),
            dma((chunks,)),
            dma((chunks,)),
            dma((7,)),
            dma((2, 4)),
            dma((per_core, 2 * nz, 5)),
            dma((per_core, 2 * nz)),
            dma((per_core, 2, 4, 2, 3)),
            dma((per_core, 2, 4, 2)),
            dma((nz - 1,)),
            dma((nz,)),
        ],
        compiler_params=pltpu.CompilerParams(
            collective_id=1, has_side_effects=True, vmem_limit_bytes=60 * 1024 * 1024
        ),
    )(
        tokens,
        norm_gain[None, :],
        w_query,
        w_key,
        w_value,
        q_bias[None, :],
        k_bias[None, :],
        v_bias[None, :],
        w_out.T,
        cosine,
        sine,
    )


def by_mesh(tokens, norm_gain, w_query, w_key, *rest):
    blocks, heads = lax.axis_size("blk"), lax.axis_size("head")
    groups = w_key.shape[1] // HD
    fits = blocks == 16 and heads == 2 and groups == 4 and w_query.shape[1] == 2 * G * HD
    run = in_planes if fits else on_device
    return run(tokens, norm_gain, w_query, w_key, *rest)


def solution(mesh):
    placed = (
        P(("blk", "head"), None),
        P(),
        P("blk", "head"),
        P("blk", None),
        P("blk", None),
        P("head"),
        P(),
        P(),
        P("head", "blk"),
    )
    return jax.shard_map(
        by_mesh, mesh=mesh, in_specs=placed, out_specs=P(("blk", "head"), None), check_vma=False
    )
```

```python
import functools
import math

import jax
import jax.numpy as jnp
from jax import lax
from jax.experimental import pallas as pl
from jax.experimental.pallas import tpu as pltpu
from jax.sharding import PartitionSpec as P

HD = 128
G = 6
MESH = pl.DeviceIdType.MESH

theta_base = 1000000.0
eps_norm = 1e-06
masked_score = -1e30

WQ, WKV, WO, KV, WQ_TAIL, WO_TAIL = range(6)
UP, DOWN, ACROSS, CORE = range(4)


def block_width(rows, limit):
    width = min(rows, limit)
    while rows % width:
        width -= 1
    return width


def kernel(
    sizes,
    tokens_ref,
    gain_ref,
    w_query_ref,
    w_key_ref,
    w_value_ref,
    q_bias_ref,
    k_bias_ref,
    v_bias_ref,
    w_out_ref,
    cos_ref,
    sin_ref,
    out_ref,
    wq,
    wkv,
    wo,
    kv,
    normed,
    query,
    attended,
    partial,
    outgoing,
    incoming,
    local_sem,
    send_sem,
    recv_sem,
    norm_send,
    norm_recv,
    sum_send,
    sum_recv,
):
    blocks, heads = sizes
    nz = blocks // 4
    me = lax.axis_index("blk")
    head = lax.axis_index("head")
    z, y, c = me // 4, (me // 2) % 2, me % 2
    local_rows, width = tokens_ref.shape
    group_rows = local_rows * heads
    heads_here = wq.shape[1] // HD
    kv_here = wkv.shape[1] // (2 * HD)
    per_kv = heads_here // kv_here
    kv_cols = kv_here * HD
    kv_start = pl.multiple_of((head * heads_here // G) * HD, HD)
    buffers = {WQ: wq, WKV: wkv, WO: wo, KV: kv, WQ_TAIL: wq, WO_TAIL: wo}
    queries, outs = (WQ, WQ_TAIL), (WO, WO_TAIL)
    scale = 1.0 / math.sqrt(HD)

    def slot_of(zz, yy, cc):
        return (zz * 2 + yy) * 2 + cc

    def rows_of(item, slot):
        each = buffers[item].shape[0] // blocks
        first, size = 0, each
        if item in queries + outs:
            cut = each // 2 // 16 * 16
            first, size = (0, cut) if item in (WQ, WO) else (cut, each - cut)
        return buffers[item].at[pl.ds(pl.multiple_of(slot * each + first, 16), size)]

    def whole_rows(ref):
        each = ref.shape[0] // blocks
        return ref.at[pl.ds(pl.multiple_of(me * each, each), each)]

    def target(route):
        step = {UP: 4, DOWN: -4, ACROSS: 2 - 4 * y, CORE: 1 - 2 * c}[route]
        return (me + step, head)

    def copy(item, slot, route):
        part = rows_of(item, slot)
        return pltpu.make_async_remote_copy(
            src_ref=part,
            dst_ref=part,
            send_sem=send_sem.at[item, slot, route],
            recv_sem=recv_sem.at[item, slot],
            device_id=target(route),
            device_id_type=MESH,
        )

    def send(item, slot, route):
        if route == UP:
            pl.when(z < nz - 1)(lambda: copy(item, slot, route).start())
        elif route == DOWN:
            pl.when(z > 0)(lambda: copy(item, slot, route).start())
        else:
            copy(item, slot, route).start()

    def sent(item, slot, route):
        if route == UP:
            pl.when(z < nz - 1)(lambda: copy(item, slot, route).wait_send())
        elif route == DOWN:
            pl.when(z > 0)(lambda: copy(item, slot, route).wait_send())
        else:
            copy(item, slot, route).wait_send()

    def arrived(item, slot):
        copy(item, slot, CORE).wait_recv()

    def below(k, act):
        pl.when(z >= k)(lambda: act(z - k))

    def above(k, act):
        pl.when(z + k < nz)(lambda: act(z + k))

    def z_step(item, k, yy, then=()):
        def from_below(zz):
            slot = slot_of(zz, yy, c)
            arrived(item, slot)
            for route in (UP,) + then:
                send(item, slot, route)

        def from_above(zz):
            slot = slot_of(zz, yy, c)
            arrived(item, slot)
            for route in (DOWN,) + then:
                send(item, slot, route)

        below(k, from_below)
        above(k, from_above)

    def at_distance(k, act):
        if k == 0:
            act(z)
        else:
            below(k, act)
            above(k, act)

    def across(item, k):
        def act(zz):
            slot = slot_of(zz, 1 - y, c)
            arrived(item, slot)
            send(item, slot, CORE)

        at_distance(k, act)

    def finish(item):
        for zz in range(nz):
            for yy in range(2):
                arrived(item, slot_of(zz, yy, 1 - c))

    def drain(item, both):
        for yy in (y, 1 - y) if both else (y,):
            for route in (UP, DOWN):
                sent(item, slot_of(z, yy, c), route)
            for k in range(1, nz):
                below(k, lambda zz, yy=yy: sent(item, slot_of(zz, yy, c), UP))
                above(k, lambda zz, yy=yy: sent(item, slot_of(zz, yy, c), DOWN))
        if both:
            sent(item, me, ACROSS)
        for zz in range(nz):
            if not both:
                sent(item, slot_of(zz, y, c), ACROSS)
            for yy in range(2):
                sent(item, slot_of(zz, yy, c), CORE)

    own = [
        pltpu.make_async_copy(w_query_ref, whole_rows(wq), local_sem.at[0]),
        pltpu.make_async_copy(
            w_key_ref.at[:, pl.ds(kv_start, kv_cols)],
            rows_of(WKV, me).at[:, pl.ds(0, kv_cols)],
            local_sem.at[1],
        ),
        pltpu.make_async_copy(
            w_value_ref.at[:, pl.ds(kv_start, kv_cols)],
            rows_of(WKV, me).at[:, pl.ds(kv_cols, kv_cols)],
            local_sem.at[2],
        ),
        pltpu.make_async_copy(w_out_ref, whole_rows(wo), local_sem.at[3]),
    ]
    for one in own:
        one.start()

    barrier = pltpu.get_barrier_semaphore()

    def greet(blk, hd):
        pl.semaphore_signal(barrier, inc=1, device_id=(blk, hd), device_id_type=MESH)

    pl.when(z < nz - 1)(lambda: greet(me + 4, head))
    pl.when(z > 0)(lambda: greet(me - 4, head))
    greet(target(ACROSS)[0], head)
    greet(target(CORE)[0], head)
    peers = [lax.rem(head + d, heads) for d in range(1, heads)]
    for peer in peers:
        greet(me, peer)
    ends = jnp.where(z < nz - 1, 1, 0) + jnp.where(z > 0, 1, 0)
    pl.semaphore_wait(barrier, ends + 2 + len(peers))

    own[1].wait()
    own[2].wait()
    for route in (ACROSS, UP, DOWN, CORE):
        send(WKV, me, route)
    own[0].wait()
    own[3].wait()
    for item in queries + outs:
        for route in (ACROSS, CORE):
            send(item, me, route)

    my_rows = pl.ds(pl.multiple_of(head * local_rows, local_rows), local_rows)
    floats = tokens_ref[...].astype(jnp.float32)
    normed[my_rows, :] = (
        floats
        * lax.rsqrt(jnp.mean(floats * floats, axis=1, keepdims=True) + eps_norm)
        * gain_ref[...]
    ).astype(jnp.bfloat16)

    there = slot_of(z, 1 - y, c)
    arrived(WKV, there)
    for route in (UP, DOWN, CORE):
        send(WKV, there, route)

    def norm_copy(d):
        return pltpu.make_async_remote_copy(
            src_ref=normed.at[my_rows],
            dst_ref=normed.at[my_rows],
            send_sem=norm_send.at[d],
            recv_sem=norm_recv.at[d],
            device_id=(me, peers[d]),
            device_id_type=MESH,
        )

    for d in range(len(peers)):
        norm_copy(d).start()

    for k in range(1, nz):
        z_step(WKV, k, y, (CORE,))
        z_step(WKV, k, 1 - y, (CORE,))
        if k == max(1, nz - 2):
            for item in queries:
                for route in (UP, DOWN):
                    send(item, me, route)
    for d in range(len(peers)):
        norm_copy(d).wait_recv()
    finish(WKV)

    cosine, sine = cos_ref[...], sin_ref[...]

    def turn(values):
        return values * cosine + pltpu.roll(values, HD // 2, 1) * sine

    kv_rows = pl.ds(pl.multiple_of(me * group_rows, group_rows), group_rows)
    sums = jnp.dot(normed[...], wkv[...], preferred_element_type=jnp.float32)
    for g in range(kv_here):
        bias = k_bias_ref[:, pl.ds(pl.multiple_of(kv_start + g * HD, HD), HD)]
        kv[kv_rows, pl.ds(g * HD, HD)] = turn(sums[:, g * HD : (g + 1) * HD] + bias).astype(
            jnp.bfloat16
        )
        bias = v_bias_ref[:, pl.ds(pl.multiple_of(kv_start + g * HD, HD), HD)]
        at = kv_cols + g * HD
        kv[kv_rows, pl.ds(at, HD)] = (sums[:, at : at + HD] + bias).astype(jnp.bfloat16)

    for item in queries:
        across(item, 0)
    for route in (UP, DOWN, ACROSS, CORE):
        send(KV, me, route)

    for k in range(1, nz):
        for item in queries:
            z_step(item, k, y, (ACROSS, CORE))
        z_step(KV, k, y, (ACROSS, CORE))
        if k == max(1, nz - 2):
            for item in outs:
                for route in (UP, DOWN):
                    send(item, me, route)
    for k in range(1, nz):
        if k == nz - 1:
            for item in outs:
                z_step(item, 1, y, (ACROSS, CORE))
        for item in queries:
            across(item, k)
    for k in range(nz):
        across(KV, k)
    for item in queries + (KV,):
        finish(item)

    joined = 2 if heads_here % 2 == 0 else 1

    def project(n, carry):
        cols = pl.ds(pl.multiple_of(n * joined * HD, joined * HD), joined * HD)
        total = jnp.dot(normed[...], wq[:, cols], preferred_element_type=jnp.float32)
        total = total + q_bias_ref[:, cols]
        for j in range(joined):
            query[n * joined + j] = turn(total[:, j * HD : (j + 1) * HD]).astype(jnp.bfloat16)
        return carry

    lax.fori_loop(0, heads_here // joined, project, 0)

    if nz > 2:
        for item in outs:
            z_step(item, 2, y, (ACROSS, CORE))

    keys = kv.shape[0]
    span = block_width(keys, 512)
    stacked = per_kv * group_rows
    last_query = me * group_rows + group_rows - 1
    steps = last_query // span + 1

    for g in range(kv_here):
        q = query[g * per_kv : (g + 1) * per_kv].reshape(stacked, HD)

        def attend(j, state, q=q, g=g):
            top, total, acc = state
            at = pl.ds(pl.multiple_of(j * span, span), span)
            scores = (
                lax.dot_general(
                    q,
                    kv[at, pl.ds(g * HD, HD)],
                    (((1,), (1,)), ((), ())),
                    preferred_element_type=jnp.float32,
                )
                * scale
            )
            shape = (per_kv, group_rows, span)
            rows = lax.broadcasted_iota(jnp.int32, shape, 1).reshape(stacked, span)
            columns = lax.broadcasted_iota(jnp.int32, (stacked, span), 1)
            visible = columns + j * span <= rows + me * group_rows
            scores = jnp.where(visible, scores, masked_score)
            new_top = jnp.maximum(top, jnp.max(scores, axis=1, keepdims=True))
            weights = jnp.where(visible, jnp.exp(scores - new_top), 0.0)
            fade = jnp.exp(top - new_top)
            total = total * fade + jnp.sum(weights, axis=1, keepdims=True)
            acc = acc * fade + jnp.dot(
                weights.astype(jnp.bfloat16),
                kv[at, pl.ds(kv_cols + g * HD, HD)],
                preferred_element_type=jnp.float32,
            )
            return (new_top, total, acc)

        start = (
            jnp.full((stacked, 1), masked_score, jnp.float32),
            jnp.zeros((stacked, 1), jnp.float32),
            jnp.zeros((stacked, HD), jnp.float32),
        )
        top, total, acc = lax.fori_loop(0, steps, attend, start)
        result = (acc / total).astype(jnp.bfloat16)
        for r in range(per_kv):
            attended[:, pl.ds((g * per_kv + r) * HD, HD)] = result[
                r * group_rows : (r + 1) * group_rows
            ]
        for k in range(3, nz):
            if g == 0:
                z_step(WO, k, y, (ACROSS, CORE))
    for k in range(3, nz):
        z_step(WO_TAIL, k, y, (ACROSS, CORE))

    each = wo.shape[0] // blocks
    grouped = (4 * each) % HD == 0
    groups = nz if grouped else 1
    chunk = width // groups

    def sum_copy(d, i, start):
        rows = pl.ds(pl.multiple_of(peers[d] * local_rows, local_rows), local_rows)
        cols = pl.ds(pl.multiple_of(start, HD), chunk)
        return pltpu.make_async_remote_copy(
            src_ref=outgoing.at[rows, cols],
            dst_ref=incoming.at[d, :, cols],
            send_sem=sum_send.at[d, i],
            recv_sem=sum_recv.at[d, i],
            device_id=(me, peers[d]),
            device_id_type=MESH,
        )

    def produce(start, size):
        cols = pl.ds(pl.multiple_of(start, HD), size)
        result = lax.dot_general(
            attended[...],
            wo[cols, :],
            (((1,), (1,)), ((), ())),
            preferred_element_type=jnp.float32,
        )
        partial[:, cols] = result
        outgoing[:, cols] = result.astype(jnp.bfloat16)

    def place(i):
        way = 1 - 2 * (z // max(1, nz // 2)) if nz > 1 else 1
        return lax.rem(z + way * i + nz, nz)

    if grouped:

        def produce_group(i, carry):
            zz = place(i)
            slot = slot_of(zz, 1 - y, c)
            for item in outs:
                arrived(item, slot)
                send(item, slot, CORE)
            for item in outs:
                for yy in range(2):
                    arrived(item, slot_of(zz, yy, 1 - c))
            produce(zz * 4 * each, chunk)
            for d in range(len(peers)):
                sum_copy(d, i, zz * chunk).start()
            return carry

        lax.fori_loop(0, nz, produce_group, 0)
    else:
        for item in outs:
            for k in range(nz):
                across(item, k)
            finish(item)
        part = 256
        lax.fori_loop(0, width // part, lambda n, carry: (produce(n * part, part), carry)[1], 0)
        for d in range(len(peers)):
            sum_copy(d, 0, 0).start()

    for item in queries + outs + (WKV, KV):
        drain(item, item == WKV)
    for d in range(len(peers)):
        norm_copy(d).wait_send()

    def collect(i, carry):
        start = place(i) * chunk if grouped else 0
        cols = pl.ds(pl.multiple_of(start, HD), chunk)
        for d in range(len(peers)):
            sum_copy(d, i, start).wait_recv()
        result = partial[my_rows, cols]
        for d in range(len(peers)):
            result = result + incoming[d, :, cols].astype(jnp.float32)
        out_ref[:, cols] = result.astype(jnp.bfloat16)
        for d in range(len(peers)):
            sum_copy(d, i, start).wait_send()
        return carry

    lax.fori_loop(0, groups, collect, 0)


def on_device(tokens, norm_gain, w_query, w_key, w_value, q_bias, k_bias, v_bias, w_out):
    blocks, heads = lax.axis_size("blk"), lax.axis_size("head")
    local_rows, width = tokens.shape
    group_rows = local_rows * heads
    heads_here = w_query.shape[1] // HD
    kv_here = max(1, heads_here // G)
    positions = lax.axis_index("blk") * group_rows + jnp.arange(group_rows, dtype=jnp.int32)
    half = HD // 2
    freq = theta_base ** (-(jnp.arange(half, dtype=jnp.float32) * 2.0 / HD))
    angles = positions.astype(jnp.float32)[:, None] * freq[None, :]
    cosine, sine = jnp.cos(angles), jnp.sin(angles)
    cosine = jnp.concatenate([cosine, cosine], axis=1)
    sine = jnp.concatenate([-sine, sine], axis=1)
    inner = heads_here * HD
    vmem = pl.BlockSpec(memory_space=pltpu.VMEM)
    hbm = pl.BlockSpec(memory_space=pl.ANY)
    others = max(1, heads - 1)
    bf16, f32 = jnp.bfloat16, jnp.float32
    return pl.pallas_call(
        functools.partial(kernel, (blocks, heads)),
        out_shape=jax.ShapeDtypeStruct((local_rows, width), bf16),
        in_specs=[vmem, vmem, hbm, hbm, hbm, vmem, vmem, vmem, hbm, vmem, vmem],
        out_specs=vmem,
        scratch_shapes=[
            pltpu.VMEM((width, inner), bf16),
            pltpu.VMEM((width, 2 * kv_here * HD), bf16),
            pltpu.VMEM((width, inner), bf16),
            pltpu.VMEM((blocks * group_rows, 2 * kv_here * HD), bf16),
            pltpu.VMEM((group_rows, width), bf16),
            pltpu.VMEM((heads_here, group_rows, HD), bf16),
            pltpu.VMEM((group_rows, inner), bf16),
            pltpu.VMEM((group_rows, width), f32),
            pltpu.VMEM((group_rows, width), bf16),
            pltpu.VMEM((others, local_rows, width), bf16),
            pltpu.SemaphoreType.DMA((4,)),
            pltpu.SemaphoreType.DMA((6, blocks, 4)),
            pltpu.SemaphoreType.DMA((6, blocks)),
            pltpu.SemaphoreType.DMA((others,)),
            pltpu.SemaphoreType.DMA((others,)),
            pltpu.SemaphoreType.DMA((others, blocks // 4)),
            pltpu.SemaphoreType.DMA((others, blocks // 4)),
        ],
        compiler_params=pltpu.CompilerParams(
            collective_id=0, has_side_effects=True, vmem_limit_bytes=60 * 1024 * 1024
        ),
    )(
        tokens,
        norm_gain[None, :],
        w_query,
        w_key,
        w_value,
        q_bias[None, :],
        k_bias[None, :],
        v_bias[None, :],
        w_out.T,
        cosine,
        sine,
    )


def plane_kernel(
    nz,
    tokens_ref,
    gain_ref,
    w_query_ref,
    w_key_ref,
    w_value_ref,
    q_bias_ref,
    k_bias_ref,
    v_bias_ref,
    w_out_ref,
    base_cos_ref,
    base_sin_ref,
    out_ref,
    tokens,
    gain,
    q_flat,
    k_bias,
    v_bias,
    cosine,
    sine,
    stage,
    w,
    normed,
    xs,
    part_out,
    part_in,
    full,
    biases,
    kv,
    hidden,
    att,
    att_other,
    wo,
    acc,
    outs,
    result,
    small_sem,
    load_sem,
    wo_load_sem,
    w_send,
    w_home,
    w_relay,
    w_rest,
    x_send,
    x_recv,
    b_sem,
    p_send,
    p_recv,
    kv_send,
    kv_recv,
    a_send,
    a_recv,
    wo_send,
    wo_recv,
    o_sem,
):
    f32, bf16 = jnp.float32, jnp.bfloat16
    me = lax.axis_index("blk")
    x = lax.axis_index("head")
    z, y, c = me // 4, (me // 2) % 2, me % 2
    rows, width = tokens_ref.shape
    each = w_query_ref.shape[0]
    depth = width // nz
    per_core = G // 2
    chunks = per_core + 1
    columns = width // nz
    zh = z // 2
    inner = ((z + 1) // 2) % 2 == 1
    outer = jnp.logical_not(inner)
    pair = z + 1 - 2 * (z % 2)
    near, far = 2 - zh, 3 - 3 * zh
    final_waits = []

    def dev(zz, yy, cc, xx):
        return ((zz * 2 + yy) * 2 + cc, xx)

    core_peer = dev(z, y, 1 - c, x)
    x_peer = dev(z, y, c, 1 - x)
    y_peer = dev(z, 1 - y, c, x)
    diagonal = dev(z, 1 - y, c, 1 - x)

    def go(src, dst, ssem, rsem, to, when=None):
        one = pltpu.make_async_remote_copy(
            src_ref=src, dst_ref=dst, send_sem=ssem, recv_sem=rsem, device_id=to, device_id_type=MESH
        )
        if when is None:
            one.start()
        else:
            pl.when(when)(one.start)

    def got(like, rsem):
        pltpu.make_async_remote_copy(
            src_ref=like, dst_ref=like, send_sem=b_sem.at[0], recv_sem=rsem, device_id=x_peer, device_id_type=MESH
        ).wait_recv()

    def at_end(like, ssem, when=None):
        one = pltpu.make_async_remote_copy(
            src_ref=like, dst_ref=like, send_sem=ssem, recv_sem=b_sem.at[1], device_id=x_peer, device_id_type=MESH
        )
        if when is None:
            final_waits.append(one.wait_send)
        else:
            final_waits.append(lambda: pl.when(when)(one.wait_send))

    small = [
        pltpu.make_async_copy(tokens_ref, tokens, small_sem.at[0]),
        pltpu.make_async_copy(gain_ref, gain, small_sem.at[1]),
        pltpu.make_async_copy(q_bias_ref, q_flat, small_sem.at[2]),
        pltpu.make_async_copy(k_bias_ref, k_bias, small_sem.at[3]),
        pltpu.make_async_copy(v_bias_ref, v_bias, small_sem.at[4]),
    ]
    for one in small:
        one.start()

    barrier = pltpu.get_barrier_semaphore()
    friends = [core_peer, x_peer, y_peer, diagonal]
    for d in range(1, nz):
        for f in range(2):
            friends.append(dev((z + d) % nz, y, (c + f) % 2, x))
    for friend in friends:
        pl.semaphore_signal(barrier, inc=1, device_id=friend, device_id_type=MESH)

    mine = y * 2 + c

    def block(xx, j, s):
        return w.at[
            j,
            pl.ds(pl.multiple_of(s * each, 16), each),
            pl.ds(pl.multiple_of(xx * 2 * HD, HD), 2 * HD),
        ]

    def blocks_like(n):
        return w.at[0, pl.ds(0, n * each), pl.ds(0, 2 * HD)]

    def load(f, j):
        place = stage.at[j] if f else block(x, j, mine)
        cc = (c + f) % 2
        sem = load_sem.at[j]
        if j == 0:
            at = pl.ds(pl.multiple_of(2 * x * HD, HD), 2 * HD)
            pl.when(cc == 0)(pltpu.make_async_copy(w_key_ref.at[:, at], place, sem).start)
            pl.when(cc == 1)(pltpu.make_async_copy(w_value_ref.at[:, at], place, sem).start)
        else:
            for gl in range(2):
                at = pl.ds(pl.multiple_of((gl * G + cc * per_core + j - 1) * HD, HD), HD)
                pltpu.make_async_copy(
                    w_query_ref.at[:, at], place.at[:, pl.ds(gl * HD, HD)], sem
                ).start()

    def loaded(j):
        pltpu.make_async_copy(blocks_like(2), blocks_like(2), load_sem.at[j]).wait()

    for j in range(chunks):
        for f in range(2):
            load(f, j)

    wo_cols = 2 * 2 * HD
    half_rows = each // 2

    def wo_block(h, xx, s, half):
        first = pl.multiple_of(s * each + half * half_rows, 16)
        return wo.at[h, pl.ds(first, half_rows), pl.ds(pl.multiple_of(xx * wo_cols, HD), wo_cols)]

    def wo_like(n):
        return wo.at[0, pl.ds(0, n * half_rows), pl.ds(0, wo_cols)]

    for h in range(per_core):
        for gl in range(2):
            for cc in range(2):
                zz = 2 * x + gl
                pltpu.make_async_copy(
                    w_out_ref.at[:, pl.ds((gl * G + cc * per_core + h) * HD, HD)],
                    wo.at[
                        h,
                        pl.ds(pl.multiple_of((y * 2 + c) * each, 16), each),
                        pl.ds(pl.multiple_of((zz * 2 + cc) * HD, HD), HD),
                    ],
                    wo_load_sem.at[h],
                ).start()

    small[0].wait()
    small[1].wait()
    floats = tokens[...].astype(f32)
    values = (
        floats
        * lax.rsqrt(jnp.mean(floats * floats, axis=1, keepdims=True) + eps_norm)
        * gain[...].reshape(1, width)
    ).astype(bf16)
    for n in range(nz):
        normed[n] = values[:, n * depth : (n + 1) * depth]
    at_me = pl.ds(pl.multiple_of((z * 2 + c) * rows, rows), rows)
    xs[at_me, :] = normed[z]
    small[2].wait()
    flat = q_flat[...]
    for n in range(q_flat.shape[0] // HD):
        biases[x, n] = flat[n * HD : (n + 1) * HD].reshape(1, HD)
    small[3].wait()
    small[4].wait()

    pl.semaphore_wait(barrier, len(friends))

    def home_send(j, s, cc):
        here = block(x, j, s)
        for to, ssem, relayed in ((x_peer, w_send.at[0], cc == 1), (y_peer, w_send.at[1], cc == 0)):
            go(here, here, ssem, w_relay.at[j], to, relayed)
            go(here, here, ssem, w_rest.at[j], to, jnp.logical_not(relayed))

    def own_block(j):
        loaded(j)
        go(stage.at[j], block(x, j, mine), w_send.at[2], w_home.at[j], core_peer)
        home_send(j, mine, c)

    def home(j):
        got(blocks_like(1), w_home.at[j])
        home_send(j, y * 2 + 1 - c, 1 - c)

    def relay_weights(j):
        got(blocks_like(2), w_relay.at[j])
        here = block(x, j, (1 - y) * 2)
        go(here, here, w_send.at[0], w_rest.at[j], x_peer)
        here = block(1 - x, j, y * 2 + 1)
        go(here, here, w_send.at[1], w_rest.at[j], y_peer)

    at_end(w.at[pl.ds(0, 3), :, pl.ds(0, 2 * HD)], w_send.at[0])
    at_end(w.at[pl.ds(0, 3), :, pl.ds(0, 2 * HD)], w_send.at[1])
    at_end(blocks_like(chunks), w_send.at[2])

    def token_block(zz, cc):
        return xs.at[pl.ds(pl.multiple_of((zz * 2 + cc) * rows, rows), rows)]

    def tokens_like(n):
        return xs.at[pl.ds(0, n * rows)]

    def send_tokens():
        for to in (far, near, pair):
            go(normed.at[to], token_block(z, c), x_send.at[0], x_recv.at[z], dev(to, y, c, x))
        go(normed.at[z], token_block(z, c), x_send.at[1], x_recv.at[nz], core_peer)

    def pass_tokens(zz):
        here = token_block(zz, c)
        got(here, x_recv.at[zz])
        go(here, here, x_send.at[1], x_recv.at[nz], core_peer)

    def wait_tokens():
        got(tokens_like(nz), x_recv.at[nz])

    at_end(tokens_like(nz - 1), x_send.at[0])
    at_end(tokens_like(nz), x_send.at[1])

    def send_biases():
        go(biases.at[x], biases.at[x], b_sem.at[0], b_sem.at[1], x_peer)

    held = xs.shape[0]
    part_rows = held // p_recv.shape[2]

    def shard(s):
        return pl.ds(pl.multiple_of(s * HD, HD), HD)

    def part_go(j, n, k, to, there):
        at = pl.ds(n * part_rows, part_rows)
        go(
            part_out.at[j, k, at],
            part_in.at[j, there, at],
            p_send.at[0],
            p_recv.at[j, there, n],
            dev(to, y, c, x),
        )

    def part_got(j, n, k):
        got(part_in.at[j, k, pl.ds(n * part_rows, part_rows)], p_recv.at[j, k, n])

    def multiply(j):
        got(blocks_like(4), w_rest.at[j])
        full[j] = jnp.dot(xs[...], w[j], preferred_element_type=f32)

        def send():
            for k, s in enumerate((far, near, pair)):
                for n in range(p_recv.shape[2]):
                    at = pl.ds(n * part_rows, part_rows)
                    part_out[j, k, at] = full[j, at, shard(s)].astype(bf16)
                    part_go(j, n, k, pair, k)

        pl.when(outer)(send)

    def chain(j, steps):
        def act():
            for k, s, source, to, there in steps:
                for n in range(p_recv.shape[2]):
                    at = pl.ds(n * part_rows, part_rows)
                    part_got(j, n, source)
                    part_out[j, k, at] = (
                        full[j, at, shard(s)] + part_in[j, source, at].astype(f32)
                    ).astype(bf16)
                    part_go(j, n, k, to, there)

        pl.when(inner)(act)

    def inward(j):
        chain(j, ((0, far, 0, near, 3), (1, near, 1, near, 4)))

    def outward(j):
        chain(j, ((2, pair, 3, pair, 2),))

    def summed(j):
        def more():
            for n in range(p_recv.shape[2]):
                part_got(j, n, 4)
            full[j, :, shard(z)] = full[j, :, shard(z)] + part_in[j, 4].astype(f32)

        pl.when(inner)(more)
        for n in range(p_recv.shape[2]):
            part_got(j, n, 2)
        return full[j, :, shard(z)] + part_in[j, 2].astype(f32)

    at_end(part_out, p_send.at[0])

    def turn(values):
        return values * cosine[...] + pltpu.roll(values, HD // 2, 1) * sine[...]

    here_src = y * 2 + x
    others = [(1 - y) * 2 + x, y * 2 + 1 - x, (1 - y) * 2 + 1 - x]

    def make_tables():
        signs = jnp.where(lax.broadcasted_iota(jnp.int32, (1, HD), 1) < HD // 2, -1.0, 1.0)
        cos_in, sin_in = base_cos_ref[2 * nz :], base_sin_ref[2 * nz :]
        for n in range(2 * nz):
            cos_at, sin_at = base_cos_ref[n : n + 1], base_sin_ref[n : n + 1]
            cosine[n * rows : (n + 1) * rows] = cos_at * cos_in - sin_at * sin_in
            sine[n * rows : (n + 1) * rows] = (sin_at * cos_in + cos_at * sin_in) * signs
        at = lax.broadcasted_iota(jnp.int32, (2 * rows, 8 * rows), 1)
        within = at % (2 * rows)
        key_at = (
            (at // (4 * rows)) * 4 + (within // rows) * 2 + (at // (2 * rows)) % 2
        ) * rows + within % rows
        at = lax.broadcasted_iota(jnp.int32, (2 * rows, 8 * rows), 0)
        query_at = (y * 4 + (at // rows) * 2 + x) * rows + at % rows
        hidden[...] = jnp.where(key_at <= query_at, 0.0, masked_score)

    def make_kv():
        at_group = pl.ds(pl.multiple_of(z * HD, HD), HD)
        total = summed(0)
        kv[c, here_src] = jnp.where(
            c == 0, turn(total + k_bias[:, at_group]), total + v_bias[:, at_group]
        ).astype(bf16)
        here = kv.at[c, here_src]
        go(here, here, kv_send.at[0], kv_recv.at[0], x_peer)
        go(here, here, kv_send.at[0], kv_recv.at[1], y_peer)
        go(here, here, kv_send.at[0], kv_recv.at[2], diagonal)
        go(here, here, kv_send.at[1], kv_recv.at[3], core_peer)

    def kv_pass():
        for n, s in ((0, others[1]), (1, others[0]), (2, others[2])):
            here = kv.at[c, s]
            got(here, kv_recv.at[n])
            go(here, here, kv_send.at[1], kv_recv.at[3], core_peer)

    def kv_peer():
        got(kv.at[0], kv_recv.at[3])
        got(biases.at[1 - x], b_sem.at[1])

    at_end(kv.at[0, pl.ds(0, 3)], kv_send.at[0])
    at_end(kv.at[0], kv_send.at[1])
    at_end(biases.at[0], b_sem.at[0])

    factor = math.log2(math.e) / math.sqrt(HD)

    def att_piece(h, zz, cc):
        return att.at[h, :, pl.ds(pl.multiple_of((zz * 2 + cc) * HD, HD), HD)]

    def attend(h):
        total = summed(h + 1) + biases[zh, (z % 2) * G + c * per_core + h]
        query = turn(total).astype(bf16)
        cols_of_me = pl.ds(pl.multiple_of((z * 2 + c) * HD, HD), HD)
        for t in range(nz):
            q = query[t * 2 * rows : (t + 1) * 2 * rows]
            scores = []
            for u in range(t + 1):
                keys = kv[0, :, u * 2 * rows : (u + 1) * 2 * rows].reshape(8 * rows, HD)
                one = lax.dot_general(
                    q, keys, (((1,), (1,)), ((), ())), preferred_element_type=f32
                )
                scores.append(one + hidden[...] if u == t else one)
            top = jnp.max(functools.reduce(jnp.maximum, scores), axis=1, keepdims=True)
            mixed, sums = None, None
            for u in range(t + 1):
                weights = jnp.exp2((scores[u] - top) * factor)
                sums = weights if sums is None else sums + weights
                vals = kv[1, :, u * 2 * rows : (u + 1) * 2 * rows].reshape(8 * rows, HD)
                one = jnp.dot(weights.astype(bf16), vals, preferred_element_type=f32)
                mixed = one if mixed is None else mixed + one
            mixed = (mixed / jnp.sum(sums, axis=1, keepdims=True)).astype(bf16)
            low, high = mixed[:rows], mixed[rows:]
            att[h, t * rows : (t + 1) * rows, cols_of_me] = jnp.where(c == 0, low, high)
            att_other[h, t * rows : (t + 1) * rows, :] = jnp.where(c == 0, high, low)
        here, there = att_piece(h, z, c), att_other.at[h]
        go(here, here, a_send.at[0], a_recv.at[h, z], dev(near, y, c, x), inner)
        go(there, here, a_send.at[0], a_recv.at[h, z], dev(near, y, 1 - c, x), inner)
        go(here, here, a_send.at[1], a_recv.at[h, z], dev(pair, y, c, x))
        go(there, here, a_send.at[1], a_recv.at[h, z], dev(pair, y, 1 - c, x))
        go(there, here, a_send.at[2], a_recv.at[h, z], core_peer)

    def att_like(n):
        return att.at[0, :, pl.ds(0, n * HD)]

    def relay_attended(h, zz, to):
        def act():
            got(att_like(2), a_recv.at[h, zz])
            for cc in range(2):
                here = att_piece(h, zz, cc)
                go(here, here, a_send.at[3], a_recv.at[h, zz], dev(to, y, c, x))

        pl.when(inner)(act)

    def from_near(h):
        relay_attended(h, near, pair)

    def from_pair(h):
        relay_attended(h, pair, near)

    def from_far(h):
        relay_attended(h, far, pair)

    def gathered(h):
        def act():
            for zz in (pair, near, far):
                got(att_like(2), a_recv.at[h, zz])

        pl.when(outer)(act)

    at_end(att.at[:, :, pl.ds(0, 2 * HD)], a_send.at[0], inner)
    at_end(att.at[:, :, pl.ds(0, 2 * HD)], a_send.at[1])
    at_end(att.at[:, :, pl.ds(0, HD)], a_send.at[2])
    at_end(att.at[:, :, pl.ds(0, 6 * HD)], a_send.at[3], inner)

    def wo_go(h, xx, s, half, n, rsem, to):
        here = wo_block(h, xx, s, half)
        go(here, here, wo_send.at[n], rsem, to)

    def wo_begin(h):
        like = wo.at[h, pl.ds(0, each), pl.ds(0, wo_cols)]
        pltpu.make_async_copy(like, like, wo_load_sem.at[h]).wait()
        for half in range(2):
            for n, to in enumerate((x_peer, y_peer, core_peer)):
                wo_go(h, x, y * 2 + c, half, n, wo_recv.at[h, n], to)

    def wo_relay(h):
        got(wo_like(2), wo_recv.at[h, 1])
        wo_go(h, x, (1 - y) * 2 + c, 0, 0, wo_recv.at[h, 3], x_peer)
        got(wo_like(2), wo_recv.at[h, 0])
        wo_go(h, 1 - x, y * 2 + c, 1, 1, wo_recv.at[h, 3], y_peer)
        for half in range(2):
            wo_go(h, x, (1 - y) * 2 + c, half, 2, wo_recv.at[h, 2], core_peer)
            wo_go(h, 1 - x, y * 2 + c, half, 2, wo_recv.at[h, 2], core_peer)

    def wo_finish(h):
        got(wo_like(2), wo_recv.at[h, 3])
        for half in range(2):
            wo_go(h, 1 - x, (1 - y) * 2 + c, half, 2, wo_recv.at[h, 2], core_peer)

    def wo_wait(h):
        got(wo_like(8), wo_recv.at[h, 2])

    at_end(wo.at[:, pl.ds(0, 3 * half_rows), pl.ds(0, wo_cols)], wo_send.at[0])
    at_end(wo.at[:, pl.ds(0, 3 * half_rows), pl.ds(0, wo_cols)], wo_send.at[1])
    at_end(wo.at[:, pl.ds(0, 8 * half_rows), pl.ds(0, wo_cols)], wo_send.at[2])

    def produce(h):
        wo_wait(h)
        gathered(h)
        got(att_like(1), a_recv.at[h, z])
        for first in range(0, columns, 512):
            size = min(512, columns - first)
            part = lax.dot_general(
                att[h], wo[h, first : first + size, :], (((1,), (1,)), ((), ())), preferred_element_type=f32
            )
            if h:
                part = part + acc[:, first : first + size]
            if h < per_core - 1:
                acc[:, first : first + size] = part
            else:
                for t in range(nz):
                    outs[t, :, first : first + size] = part[t * rows : (t + 1) * rows].astype(bf16)

    def result_cols(zz):
        return pl.ds(pl.multiple_of(zz * columns, HD), columns)

    def last():
        for d in range(1, nz):
            to = (z + d) % nz
            go(outs.at[to], result.at[:, result_cols(z)], o_sem.at[0], o_sem.at[1], dev(to, y, c, x))

    at_end(outs.at[pl.ds(0, nz - 1)], o_sem.at[0])

    send_tokens()
    own_block(0)
    send_biases()
    home(0)
    own_block(1)
    make_tables()
    relay_weights(0)
    home(1)
    own_block(2)
    pass_tokens(pair)
    pass_tokens(near)
    pass_tokens(far)
    wait_tokens()
    multiply(0)
    relay_weights(1)
    home(2)
    own_block(3)
    inward(0)
    home(3)
    multiply(1)
    relay_weights(2)
    outward(0)
    make_kv()
    inward(1)
    multiply(2)
    outward(1)
    relay_weights(3)
    kv_pass()
    kv_peer()
    attend(0)
    inward(2)
    outward(2)
    multiply(3)
    from_pair(0)
    inward(3)
    from_near(0)
    wo_begin(0)
    attend(1)
    outward(3)
    from_far(0)
    wo_begin(1)
    from_pair(1)
    attend(2)
    from_near(1)
    wo_relay(0)
    wo_begin(2)
    from_far(1)
    from_pair(2)
    wo_finish(0)
    wo_relay(1)
    from_near(2)
    produce(0)
    wo_finish(1)
    wo_relay(2)
    from_far(2)
    produce(1)
    wo_finish(2)
    produce(2)
    last()
    out_ref[:, result_cols(z)] = outs[z]
    for done in final_waits:
        done()
    got(outs.at[pl.ds(0, nz - 1)], o_sem.at[1])
    for d in range(1, nz):
        zz = (z + d) % nz
        out_ref[:, result_cols(zz)] = result[:, result_cols(zz)]


def in_planes(tokens, norm_gain, w_query, w_key, w_value, q_bias, k_bias, v_bias, w_out):
    blocks = lax.axis_size("blk")
    nz = blocks // 4
    rows, width = tokens.shape
    me, x = lax.axis_index("blk"), lax.axis_index("head")
    inner, each, per_core = w_query.shape[1], w_query.shape[0], G // 2
    chunks, held, columns = per_core + 1, 2 * nz * rows, width // nz
    where = jnp.arange(2 * nz, dtype=jnp.int32)
    there = (where // 2) * 4 + ((me // 2) % 2) * 2 + where % 2
    positions = jnp.concatenate([(there * 2 + x) * rows, jnp.arange(rows, dtype=jnp.int32)])
    half = HD // 2
    lanes = jnp.arange(HD, dtype=jnp.int32) % half
    freq = theta_base ** (-(lanes.astype(jnp.float32) * 2.0 / HD))
    angles = positions.astype(jnp.float32)[:, None] * freq[None, :]
    base_cos, base_sin = jnp.cos(angles), jnp.sin(angles)
    vmem = pl.BlockSpec(memory_space=pltpu.VMEM)
    hbm = pl.BlockSpec(memory_space=pltpu.HBM)
    bf16, f32 = jnp.bfloat16, jnp.float32
    dma = pltpu.SemaphoreType.DMA
    return pl.pallas_call(
        functools.partial(plane_kernel, nz),
        out_shape=jax.ShapeDtypeStruct((rows, width), bf16),
        in_specs=[hbm] * 9 + [vmem] * 2,
        out_specs=vmem,
        scratch_shapes=[
            pltpu.VMEM((rows, width), bf16),
            pltpu.VMEM((width,), f32),
            pltpu.VMEM((inner,), f32),
            pltpu.VMEM((1, w_key.shape[1]), f32),
            pltpu.VMEM((1, w_key.shape[1]), f32),
            pltpu.VMEM((held, HD), f32),
            pltpu.VMEM((held, HD), f32),
            pltpu.VMEM((chunks, each, 2 * HD), bf16),
            pltpu.VMEM((chunks, 4 * each, 4 * HD), bf16),
            pltpu.VMEM((nz, rows, width // nz), bf16),
            pltpu.VMEM((held, width // nz), bf16),
            pltpu.VMEM((chunks, 3, held, HD), bf16),
            pltpu.VMEM((chunks, 5, held, HD), bf16),
            pltpu.VMEM((chunks, held, 4 * HD), f32),
            pltpu.VMEM((2, inner // HD, 1, HD), f32),
            pltpu.VMEM((2, 4, held, HD), bf16),
            pltpu.VMEM((2 * rows, 8 * rows), f32),
            pltpu.VMEM((per_core, nz * rows, 2 * nz * HD), bf16),
            pltpu.VMEM((per_core, nz * rows, HD), bf16),
            pltpu.VMEM((per_core, columns, 2 * nz * HD), bf16),
            pltpu.VMEM((nz * rows, columns), f32),
            pltpu.VMEM((nz, rows, columns), bf16),
            pltpu.VMEM((rows, width), bf16),
            dma((5,)),
            dma((chunks,)),
            dma((per_core,)),
            dma((3,)),
            dma((chunks,)),
            dma((chunks,)),
            dma((chunks,)),
            dma((2,)),
            dma((nz + 1,)),
            dma((2,)),
            dma((1,)),
            dma((chunks, 5, 2)),
            dma((2,)),
            dma((4,)),
            dma((4,)),
            dma((per_core, nz)),
            dma((3,)),
            dma((per_core, 4)),
            dma((2,)),
        ],
        compiler_params=pltpu.CompilerParams(
            collective_id=1, has_side_effects=True, vmem_limit_bytes=63 * 1024 * 1024
        ),
    )(
        tokens,
        norm_gain,
        w_query,
        w_key,
        w_value,
        q_bias,
        k_bias[None, :],
        v_bias[None, :],
        w_out.T,
        base_cos,
        base_sin,
    )


def by_mesh(tokens, norm_gain, w_query, w_key, *rest):
    blocks, heads = lax.axis_size("blk"), lax.axis_size("head")
    groups = w_key.shape[1] // HD
    fits = blocks == 16 and heads == 2 and groups == 4 and w_query.shape[1] == 2 * G * HD
    run = in_planes if fits else on_device
    return run(tokens, norm_gain, w_query, w_key, *rest)


def solution(mesh):
    placed = (
        P(("blk", "head"), None),
        P(),
        P("blk", "head"),
        P("blk", None),
        P("blk", None),
        P("head"),
        P(),
        P(),
        P("head", "blk"),
    )
    return jax.shard_map(
        by_mesh, mesh=mesh, in_specs=placed, out_specs=P(("blk", "head"), None), check_vma=False
    )
```

```python
import functools
import math

import jax
import jax.numpy as jnp
import numpy as np
from jax import lax
from jax.experimental import pallas as pl
from jax.experimental.pallas import tpu as pltpu
from jax.sharding import PartitionSpec as P

HD = 128
G = 6
MESH = pl.DeviceIdType.MESH

theta_base = 1000000.0
eps_norm = 1e-06
masked_score = -1e30

WQ, WKV, WO, KV, WQ_TAIL, WO_TAIL = range(6)
UP, DOWN, ACROSS, CORE = range(4)


def block_width(rows, limit):
    width = min(rows, limit)
    while rows % width:
        width -= 1
    return width


def kernel(
    sizes,
    tokens_ref,
    gain_ref,
    w_query_ref,
    w_key_ref,
    w_value_ref,
    q_bias_ref,
    k_bias_ref,
    v_bias_ref,
    w_out_ref,
    cos_ref,
    sin_ref,
    out_ref,
    wq,
    wkv,
    wo,
    kv,
    normed,
    query,
    attended,
    partial,
    outgoing,
    incoming,
    local_sem,
    send_sem,
    recv_sem,
    norm_send,
    norm_recv,
    sum_send,
    sum_recv,
):
    blocks, heads = sizes
    nz = blocks // 4
    me = lax.axis_index("blk")
    head = lax.axis_index("head")
    z, y, c = me // 4, (me // 2) % 2, me % 2
    local_rows, width = tokens_ref.shape
    group_rows = local_rows * heads
    heads_here = wq.shape[1] // HD
    kv_here = wkv.shape[1] // (2 * HD)
    per_kv = heads_here // kv_here
    kv_cols = kv_here * HD
    kv_start = pl.multiple_of((head * heads_here // G) * HD, HD)
    buffers = {WQ: wq, WKV: wkv, WO: wo, KV: kv, WQ_TAIL: wq, WO_TAIL: wo}
    queries, outs = (WQ, WQ_TAIL), (WO, WO_TAIL)
    scale = 1.0 / math.sqrt(HD)

    def slot_of(zz, yy, cc):
        return (zz * 2 + yy) * 2 + cc

    def rows_of(item, slot):
        each = buffers[item].shape[0] // blocks
        first, size = 0, each
        if item in queries + outs:
            cut = each // 2 // 16 * 16
            first, size = (0, cut) if item in (WQ, WO) else (cut, each - cut)
        return buffers[item].at[pl.ds(pl.multiple_of(slot * each + first, 16), size)]

    def whole_rows(ref):
        each = ref.shape[0] // blocks
        return ref.at[pl.ds(pl.multiple_of(me * each, each), each)]

    def target(route):
        step = {UP: 4, DOWN: -4, ACROSS: 2 - 4 * y, CORE: 1 - 2 * c}[route]
        return (me + step, head)

    def copy(item, slot, route):
        part = rows_of(item, slot)
        return pltpu.make_async_remote_copy(
            src_ref=part,
            dst_ref=part,
            send_sem=send_sem.at[item, slot, route],
            recv_sem=recv_sem.at[item, slot],
            device_id=target(route),
            device_id_type=MESH,
        )

    def send(item, slot, route):
        if route == UP:
            pl.when(z < nz - 1)(lambda: copy(item, slot, route).start())
        elif route == DOWN:
            pl.when(z > 0)(lambda: copy(item, slot, route).start())
        else:
            copy(item, slot, route).start()

    def sent(item, slot, route):
        if route == UP:
            pl.when(z < nz - 1)(lambda: copy(item, slot, route).wait_send())
        elif route == DOWN:
            pl.when(z > 0)(lambda: copy(item, slot, route).wait_send())
        else:
            copy(item, slot, route).wait_send()

    def arrived(item, slot):
        copy(item, slot, CORE).wait_recv()

    def below(k, act):
        pl.when(z >= k)(lambda: act(z - k))

    def above(k, act):
        pl.when(z + k < nz)(lambda: act(z + k))

    def z_step(item, k, yy, then=()):
        def from_below(zz):
            slot = slot_of(zz, yy, c)
            arrived(item, slot)
            for route in (UP,) + then:
                send(item, slot, route)

        def from_above(zz):
            slot = slot_of(zz, yy, c)
            arrived(item, slot)
            for route in (DOWN,) + then:
                send(item, slot, route)

        below(k, from_below)
        above(k, from_above)

    def at_distance(k, act):
        if k == 0:
            act(z)
        else:
            below(k, act)
            above(k, act)

    def across(item, k):
        def act(zz):
            slot = slot_of(zz, 1 - y, c)
            arrived(item, slot)
            send(item, slot, CORE)

        at_distance(k, act)

    def finish(item):
        for zz in range(nz):
            for yy in range(2):
                arrived(item, slot_of(zz, yy, 1 - c))

    def drain(item, both):
        for yy in (y, 1 - y) if both else (y,):
            for route in (UP, DOWN):
                sent(item, slot_of(z, yy, c), route)
            for k in range(1, nz):
                below(k, lambda zz, yy=yy: sent(item, slot_of(zz, yy, c), UP))
                above(k, lambda zz, yy=yy: sent(item, slot_of(zz, yy, c), DOWN))
        if both:
            sent(item, me, ACROSS)
        for zz in range(nz):
            if not both:
                sent(item, slot_of(zz, y, c), ACROSS)
            for yy in range(2):
                sent(item, slot_of(zz, yy, c), CORE)

    own = [
        pltpu.make_async_copy(w_query_ref, whole_rows(wq), local_sem.at[0]),
        pltpu.make_async_copy(
            w_key_ref.at[:, pl.ds(kv_start, kv_cols)],
            rows_of(WKV, me).at[:, pl.ds(0, kv_cols)],
            local_sem.at[1],
        ),
        pltpu.make_async_copy(
            w_value_ref.at[:, pl.ds(kv_start, kv_cols)],
            rows_of(WKV, me).at[:, pl.ds(kv_cols, kv_cols)],
            local_sem.at[2],
        ),
        pltpu.make_async_copy(w_out_ref, whole_rows(wo), local_sem.at[3]),
    ]
    for one in own:
        one.start()

    barrier = pltpu.get_barrier_semaphore()

    def greet(blk, hd):
        pl.semaphore_signal(barrier, inc=1, device_id=(blk, hd), device_id_type=MESH)

    pl.when(z < nz - 1)(lambda: greet(me + 4, head))
    pl.when(z > 0)(lambda: greet(me - 4, head))
    greet(target(ACROSS)[0], head)
    greet(target(CORE)[0], head)
    peers = [lax.rem(head + d, heads) for d in range(1, heads)]
    for peer in peers:
        greet(me, peer)
    ends = jnp.where(z < nz - 1, 1, 0) + jnp.where(z > 0, 1, 0)
    pl.semaphore_wait(barrier, ends + 2 + len(peers))

    own[1].wait()
    own[2].wait()
    for route in (ACROSS, UP, DOWN, CORE):
        send(WKV, me, route)
    own[0].wait()
    own[3].wait()
    for item in queries + outs:
        for route in (ACROSS, CORE):
            send(item, me, route)

    my_rows = pl.ds(pl.multiple_of(head * local_rows, local_rows), local_rows)
    floats = tokens_ref[...].astype(jnp.float32)
    normed[my_rows, :] = (
        floats
        * lax.rsqrt(jnp.mean(floats * floats, axis=1, keepdims=True) + eps_norm)
        * gain_ref[...]
    ).astype(jnp.bfloat16)

    there = slot_of(z, 1 - y, c)
    arrived(WKV, there)
    for route in (UP, DOWN, CORE):
        send(WKV, there, route)

    def norm_copy(d):
        return pltpu.make_async_remote_copy(
            src_ref=normed.at[my_rows],
            dst_ref=normed.at[my_rows],
            send_sem=norm_send.at[d],
            recv_sem=norm_recv.at[d],
            device_id=(me, peers[d]),
            device_id_type=MESH,
        )

    for d in range(len(peers)):
        norm_copy(d).start()

    for k in range(1, nz):
        z_step(WKV, k, y, (CORE,))
        z_step(WKV, k, 1 - y, (CORE,))
        if k == max(1, nz - 2):
            for item in queries:
                for route in (UP, DOWN):
                    send(item, me, route)
    for d in range(len(peers)):
        norm_copy(d).wait_recv()
    finish(WKV)

    cosine, sine = cos_ref[...], sin_ref[...]

    def turn(values):
        return values * cosine + pltpu.roll(values, HD // 2, 1) * sine

    kv_rows = pl.ds(pl.multiple_of(me * group_rows, group_rows), group_rows)
    sums = jnp.dot(normed[...], wkv[...], preferred_element_type=jnp.float32)
    for g in range(kv_here):
        bias = k_bias_ref[:, pl.ds(pl.multiple_of(kv_start + g * HD, HD), HD)]
        kv[kv_rows, pl.ds(g * HD, HD)] = turn(sums[:, g * HD : (g + 1) * HD] + bias).astype(
            jnp.bfloat16
        )
        bias = v_bias_ref[:, pl.ds(pl.multiple_of(kv_start + g * HD, HD), HD)]
        at = kv_cols + g * HD
        kv[kv_rows, pl.ds(at, HD)] = (sums[:, at : at + HD] + bias).astype(jnp.bfloat16)

    for item in queries:
        across(item, 0)
    for route in (UP, DOWN, ACROSS, CORE):
        send(KV, me, route)

    for k in range(1, nz):
        for item in queries:
            z_step(item, k, y, (ACROSS, CORE))
        z_step(KV, k, y, (ACROSS, CORE))
        if k == max(1, nz - 2):
            for item in outs:
                for route in (UP, DOWN):
                    send(item, me, route)
    for k in range(1, nz):
        if k == nz - 1:
            for item in outs:
                z_step(item, 1, y, (ACROSS, CORE))
        for item in queries:
            across(item, k)
    for k in range(nz):
        across(KV, k)
    for item in queries + (KV,):
        finish(item)

    joined = 2 if heads_here % 2 == 0 else 1

    def project(n, carry):
        cols = pl.ds(pl.multiple_of(n * joined * HD, joined * HD), joined * HD)
        total = jnp.dot(normed[...], wq[:, cols], preferred_element_type=jnp.float32)
        total = total + q_bias_ref[:, cols]
        for j in range(joined):
            query[n * joined + j] = turn(total[:, j * HD : (j + 1) * HD]).astype(jnp.bfloat16)
        return carry

    lax.fori_loop(0, heads_here // joined, project, 0)

    if nz > 2:
        for item in outs:
            z_step(item, 2, y, (ACROSS, CORE))

    keys = kv.shape[0]
    span = block_width(keys, 512)
    stacked = per_kv * group_rows
    last_query = me * group_rows + group_rows - 1
    steps = last_query // span + 1

    for g in range(kv_here):
        q = query[g * per_kv : (g + 1) * per_kv].reshape(stacked, HD)

        def attend(j, state, q=q, g=g):
            top, total, acc = state
            at = pl.ds(pl.multiple_of(j * span, span), span)
            scores = (
                lax.dot_general(
                    q,
                    kv[at, pl.ds(g * HD, HD)],
                    (((1,), (1,)), ((), ())),
                    preferred_element_type=jnp.float32,
                )
                * scale
            )
            shape = (per_kv, group_rows, span)
            rows = lax.broadcasted_iota(jnp.int32, shape, 1).reshape(stacked, span)
            columns = lax.broadcasted_iota(jnp.int32, (stacked, span), 1)
            visible = columns + j * span <= rows + me * group_rows
            scores = jnp.where(visible, scores, masked_score)
            new_top = jnp.maximum(top, jnp.max(scores, axis=1, keepdims=True))
            weights = jnp.where(visible, jnp.exp(scores - new_top), 0.0)
            fade = jnp.exp(top - new_top)
            total = total * fade + jnp.sum(weights, axis=1, keepdims=True)
            acc = acc * fade + jnp.dot(
                weights.astype(jnp.bfloat16),
                kv[at, pl.ds(kv_cols + g * HD, HD)],
                preferred_element_type=jnp.float32,
            )
            return (new_top, total, acc)

        start = (
            jnp.full((stacked, 1), masked_score, jnp.float32),
            jnp.zeros((stacked, 1), jnp.float32),
            jnp.zeros((stacked, HD), jnp.float32),
        )
        top, total, acc = lax.fori_loop(0, steps, attend, start)
        result = (acc / total).astype(jnp.bfloat16)
        for r in range(per_kv):
            attended[:, pl.ds((g * per_kv + r) * HD, HD)] = result[
                r * group_rows : (r + 1) * group_rows
            ]
        for k in range(3, nz):
            if g == 0:
                z_step(WO, k, y, (ACROSS, CORE))
    for k in range(3, nz):
        z_step(WO_TAIL, k, y, (ACROSS, CORE))

    each = wo.shape[0] // blocks
    grouped = (4 * each) % HD == 0
    groups = nz if grouped else 1
    chunk = width // groups

    def sum_copy(d, i, start):
        rows = pl.ds(pl.multiple_of(peers[d] * local_rows, local_rows), local_rows)
        cols = pl.ds(pl.multiple_of(start, HD), chunk)
        return pltpu.make_async_remote_copy(
            src_ref=outgoing.at[rows, cols],
            dst_ref=incoming.at[d, :, cols],
            send_sem=sum_send.at[d, i],
            recv_sem=sum_recv.at[d, i],
            device_id=(me, peers[d]),
            device_id_type=MESH,
        )

    def produce(start, size):
        cols = pl.ds(pl.multiple_of(start, HD), size)
        result = lax.dot_general(
            attended[...],
            wo[cols, :],
            (((1,), (1,)), ((), ())),
            preferred_element_type=jnp.float32,
        )
        partial[:, cols] = result
        outgoing[:, cols] = result.astype(jnp.bfloat16)

    def place(i):
        way = 1 - 2 * (z // max(1, nz // 2)) if nz > 1 else 1
        return lax.rem(z + way * i + nz, nz)

    if grouped:

        def produce_group(i, carry):
            zz = place(i)
            slot = slot_of(zz, 1 - y, c)
            for item in outs:
                arrived(item, slot)
                send(item, slot, CORE)
            for item in outs:
                for yy in range(2):
                    arrived(item, slot_of(zz, yy, 1 - c))
            produce(zz * 4 * each, chunk)
            for d in range(len(peers)):
                sum_copy(d, i, zz * chunk).start()
            return carry

        lax.fori_loop(0, nz, produce_group, 0)
    else:
        for item in outs:
            for k in range(nz):
                across(item, k)
            finish(item)
        part = 256
        lax.fori_loop(0, width // part, lambda n, carry: (produce(n * part, part), carry)[1], 0)
        for d in range(len(peers)):
            sum_copy(d, 0, 0).start()

    for item in queries + outs + (WKV, KV):
        drain(item, item == WKV)
    for d in range(len(peers)):
        norm_copy(d).wait_send()

    def collect(i, carry):
        start = place(i) * chunk if grouped else 0
        cols = pl.ds(pl.multiple_of(start, HD), chunk)
        for d in range(len(peers)):
            sum_copy(d, i, start).wait_recv()
        result = partial[my_rows, cols]
        for d in range(len(peers)):
            result = result + incoming[d, :, cols].astype(jnp.float32)
        out_ref[:, cols] = result.astype(jnp.bfloat16)
        for d in range(len(peers)):
            sum_copy(d, i, start).wait_send()
        return carry

    lax.fori_loop(0, groups, collect, 0)


def on_device(tokens, norm_gain, w_query, w_key, w_value, q_bias, k_bias, v_bias, w_out):
    blocks, heads = lax.axis_size("blk"), lax.axis_size("head")
    local_rows, width = tokens.shape
    group_rows = local_rows * heads
    heads_here = w_query.shape[1] // HD
    kv_here = max(1, heads_here // G)
    positions = lax.axis_index("blk") * group_rows + jnp.arange(group_rows, dtype=jnp.int32)
    half = HD // 2
    freq = theta_base ** (-(jnp.arange(half, dtype=jnp.float32) * 2.0 / HD))
    angles = positions.astype(jnp.float32)[:, None] * freq[None, :]
    cosine, sine = jnp.cos(angles), jnp.sin(angles)
    cosine = jnp.concatenate([cosine, cosine], axis=1)
    sine = jnp.concatenate([-sine, sine], axis=1)
    inner = heads_here * HD
    vmem = pl.BlockSpec(memory_space=pltpu.VMEM)
    hbm = pl.BlockSpec(memory_space=pl.ANY)
    others = max(1, heads - 1)
    bf16, f32 = jnp.bfloat16, jnp.float32
    return pl.pallas_call(
        functools.partial(kernel, (blocks, heads)),
        out_shape=jax.ShapeDtypeStruct((local_rows, width), bf16),
        in_specs=[vmem, vmem, hbm, hbm, hbm, vmem, vmem, vmem, hbm, vmem, vmem],
        out_specs=vmem,
        scratch_shapes=[
            pltpu.VMEM((width, inner), bf16),
            pltpu.VMEM((width, 2 * kv_here * HD), bf16),
            pltpu.VMEM((width, inner), bf16),
            pltpu.VMEM((blocks * group_rows, 2 * kv_here * HD), bf16),
            pltpu.VMEM((group_rows, width), bf16),
            pltpu.VMEM((heads_here, group_rows, HD), bf16),
            pltpu.VMEM((group_rows, inner), bf16),
            pltpu.VMEM((group_rows, width), f32),
            pltpu.VMEM((group_rows, width), bf16),
            pltpu.VMEM((others, local_rows, width), bf16),
            pltpu.SemaphoreType.DMA((4,)),
            pltpu.SemaphoreType.DMA((6, blocks, 4)),
            pltpu.SemaphoreType.DMA((6, blocks)),
            pltpu.SemaphoreType.DMA((others,)),
            pltpu.SemaphoreType.DMA((others,)),
            pltpu.SemaphoreType.DMA((others, blocks // 4)),
            pltpu.SemaphoreType.DMA((others, blocks // 4)),
        ],
        compiler_params=pltpu.CompilerParams(
            collective_id=0, has_side_effects=True, vmem_limit_bytes=60 * 1024 * 1024
        ),
    )(
        tokens,
        norm_gain[None, :],
        w_query,
        w_key,
        w_value,
        q_bias[None, :],
        k_bias[None, :],
        v_bias[None, :],
        w_out.T,
        cosine,
        sine,
    )


def plane_kernel(
    nz,
    tokens_ref,
    gain_ref,
    w_query_ref,
    w_key_ref,
    w_value_ref,
    q_bias_ref,
    k_bias_ref,
    v_bias_ref,
    w_out_ref,
    base_cos_ref,
    base_sin_ref,
    out_ref,
    tokens,
    base_cos,
    base_sin,
    gain,
    q_flat,
    k_bias,
    v_bias,
    cosine,
    sine,
    stage,
    w,
    normed,
    xs,
    part_out,
    part_in,
    full,
    biases,
    kv,
    hidden,
    att,
    att_other,
    wo,
    acc,
    outs,
    result,
    small_sem,
    load_sem,
    wo_load_sem,
    w_send,
    w_home,
    w_relay,
    w_rest,
    x_send,
    x_recv,
    b_sem,
    p_send,
    p_recv,
    kv_send,
    kv_recv,
    a_send,
    a_recv,
    wo_send,
    wo_recv,
    o_sem,
):
    f32, bf16 = jnp.float32, jnp.bfloat16
    me = lax.axis_index("blk")
    x = lax.axis_index("head")
    z, y, c = me // 4, (me // 2) % 2, me % 2
    rows, width = tokens_ref.shape
    each = w_query_ref.shape[0]
    depth = width // nz
    per_core = G // 2
    chunks = per_core + 1
    columns = width // nz
    zh = z // 2
    inner = ((z + 1) // 2) % 2 == 1
    outer = jnp.logical_not(inner)
    pair = z + 1 - 2 * (z % 2)
    near, far = 2 - zh, 3 - 3 * zh
    final_waits = []
    order = (0, nz - 1) + tuple(range(1, nz - 1))
    halves = 2
    span = nz // halves * 2 * rows

    def spot(zz):
        return jnp.where(((zz + 1) // 2) % 2 == 1, zz + 1, zz // 3)

    def dev(zz, yy, cc, xx):
        return ((zz * 2 + yy) * 2 + cc, xx)

    core_peer = dev(z, y, 1 - c, x)
    x_peer = dev(z, y, c, 1 - x)
    y_peer = dev(z, 1 - y, c, x)
    diagonal = dev(z, 1 - y, c, 1 - x)

    def go(src, dst, ssem, rsem, to, when=None):
        one = pltpu.make_async_remote_copy(
            src_ref=src, dst_ref=dst, send_sem=ssem, recv_sem=rsem, device_id=to, device_id_type=MESH
        )
        if when is None:
            one.start()
        else:
            pl.when(when)(one.start)

    def got(like, rsem):
        pltpu.make_async_remote_copy(
            src_ref=like, dst_ref=like, send_sem=b_sem.at[0], recv_sem=rsem, device_id=x_peer, device_id_type=MESH
        ).wait_recv()

    def at_end(like, ssem, when=None):
        one = pltpu.make_async_remote_copy(
            src_ref=like, dst_ref=like, send_sem=ssem, recv_sem=b_sem.at[1], device_id=x_peer, device_id_type=MESH
        )
        if when is None:
            final_waits.append(one.wait_send)
        else:
            final_waits.append(lambda: pl.when(when)(one.wait_send))

    small = [
        pltpu.make_async_copy(tokens_ref, tokens, small_sem.at[0]),
        pltpu.make_async_copy(gain_ref, gain, small_sem.at[1]),
        pltpu.make_async_copy(q_bias_ref, q_flat, small_sem.at[2]),
        pltpu.make_async_copy(k_bias_ref, k_bias, small_sem.at[3]),
        pltpu.make_async_copy(v_bias_ref, v_bias, small_sem.at[4]),
        pltpu.make_async_copy(base_cos_ref, base_cos, small_sem.at[5]),
        pltpu.make_async_copy(base_sin_ref, base_sin, small_sem.at[6]),
    ]
    for one in small:
        one.start()

    barrier = pltpu.get_barrier_semaphore()
    friends = [core_peer, x_peer, y_peer, diagonal]
    for d in range(1, nz):
        for f in range(2):
            friends.append(dev((z + d) % nz, y, (c + f) % 2, x))
    for friend in friends:
        pl.semaphore_signal(barrier, inc=1, device_id=friend, device_id_type=MESH)

    mine = y * 2 + c

    def block(xx, j, s):
        return w.at[
            j,
            pl.ds(pl.multiple_of(s * each, 16), each),
            pl.ds(pl.multiple_of(xx * 2 * HD, HD), 2 * HD),
        ]

    def blocks_like(n):
        return w.at[0, pl.ds(0, n * each), pl.ds(0, 2 * HD)]

    def load(f, j):
        place = stage.at[j] if f else block(x, j, mine)
        cc = (c + f) % 2
        sem = load_sem.at[j]
        if j == 0:
            at = pl.ds(pl.multiple_of(2 * x * HD, HD), 2 * HD)
            pl.when(cc == 0)(pltpu.make_async_copy(w_key_ref.at[:, at], place, sem).start)
            pl.when(cc == 1)(pltpu.make_async_copy(w_value_ref.at[:, at], place, sem).start)
        else:
            for gl in range(2):
                at = pl.ds(pl.multiple_of((gl * G + cc * per_core + j - 1) * HD, HD), HD)
                pltpu.make_async_copy(
                    w_query_ref.at[:, at], place.at[:, pl.ds(gl * HD, HD)], sem
                ).start()

    def loaded(j):
        pltpu.make_async_copy(blocks_like(2), blocks_like(2), load_sem.at[j]).wait()

    for j in range(chunks):
        for f in range(2):
            load(f, j)

    wo_cols = 2 * 2 * HD
    half_rows = each // 2

    def wo_block(h, xx, s, half):
        first = pl.multiple_of(s * each + half * half_rows, 16)
        return wo.at[h, pl.ds(first, half_rows), pl.ds(pl.multiple_of(xx * wo_cols, HD), wo_cols)]

    def wo_like(n):
        return wo.at[0, pl.ds(0, n * half_rows), pl.ds(0, wo_cols)]

    for h in range(per_core):
        for gl in range(2):
            for cc in range(2):
                zz = 2 * x + gl
                pltpu.make_async_copy(
                    w_out_ref.at[:, pl.ds((gl * G + cc * per_core + h) * HD, HD)],
                    wo.at[
                        h,
                        pl.ds(pl.multiple_of((y * 2 + c) * each, 16), each),
                        pl.ds(pl.multiple_of((zz * 2 + cc) * HD, HD), HD),
                    ],
                    wo_load_sem.at[h],
                ).start()

    small[0].wait()
    small[1].wait()
    floats = tokens[...].astype(f32)
    values = (
        floats
        * lax.rsqrt(jnp.mean(floats * floats, axis=1, keepdims=True) + eps_norm)
        * gain[...].reshape(1, width)
    ).astype(bf16)
    for n in range(nz):
        normed[n] = values[:, n * depth : (n + 1) * depth]
    at_me = pl.ds(pl.multiple_of((spot(z) * 2 + c) * rows, rows), rows)
    xs[at_me, :] = normed[z]
    small[2].wait()
    flat = q_flat[...]
    for n in range(q_flat.shape[0] // HD):
        biases[x, n] = flat[n * HD : (n + 1) * HD].reshape(1, HD)
    small[3].wait()
    small[4].wait()
    small[5].wait()
    small[6].wait()

    pl.semaphore_wait(barrier, len(friends))

    def home_send(j, s, cc):
        here = block(x, j, s)
        for to, ssem, relayed in ((x_peer, w_send.at[0], cc == 1), (y_peer, w_send.at[1], cc == 0)):
            go(here, here, ssem, w_relay.at[j, 1 if to is x_peer else 0], to, relayed)
            go(here, here, ssem, w_rest.at[j], to, jnp.logical_not(relayed))

    def own_block(j):
        loaded(j)
        go(stage.at[j], block(x, j, mine), w_send.at[2], w_home.at[j], core_peer)
        home_send(j, mine, c)

    def home(j):
        got(blocks_like(1), w_home.at[j])
        home_send(j, y * 2 + 1 - c, 1 - c)

    def relay_weights(j, k):
        def from_y():
            got(blocks_like(1), w_relay.at[j, 0])
            here = block(x, j, (1 - y) * 2)
            go(here, here, w_send.at[0], w_rest.at[j], x_peer)

        def from_x():
            got(blocks_like(1), w_relay.at[j, 1])
            here = block(1 - x, j, y * 2 + 1)
            go(here, here, w_send.at[1], w_rest.at[j], y_peer)

        pl.when(c == k)(from_y)
        pl.when(c != k)(from_x)

    at_end(w.at[pl.ds(0, 3), :, pl.ds(0, 2 * HD)], w_send.at[0])
    at_end(w.at[pl.ds(0, 3), :, pl.ds(0, 2 * HD)], w_send.at[1])
    at_end(blocks_like(chunks), w_send.at[2])

    def token_block(zz, cc):
        return xs.at[pl.ds(pl.multiple_of((spot(zz) * 2 + cc) * rows, rows), rows)]

    def tokens_like(n):
        return xs.at[pl.ds(0, n * rows)]

    def send_tokens():
        for to in (far, near, pair):
            go(normed.at[to], token_block(z, c), x_send.at[0], x_recv.at[z], dev(to, y, c, x))
        go(normed.at[z], token_block(z, c), x_send.at[1], x_recv.at[nz], core_peer)

    def pass_tokens(zz):
        here = token_block(zz, c)
        got(here, x_recv.at[zz])
        go(here, here, x_send.at[1], x_recv.at[nz], core_peer)

    def wait_tokens():
        got(tokens_like(nz), x_recv.at[nz])

    at_end(tokens_like(nz - 1), x_send.at[0])
    at_end(tokens_like(nz), x_send.at[1])

    def send_biases():
        go(biases.at[x], biases.at[x], b_sem.at[0], b_sem.at[1], x_peer)

    def shard(s):
        return pl.ds(pl.multiple_of(s * HD, HD), HD)

    def half_at(n):
        return pl.ds(n * span, span)

    def part_go(j, n, k, to, there):
        go(
            part_out.at[j, k, half_at(n)],
            part_in.at[j, there, half_at(n)],
            p_send.at[0],
            p_recv.at[j, there, n],
            dev(to, y, c, x),
        )

    def part_got(j, n, k):
        got(part_in.at[j, k, half_at(n)], p_recv.at[j, k, n])

    def multiply(j):
        got(blocks_like(4), w_rest.at[j])
        full[j] = jnp.dot(xs[...], w[j], preferred_element_type=f32)

        def send():
            for n in range(halves):
                for k, s in enumerate((far, near, pair)):
                    part_out[j, k, half_at(n)] = full[j, half_at(n), shard(s)].astype(bf16)
                    part_go(j, n, k, pair, k)

        pl.when(outer)(send)

    def chain(j, n, steps):
        def act():
            for k, s, source, to, there in steps:
                part_got(j, n, source)
                part_out[j, k, half_at(n)] = (
                    full[j, half_at(n), shard(s)] + part_in[j, source, half_at(n)].astype(f32)
                ).astype(bf16)
                part_go(j, n, k, to, there)

        pl.when(inner)(act)

    def inward(j, n):
        chain(j, n, ((0, far, 0, near, 3), (1, near, 1, near, 4)))

    def outward(j, n):
        chain(j, n, ((2, pair, 3, pair, 2),))

    def summed(j, n):
        def more():
            part_got(j, n, 4)
            full[j, half_at(n), shard(z)] = (
                full[j, half_at(n), shard(z)] + part_in[j, 4, half_at(n)].astype(f32)
            )

        pl.when(inner)(more)
        part_got(j, n, 2)
        return full[j, half_at(n), shard(z)] + part_in[j, 2, half_at(n)].astype(f32)

    at_end(part_out, p_send.at[0])

    def turn(values, n):
        return values * cosine[half_at(n)] + pltpu.roll(values, HD // 2, 1) * sine[half_at(n)]

    here_src = y * 2 + x
    others = [(1 - y) * 2 + x, y * 2 + 1 - x, (1 - y) * 2 + 1 - x]

    def make_tables():
        signs = jnp.where(lax.broadcasted_iota(jnp.int32, (1, HD), 1) < HD // 2, -1.0, 1.0)
        starts = base_cos.shape[0] - rows
        cos_in, sin_in = base_cos[starts:], base_sin[starts:]
        for n in range(2 * nz):
            row = pl.ds((order[n // 2] * 4 + y * 2 + n % 2) * 2 + x, 1)
            cos_at, sin_at = base_cos[row], base_sin[row]
            cosine[n * rows : (n + 1) * rows] = cos_at * cos_in - sin_at * sin_in
            sine[n * rows : (n + 1) * rows] = (sin_at * cos_in + cos_at * sin_in) * signs
        at = lax.broadcasted_iota(jnp.int32, (2 * rows, 8 * rows), 1)
        within = at % (2 * rows)
        key_at = (
            (at // (4 * rows)) * 4 + (within // rows) * 2 + (at // (2 * rows)) % 2
        ) * rows + within % rows
        at = lax.broadcasted_iota(jnp.int32, (2 * rows, 8 * rows), 0)
        query_at = (y * 4 + (at // rows) * 2 + x) * rows + at % rows
        hidden[...] = jnp.where(key_at <= query_at, 0.0, masked_score)

    def kv_half(kind, s, n):
        return kv.at[kind, s, half_at(n)]

    def make_kv(n):
        at_group = pl.ds(pl.multiple_of(z * HD, HD), HD)
        total = summed(0, n)
        kv[c, here_src, half_at(n)] = jnp.where(
            c == 0, turn(total + k_bias[:, at_group], n), total + v_bias[:, at_group]
        ).astype(bf16)
        here = kv_half(c, here_src, n)
        go(here, here, kv_send.at[0], kv_recv.at[n], x_peer)
        go(here, here, kv_send.at[0], kv_recv.at[2 + n], y_peer)
        go(here, here, kv_send.at[0], kv_recv.at[4 + n], diagonal)
        go(here, here, kv_send.at[1], kv_recv.at[6], core_peer)

    def kv_pass(n):
        for k, s in ((0, others[1]), (2, others[0]), (4, others[2])):
            here = kv_half(c, s, n)
            got(here, kv_recv.at[k + n])
            go(here, here, kv_send.at[1], kv_recv.at[6], core_peer)

    def kv_peer():
        got(kv.at[0], kv_recv.at[6])
        got(biases.at[1 - x], b_sem.at[1])

    at_end(kv.at[0, pl.ds(0, 3)], kv_send.at[0])
    at_end(kv.at[0], kv_send.at[1])
    at_end(biases.at[0], b_sem.at[0])

    factor = math.log2(math.e) / math.sqrt(HD)

    att_rows = nz // halves * rows

    def att_piece(h, n, zz, cc):
        return att.at[
            h,
            pl.ds(n * att_rows, att_rows),
            pl.ds(pl.multiple_of((zz * 2 + cc) * HD, HD), HD),
        ]

    def att_like(count):
        return att.at[0, pl.ds(0, att_rows), pl.ds(0, count * HD)]

    def attend(h, n):
        total = summed(h + 1, n) + biases[zh, (z % 2) * G + c * per_core + h]
        query = turn(total, n).astype(bf16)
        cols_of_me = pl.ds(pl.multiple_of((z * 2 + c) * HD, HD), HD)
        for k in range(nz // halves):
            t = order[n * (nz // halves) + k]
            q = query[k * 2 * rows : (k + 1) * 2 * rows]
            tiles = [pl.ds(order.index(u) * 2 * rows, 2 * rows) for u in range(t + 1)]
            scores = []
            for tile in tiles:
                keys = kv[0, :, tile].reshape(8 * rows, HD)
                scores.append(
                    lax.dot_general(
                        q, keys, (((1,), (1,)), ((), ())), preferred_element_type=f32
                    )
                )
            scores[t] = scores[t] + hidden[...]
            top = jnp.max(functools.reduce(jnp.maximum, scores), axis=1, keepdims=True)
            mixed, sums = None, None
            for tile, one in zip(tiles, scores):
                weights = jnp.exp2((one - top) * factor)
                sums = weights if sums is None else sums + weights
                vals = kv[1, :, tile].reshape(8 * rows, HD)
                one = jnp.dot(weights.astype(bf16), vals, preferred_element_type=f32)
                mixed = one if mixed is None else mixed + one
            mixed = (mixed / jnp.sum(sums, axis=1, keepdims=True)).astype(bf16)
            low, high = mixed[:rows], mixed[rows:]
            at = pl.ds(n * att_rows + k * rows, rows)
            att[h, at, cols_of_me] = jnp.where(c == 0, low, high)
            att_other[h, at, :] = jnp.where(c == 0, high, low)
        here, there = att_piece(h, n, z, c), att_other.at[h, pl.ds(n * att_rows, att_rows)]
        rsem = a_recv.at[h, n, z]
        direct = (h, n) == (per_core - 1, halves - 1)

        def att_go(k, to, when=None):
            go(here, here, a_send.at[k], rsem, dev(to, y, c, x), when)
            go(there, here, a_send.at[k], rsem, dev(to, y, 1 - c, x), when)

        if direct:
            att_go(4, far)
            att_go(4, near)
        else:
            att_go(0, near, inner)
        att_go(1, pair)
        go(there, here, a_send.at[2], rsem, core_peer)

    def relay_attended(h, n, zz, to):
        def act():
            got(att_like(2), a_recv.at[h, n, zz])
            for cc in range(2):
                here = att_piece(h, n, zz, cc)
                go(here, here, a_send.at[3], a_recv.at[h, n, zz], dev(to, y, c, x))

        pl.when(inner)(act)

    def from_near(h, n):
        relay_attended(h, n, near, pair)

    def from_pair(h, n):
        relay_attended(h, n, pair, near)

    def from_far(h, n):
        relay_attended(h, n, far, pair)

    def gathered(h, n):
        def act():
            for zz in (pair, near, far):
                got(att_like(2), a_recv.at[h, n, zz])

        if (h, n) == (per_core - 1, halves - 1):
            act()
        else:
            pl.when(outer)(act)
        got(att_like(1), a_recv.at[h, n, z])

    steps = per_core * halves

    def att_sent(pieces):
        return att.at[pl.ds(0, 2), pl.ds(0, pieces * att_rows // (4 * nz)), :]

    at_end(att_sent(2 * (steps - 1)), a_send.at[0], inner)
    at_end(att_sent(4), a_send.at[4])
    at_end(att.at[:, :, pl.ds(0, 2 * HD)], a_send.at[1])
    at_end(att.at[:, :, pl.ds(0, HD)], a_send.at[2])
    at_end(att_sent(6 * (steps - 1)), a_send.at[3], inner)

    def wo_go(h, xx, s, half, n, rsem, to):
        here = wo_block(h, xx, s, half)
        go(here, here, wo_send.at[n], rsem, to)

    def wo_begin(h):
        like = wo.at[h, pl.ds(0, each), pl.ds(0, wo_cols)]
        pltpu.make_async_copy(like, like, wo_load_sem.at[h]).wait()
        for half in range(2):
            for n, to in enumerate((x_peer, y_peer, core_peer)):
                wo_go(h, x, y * 2 + c, half, n, wo_recv.at[h, n], to)

    def wo_relay(h):
        got(wo_like(2), wo_recv.at[h, 1])
        wo_go(h, x, (1 - y) * 2 + c, 0, 0, wo_recv.at[h, 3], x_peer)
        got(wo_like(2), wo_recv.at[h, 0])
        wo_go(h, 1 - x, y * 2 + c, 1, 1, wo_recv.at[h, 3], y_peer)
        for half in range(2):
            wo_go(h, x, (1 - y) * 2 + c, half, 2, wo_recv.at[h, 2], core_peer)
            wo_go(h, 1 - x, y * 2 + c, half, 2, wo_recv.at[h, 2], core_peer)

    def wo_finish(h):
        got(wo_like(2), wo_recv.at[h, 3])
        for half in range(2):
            wo_go(h, 1 - x, (1 - y) * 2 + c, half, 2, wo_recv.at[h, 2], core_peer)

    def wo_wait(h):
        got(wo_like(8), wo_recv.at[h, 2])

    at_end(wo.at[:, pl.ds(0, 3 * half_rows), pl.ds(0, wo_cols)], wo_send.at[0])
    at_end(wo.at[:, pl.ds(0, 3 * half_rows), pl.ds(0, wo_cols)], wo_send.at[1])
    at_end(wo.at[:, pl.ds(0, 8 * half_rows), pl.ds(0, wo_cols)], wo_send.at[2])

    def produce(h, n):
        gathered(h, n)
        at = slice(n * att_rows, (n + 1) * att_rows)
        for first in range(0, columns, 512):
            cols = slice(first, min(first + 512, columns))
            part = lax.dot_general(
                att[h, at], wo[h, cols, :], (((1,), (1,)), ((), ())), preferred_element_type=f32
            )
            if h:
                part = part + acc[at, cols]
            if h < per_core - 1:
                acc[at, cols] = part
            else:
                for k in range(nz // halves):
                    t = order[n * (nz // halves) + k]
                    outs[t, :, cols] = part[k * rows : (k + 1) * rows].astype(bf16)

    def result_cols(zz):
        return pl.ds(pl.multiple_of(zz * columns, HD), columns)

    def last(n):
        for k in range(nz // halves):
            t = order[n * (nz // halves) + k]
            go(
                outs.at[t],
                result.at[:, result_cols(z)],
                o_sem.at[0],
                o_sem.at[1],
                dev(t, y, c, x),
                z != t,
            )

    at_end(outs.at[pl.ds(0, nz - 1)], o_sem.at[0])

    send_tokens()
    own_block(0)
    send_biases()
    home(0)
    make_tables()
    relay_weights(0, 0)
    relay_weights(0, 1)
    own_block(1)
    home(1)
    pass_tokens(pair)
    pass_tokens(near)
    pass_tokens(far)
    wait_tokens()
    multiply(0)
    relay_weights(1, 0)
    relay_weights(1, 1)
    own_block(2)
    home(2)
    inward(0, 0)
    multiply(1)
    outward(0, 0)
    inward(0, 1)
    relay_weights(2, 0)
    relay_weights(2, 1)
    make_kv(0)
    outward(0, 1)
    make_kv(1)
    own_block(3)
    home(3)
    inward(1, 0)
    multiply(2)
    outward(1, 0)
    inward(1, 1)
    outward(1, 1)
    kv_pass(0)
    inward(2, 0)
    kv_pass(1)
    kv_peer()
    attend(0, 0)
    relay_weights(3, 0)
    relay_weights(3, 1)
    attend(0, 1)
    wo_begin(0)
    inward(2, 1)
    from_near(0, 0)
    outward(2, 0)
    from_near(0, 1)
    multiply(3)
    wo_begin(1)
    outward(2, 1)
    from_pair(0, 0)
    from_pair(0, 1)
    attend(1, 0)
    wo_relay(0)
    attend(1, 1)
    inward(3, 0)
    from_near(1, 0)
    from_far(0, 0)
    from_near(1, 1)
    wo_begin(2)
    outward(3, 0)
    inward(3, 1)
    from_far(0, 1)
    wo_relay(1)
    from_pair(1, 0)
    outward(3, 1)
    attend(2, 0)
    from_pair(1, 1)
    attend(2, 1)
    wo_finish(0)
    from_far(1, 0)
    from_near(2, 0)
    from_far(1, 1)
    wo_relay(2)
    from_pair(2, 0)
    wo_finish(1)
    wo_wait(0)
    produce(0, 0)
    produce(0, 1)
    from_far(2, 0)
    wo_finish(2)
    wo_wait(1)
    produce(1, 0)
    produce(1, 1)
    wo_wait(2)
    produce(2, 0)
    last(0)
    produce(2, 1)
    last(1)
    out_ref[:, result_cols(z)] = outs[z]
    for done in final_waits:
        done()
    got(outs.at[pl.ds(0, nz - 1)], o_sem.at[1])
    for d in range(1, nz):
        zz = (z + d) % nz
        out_ref[:, result_cols(zz)] = result[:, result_cols(zz)]


def in_planes(tokens, norm_gain, w_query, w_key, w_value, q_bias, k_bias, v_bias, w_out):
    blocks = lax.axis_size("blk")
    nz = blocks // 4
    rows, width = tokens.shape
    inner, each, per_core = w_query.shape[1], w_query.shape[0], G // 2
    chunks, held, columns = per_core + 1, 2 * nz * rows, width // nz
    positions = np.concatenate([np.arange(2 * blocks) * rows, np.arange(rows)])
    lanes = np.arange(HD) % (HD // 2)
    angles = positions[:, None] * theta_base ** (-2.0 * lanes / HD)[None, :]
    base_cos = jnp.asarray(np.cos(angles), jnp.float32)
    base_sin = jnp.asarray(np.sin(angles), jnp.float32)
    vmem = pl.BlockSpec(memory_space=pltpu.VMEM)
    hbm = pl.BlockSpec(memory_space=pltpu.HBM)
    bf16, f32 = jnp.bfloat16, jnp.float32
    dma = pltpu.SemaphoreType.DMA
    return pl.pallas_call(
        functools.partial(plane_kernel, nz),
        out_shape=jax.ShapeDtypeStruct((rows, width), bf16),
        in_specs=[hbm] * 11,
        out_specs=vmem,
        scratch_shapes=[
            pltpu.VMEM((rows, width), bf16),
            pltpu.VMEM(base_cos.shape, f32),
            pltpu.VMEM(base_sin.shape, f32),
            pltpu.VMEM((width,), f32),
            pltpu.VMEM((inner,), f32),
            pltpu.VMEM((1, w_key.shape[1]), f32),
            pltpu.VMEM((1, w_key.shape[1]), f32),
            pltpu.VMEM((held, HD), f32),
            pltpu.VMEM((held, HD), f32),
            pltpu.VMEM((chunks, each, 2 * HD), bf16),
            pltpu.VMEM((chunks, 4 * each, 4 * HD), bf16),
            pltpu.VMEM((nz, rows, width // nz), bf16),
            pltpu.VMEM((held, width // nz), bf16),
            pltpu.VMEM((chunks, 3, held, HD), bf16),
            pltpu.VMEM((chunks, 5, held, HD), bf16),
            pltpu.VMEM((chunks, held, 4 * HD), f32),
            pltpu.VMEM((2, inner // HD, 1, HD), f32),
            pltpu.VMEM((2, 4, held, HD), bf16),
            pltpu.VMEM((2 * rows, 8 * rows), f32),
            pltpu.VMEM((per_core, nz * rows, 2 * nz * HD), bf16),
            pltpu.VMEM((per_core, nz * rows, HD), bf16),
            pltpu.VMEM((per_core, columns, 2 * nz * HD), bf16),
            pltpu.VMEM((nz * rows, columns), f32),
            pltpu.VMEM((nz, rows, columns), bf16),
            pltpu.VMEM((rows, width), bf16),
            dma((7,)),
            dma((chunks,)),
            dma((per_core,)),
            dma((3,)),
            dma((chunks,)),
            dma((chunks, 2)),
            dma((chunks,)),
            dma((2,)),
            dma((nz + 1,)),
            dma((2,)),
            dma((1,)),
            dma((chunks, 5, 2)),
            dma((2,)),
            dma((7,)),
            dma((5,)),
            dma((per_core, 2, nz)),
            dma((3,)),
            dma((per_core, 4)),
            dma((2,)),
        ],
        compiler_params=pltpu.CompilerParams(
            collective_id=1, has_side_effects=True, vmem_limit_bytes=63 * 1024 * 1024
        ),
    )(
        tokens,
        norm_gain,
        w_query,
        w_key,
        w_value,
        q_bias,
        k_bias[None, :],
        v_bias[None, :],
        w_out.T,
        base_cos,
        base_sin,
    )


def by_mesh(tokens, norm_gain, w_query, w_key, *rest):
    blocks, heads = lax.axis_size("blk"), lax.axis_size("head")
    groups = w_key.shape[1] // HD
    fits = blocks == 16 and heads == 2 and groups == 4 and w_query.shape[1] == 2 * G * HD
    run = in_planes if fits else on_device
    return run(tokens, norm_gain, w_query, w_key, *rest)


def solution(mesh):
    placed = (
        P(("blk", "head"), None),
        P(),
        P("blk", "head"),
        P("blk", None),
        P("blk", None),
        P("head"),
        P(),
        P(),
        P("head", "blk"),
    )
    return jax.shard_map(
        by_mesh, mesh=mesh, in_specs=placed, out_specs=P(("blk", "head"), None), check_vma=False
    )
```

```python
import functools
import math

import jax
import jax.numpy as jnp
import numpy as np
from jax import lax
from jax.experimental import pallas as pl
from jax.experimental.pallas import tpu as pltpu
from jax.sharding import PartitionSpec as P

HD = 128
G = 6
MESH = pl.DeviceIdType.MESH

theta_base = 1000000.0
eps_norm = 1e-06
masked_score = -1e30

WQ, WKV, WO, KV, WQ_TAIL, WO_TAIL = range(6)
UP, DOWN, ACROSS, CORE = range(4)


def block_width(rows, limit):
    width = min(rows, limit)
    while rows % width:
        width -= 1
    return width


def kernel(
    sizes,
    tokens_ref,
    gain_ref,
    w_query_ref,
    w_key_ref,
    w_value_ref,
    q_bias_ref,
    k_bias_ref,
    v_bias_ref,
    w_out_ref,
    cos_ref,
    sin_ref,
    out_ref,
    wq,
    wkv,
    wo,
    kv,
    normed,
    query,
    attended,
    partial,
    outgoing,
    incoming,
    local_sem,
    send_sem,
    recv_sem,
    norm_send,
    norm_recv,
    sum_send,
    sum_recv,
):
    blocks, heads = sizes
    nz = blocks // 4
    me = lax.axis_index("blk")
    head = lax.axis_index("head")
    z, y, c = me // 4, (me // 2) % 2, me % 2
    local_rows, width = tokens_ref.shape
    group_rows = local_rows * heads
    heads_here = wq.shape[1] // HD
    kv_here = wkv.shape[1] // (2 * HD)
    per_kv = heads_here // kv_here
    kv_cols = kv_here * HD
    kv_start = pl.multiple_of((head * heads_here // G) * HD, HD)
    buffers = {WQ: wq, WKV: wkv, WO: wo, KV: kv, WQ_TAIL: wq, WO_TAIL: wo}
    queries, outs = (WQ, WQ_TAIL), (WO, WO_TAIL)
    scale = 1.0 / math.sqrt(HD)

    def slot_of(zz, yy, cc):
        return (zz * 2 + yy) * 2 + cc

    def rows_of(item, slot):
        each = buffers[item].shape[0] // blocks
        first, size = 0, each
        if item in queries + outs:
            cut = each // 2 // 16 * 16
            first, size = (0, cut) if item in (WQ, WO) else (cut, each - cut)
        return buffers[item].at[pl.ds(pl.multiple_of(slot * each + first, 16), size)]

    def whole_rows(ref):
        each = ref.shape[0] // blocks
        return ref.at[pl.ds(pl.multiple_of(me * each, each), each)]

    def target(route):
        step = {UP: 4, DOWN: -4, ACROSS: 2 - 4 * y, CORE: 1 - 2 * c}[route]
        return (me + step, head)

    def copy(item, slot, route):
        part = rows_of(item, slot)
        return pltpu.make_async_remote_copy(
            src_ref=part,
            dst_ref=part,
            send_sem=send_sem.at[item, slot, route],
            recv_sem=recv_sem.at[item, slot],
            device_id=target(route),
            device_id_type=MESH,
        )

    def send(item, slot, route):
        if route == UP:
            pl.when(z < nz - 1)(lambda: copy(item, slot, route).start())
        elif route == DOWN:
            pl.when(z > 0)(lambda: copy(item, slot, route).start())
        else:
            copy(item, slot, route).start()

    def sent(item, slot, route):
        if route == UP:
            pl.when(z < nz - 1)(lambda: copy(item, slot, route).wait_send())
        elif route == DOWN:
            pl.when(z > 0)(lambda: copy(item, slot, route).wait_send())
        else:
            copy(item, slot, route).wait_send()

    def arrived(item, slot):
        copy(item, slot, CORE).wait_recv()

    def below(k, act):
        pl.when(z >= k)(lambda: act(z - k))

    def above(k, act):
        pl.when(z + k < nz)(lambda: act(z + k))

    def z_step(item, k, yy, then=()):
        def from_below(zz):
            slot = slot_of(zz, yy, c)
            arrived(item, slot)
            for route in (UP,) + then:
                send(item, slot, route)

        def from_above(zz):
            slot = slot_of(zz, yy, c)
            arrived(item, slot)
            for route in (DOWN,) + then:
                send(item, slot, route)

        below(k, from_below)
        above(k, from_above)

    def at_distance(k, act):
        if k == 0:
            act(z)
        else:
            below(k, act)
            above(k, act)

    def across(item, k):
        def act(zz):
            slot = slot_of(zz, 1 - y, c)
            arrived(item, slot)
            send(item, slot, CORE)

        at_distance(k, act)

    def finish(item):
        for zz in range(nz):
            for yy in range(2):
                arrived(item, slot_of(zz, yy, 1 - c))

    def drain(item, both):
        for yy in (y, 1 - y) if both else (y,):
            for route in (UP, DOWN):
                sent(item, slot_of(z, yy, c), route)
            for k in range(1, nz):
                below(k, lambda zz, yy=yy: sent(item, slot_of(zz, yy, c), UP))
                above(k, lambda zz, yy=yy: sent(item, slot_of(zz, yy, c), DOWN))
        if both:
            sent(item, me, ACROSS)
        for zz in range(nz):
            if not both:
                sent(item, slot_of(zz, y, c), ACROSS)
            for yy in range(2):
                sent(item, slot_of(zz, yy, c), CORE)

    own = [
        pltpu.make_async_copy(w_query_ref, whole_rows(wq), local_sem.at[0]),
        pltpu.make_async_copy(
            w_key_ref.at[:, pl.ds(kv_start, kv_cols)],
            rows_of(WKV, me).at[:, pl.ds(0, kv_cols)],
            local_sem.at[1],
        ),
        pltpu.make_async_copy(
            w_value_ref.at[:, pl.ds(kv_start, kv_cols)],
            rows_of(WKV, me).at[:, pl.ds(kv_cols, kv_cols)],
            local_sem.at[2],
        ),
        pltpu.make_async_copy(w_out_ref, whole_rows(wo), local_sem.at[3]),
    ]
    for one in own:
        one.start()

    barrier = pltpu.get_barrier_semaphore()

    def greet(blk, hd):
        pl.semaphore_signal(barrier, inc=1, device_id=(blk, hd), device_id_type=MESH)

    pl.when(z < nz - 1)(lambda: greet(me + 4, head))
    pl.when(z > 0)(lambda: greet(me - 4, head))
    greet(target(ACROSS)[0], head)
    greet(target(CORE)[0], head)
    peers = [lax.rem(head + d, heads) for d in range(1, heads)]
    for peer in peers:
        greet(me, peer)
    ends = jnp.where(z < nz - 1, 1, 0) + jnp.where(z > 0, 1, 0)
    pl.semaphore_wait(barrier, ends + 2 + len(peers))

    own[1].wait()
    own[2].wait()
    for route in (ACROSS, UP, DOWN, CORE):
        send(WKV, me, route)
    own[0].wait()
    own[3].wait()
    for item in queries + outs:
        for route in (ACROSS, CORE):
            send(item, me, route)

    my_rows = pl.ds(pl.multiple_of(head * local_rows, local_rows), local_rows)
    floats = tokens_ref[...].astype(jnp.float32)
    normed[my_rows, :] = (
        floats
        * lax.rsqrt(jnp.mean(floats * floats, axis=1, keepdims=True) + eps_norm)
        * gain_ref[...]
    ).astype(jnp.bfloat16)

    there = slot_of(z, 1 - y, c)
    arrived(WKV, there)
    for route in (UP, DOWN, CORE):
        send(WKV, there, route)

    def norm_copy(d):
        return pltpu.make_async_remote_copy(
            src_ref=normed.at[my_rows],
            dst_ref=normed.at[my_rows],
            send_sem=norm_send.at[d],
            recv_sem=norm_recv.at[d],
            device_id=(me, peers[d]),
            device_id_type=MESH,
        )

    for d in range(len(peers)):
        norm_copy(d).start()

    for k in range(1, nz):
        z_step(WKV, k, y, (CORE,))
        z_step(WKV, k, 1 - y, (CORE,))
        if k == max(1, nz - 2):
            for item in queries:
                for route in (UP, DOWN):
                    send(item, me, route)
    for d in range(len(peers)):
        norm_copy(d).wait_recv()
    finish(WKV)

    cosine, sine = cos_ref[...], sin_ref[...]

    def turn(values):
        return values * cosine + pltpu.roll(values, HD // 2, 1) * sine

    kv_rows = pl.ds(pl.multiple_of(me * group_rows, group_rows), group_rows)
    sums = jnp.dot(normed[...], wkv[...], preferred_element_type=jnp.float32)
    for g in range(kv_here):
        bias = k_bias_ref[:, pl.ds(pl.multiple_of(kv_start + g * HD, HD), HD)]
        kv[kv_rows, pl.ds(g * HD, HD)] = turn(sums[:, g * HD : (g + 1) * HD] + bias).astype(
            jnp.bfloat16
        )
        bias = v_bias_ref[:, pl.ds(pl.multiple_of(kv_start + g * HD, HD), HD)]
        at = kv_cols + g * HD
        kv[kv_rows, pl.ds(at, HD)] = (sums[:, at : at + HD] + bias).astype(jnp.bfloat16)

    for item in queries:
        across(item, 0)
    for route in (UP, DOWN, ACROSS, CORE):
        send(KV, me, route)

    for k in range(1, nz):
        for item in queries:
            z_step(item, k, y, (ACROSS, CORE))
        z_step(KV, k, y, (ACROSS, CORE))
        if k == max(1, nz - 2):
            for item in outs:
                for route in (UP, DOWN):
                    send(item, me, route)
    for k in range(1, nz):
        if k == nz - 1:
            for item in outs:
                z_step(item, 1, y, (ACROSS, CORE))
        for item in queries:
            across(item, k)
    for k in range(nz):
        across(KV, k)
    for item in queries + (KV,):
        finish(item)

    joined = 2 if heads_here % 2 == 0 else 1

    def project(n, carry):
        cols = pl.ds(pl.multiple_of(n * joined * HD, joined * HD), joined * HD)
        total = jnp.dot(normed[...], wq[:, cols], preferred_element_type=jnp.float32)
        total = total + q_bias_ref[:, cols]
        for j in range(joined):
            query[n * joined + j] = turn(total[:, j * HD : (j + 1) * HD]).astype(jnp.bfloat16)
        return carry

    lax.fori_loop(0, heads_here // joined, project, 0)

    if nz > 2:
        for item in outs:
            z_step(item, 2, y, (ACROSS, CORE))

    keys = kv.shape[0]
    span = block_width(keys, 512)
    stacked = per_kv * group_rows
    last_query = me * group_rows + group_rows - 1
    steps = last_query // span + 1

    for g in range(kv_here):
        q = query[g * per_kv : (g + 1) * per_kv].reshape(stacked, HD)

        def attend(j, state, q=q, g=g):
            top, total, acc = state
            at = pl.ds(pl.multiple_of(j * span, span), span)
            scores = (
                lax.dot_general(
                    q,
                    kv[at, pl.ds(g * HD, HD)],
                    (((1,), (1,)), ((), ())),
                    preferred_element_type=jnp.float32,
                )
                * scale
            )
            shape = (per_kv, group_rows, span)
            rows = lax.broadcasted_iota(jnp.int32, shape, 1).reshape(stacked, span)
            columns = lax.broadcasted_iota(jnp.int32, (stacked, span), 1)
            visible = columns + j * span <= rows + me * group_rows
            scores = jnp.where(visible, scores, masked_score)
            new_top = jnp.maximum(top, jnp.max(scores, axis=1, keepdims=True))
            weights = jnp.where(visible, jnp.exp(scores - new_top), 0.0)
            fade = jnp.exp(top - new_top)
            total = total * fade + jnp.sum(weights, axis=1, keepdims=True)
            acc = acc * fade + jnp.dot(
                weights.astype(jnp.bfloat16),
                kv[at, pl.ds(kv_cols + g * HD, HD)],
                preferred_element_type=jnp.float32,
            )
            return (new_top, total, acc)

        start = (
            jnp.full((stacked, 1), masked_score, jnp.float32),
            jnp.zeros((stacked, 1), jnp.float32),
            jnp.zeros((stacked, HD), jnp.float32),
        )
        top, total, acc = lax.fori_loop(0, steps, attend, start)
        result = (acc / total).astype(jnp.bfloat16)
        for r in range(per_kv):
            attended[:, pl.ds((g * per_kv + r) * HD, HD)] = result[
                r * group_rows : (r + 1) * group_rows
            ]
        for k in range(3, nz):
            if g == 0:
                z_step(WO, k, y, (ACROSS, CORE))
    for k in range(3, nz):
        z_step(WO_TAIL, k, y, (ACROSS, CORE))

    each = wo.shape[0] // blocks
    grouped = (4 * each) % HD == 0
    groups = nz if grouped else 1
    chunk = width // groups

    def sum_copy(d, i, start):
        rows = pl.ds(pl.multiple_of(peers[d] * local_rows, local_rows), local_rows)
        cols = pl.ds(pl.multiple_of(start, HD), chunk)
        return pltpu.make_async_remote_copy(
            src_ref=outgoing.at[rows, cols],
            dst_ref=incoming.at[d, :, cols],
            send_sem=sum_send.at[d, i],
            recv_sem=sum_recv.at[d, i],
            device_id=(me, peers[d]),
            device_id_type=MESH,
        )

    def produce(start, size):
        cols = pl.ds(pl.multiple_of(start, HD), size)
        result = lax.dot_general(
            attended[...],
            wo[cols, :],
            (((1,), (1,)), ((), ())),
            preferred_element_type=jnp.float32,
        )
        partial[:, cols] = result
        outgoing[:, cols] = result.astype(jnp.bfloat16)

    def place(i):
        way = 1 - 2 * (z // max(1, nz // 2)) if nz > 1 else 1
        return lax.rem(z + way * i + nz, nz)

    if grouped:

        def produce_group(i, carry):
            zz = place(i)
            slot = slot_of(zz, 1 - y, c)
            for item in outs:
                arrived(item, slot)
                send(item, slot, CORE)
            for item in outs:
                for yy in range(2):
                    arrived(item, slot_of(zz, yy, 1 - c))
            produce(zz * 4 * each, chunk)
            for d in range(len(peers)):
                sum_copy(d, i, zz * chunk).start()
            return carry

        lax.fori_loop(0, nz, produce_group, 0)
    else:
        for item in outs:
            for k in range(nz):
                across(item, k)
            finish(item)
        part = 256
        lax.fori_loop(0, width // part, lambda n, carry: (produce(n * part, part), carry)[1], 0)
        for d in range(len(peers)):
            sum_copy(d, 0, 0).start()

    for item in queries + outs + (WKV, KV):
        drain(item, item == WKV)
    for d in range(len(peers)):
        norm_copy(d).wait_send()

    def collect(i, carry):
        start = place(i) * chunk if grouped else 0
        cols = pl.ds(pl.multiple_of(start, HD), chunk)
        for d in range(len(peers)):
            sum_copy(d, i, start).wait_recv()
        result = partial[my_rows, cols]
        for d in range(len(peers)):
            result = result + incoming[d, :, cols].astype(jnp.float32)
        out_ref[:, cols] = result.astype(jnp.bfloat16)
        for d in range(len(peers)):
            sum_copy(d, i, start).wait_send()
        return carry

    lax.fori_loop(0, groups, collect, 0)


def on_device(tokens, norm_gain, w_query, w_key, w_value, q_bias, k_bias, v_bias, w_out):
    blocks, heads = lax.axis_size("blk"), lax.axis_size("head")
    local_rows, width = tokens.shape
    group_rows = local_rows * heads
    heads_here = w_query.shape[1] // HD
    kv_here = max(1, heads_here // G)
    positions = lax.axis_index("blk") * group_rows + jnp.arange(group_rows, dtype=jnp.int32)
    half = HD // 2
    freq = theta_base ** (-(jnp.arange(half, dtype=jnp.float32) * 2.0 / HD))
    angles = positions.astype(jnp.float32)[:, None] * freq[None, :]
    cosine, sine = jnp.cos(angles), jnp.sin(angles)
    cosine = jnp.concatenate([cosine, cosine], axis=1)
    sine = jnp.concatenate([-sine, sine], axis=1)
    inner = heads_here * HD
    vmem = pl.BlockSpec(memory_space=pltpu.VMEM)
    hbm = pl.BlockSpec(memory_space=pl.ANY)
    others = max(1, heads - 1)
    bf16, f32 = jnp.bfloat16, jnp.float32
    return pl.pallas_call(
        functools.partial(kernel, (blocks, heads)),
        out_shape=jax.ShapeDtypeStruct((local_rows, width), bf16),
        in_specs=[vmem, vmem, hbm, hbm, hbm, vmem, vmem, vmem, hbm, vmem, vmem],
        out_specs=vmem,
        scratch_shapes=[
            pltpu.VMEM((width, inner), bf16),
            pltpu.VMEM((width, 2 * kv_here * HD), bf16),
            pltpu.VMEM((width, inner), bf16),
            pltpu.VMEM((blocks * group_rows, 2 * kv_here * HD), bf16),
            pltpu.VMEM((group_rows, width), bf16),
            pltpu.VMEM((heads_here, group_rows, HD), bf16),
            pltpu.VMEM((group_rows, inner), bf16),
            pltpu.VMEM((group_rows, width), f32),
            pltpu.VMEM((group_rows, width), bf16),
            pltpu.VMEM((others, local_rows, width), bf16),
            pltpu.SemaphoreType.DMA((4,)),
            pltpu.SemaphoreType.DMA((6, blocks, 4)),
            pltpu.SemaphoreType.DMA((6, blocks)),
            pltpu.SemaphoreType.DMA((others,)),
            pltpu.SemaphoreType.DMA((others,)),
            pltpu.SemaphoreType.DMA((others, blocks // 4)),
            pltpu.SemaphoreType.DMA((others, blocks // 4)),
        ],
        compiler_params=pltpu.CompilerParams(
            collective_id=0, has_side_effects=True, vmem_limit_bytes=60 * 1024 * 1024
        ),
    )(
        tokens,
        norm_gain[None, :],
        w_query,
        w_key,
        w_value,
        q_bias[None, :],
        k_bias[None, :],
        v_bias[None, :],
        w_out.T,
        cosine,
        sine,
    )


def plane_kernel(
    nz,
    tokens_ref,
    gain_ref,
    w_query_ref,
    w_key_ref,
    w_value_ref,
    q_bias_ref,
    k_bias_ref,
    v_bias_ref,
    w_out_ref,
    base_cos_ref,
    base_sin_ref,
    out_ref,
    tokens,
    base_cos,
    base_sin,
    gain,
    q_flat,
    k_bias,
    v_bias,
    cosine,
    sine,
    stage,
    w,
    normed,
    xs,
    part_out,
    part_in,
    full,
    biases,
    kv,
    hidden,
    att,
    att_other,
    wo,
    acc,
    outs,
    result,
    small_sem,
    load_sem,
    wo_load_sem,
    w_send,
    w_home,
    w_relay,
    w_rest,
    x_send,
    x_recv,
    b_sem,
    p_send,
    p_recv,
    kv_send,
    kv_recv,
    a_send,
    a_recv,
    wo_send,
    wo_recv,
    o_sem,
):
    f32, bf16 = jnp.float32, jnp.bfloat16
    me = lax.axis_index("blk")
    x = lax.axis_index("head")
    z, y, c = me // 4, (me // 2) % 2, me % 2
    rows, width = tokens_ref.shape
    each = w_query_ref.shape[0]
    depth = width // nz
    per_core = G // 2
    chunks = per_core + 1
    columns = width // nz
    zh = z // 2
    inner = ((z + 1) // 2) % 2 == 1
    outer = jnp.logical_not(inner)
    pair = z + 1 - 2 * (z % 2)
    near, far = 2 - zh, 3 - 3 * zh
    final_waits = []
    order = (0, nz - 1) + tuple(range(1, nz - 1))
    halves = 2
    span = nz // halves * 2 * rows

    def spot(zz):
        return jnp.where(((zz + 1) // 2) % 2 == 1, zz + 1, zz // 3)

    def dev(zz, yy, cc, xx):
        return ((zz * 2 + yy) * 2 + cc, xx)

    core_peer = dev(z, y, 1 - c, x)
    x_peer = dev(z, y, c, 1 - x)
    y_peer = dev(z, 1 - y, c, x)
    diagonal = dev(z, 1 - y, c, 1 - x)

    def go(src, dst, ssem, rsem, to, when=None):
        one = pltpu.make_async_remote_copy(
            src_ref=src, dst_ref=dst, send_sem=ssem, recv_sem=rsem, device_id=to, device_id_type=MESH
        )
        if when is None:
            one.start()
        else:
            pl.when(when)(one.start)

    def got(like, rsem):
        pltpu.make_async_remote_copy(
            src_ref=like, dst_ref=like, send_sem=b_sem.at[0], recv_sem=rsem, device_id=x_peer, device_id_type=MESH
        ).wait_recv()

    def at_end(like, ssem, when=None):
        one = pltpu.make_async_remote_copy(
            src_ref=like, dst_ref=like, send_sem=ssem, recv_sem=b_sem.at[1], device_id=x_peer, device_id_type=MESH
        )
        if when is None:
            final_waits.append(one.wait_send)
        else:
            final_waits.append(lambda: pl.when(when)(one.wait_send))

    small = [
        pltpu.make_async_copy(tokens_ref, tokens, small_sem.at[0]),
        pltpu.make_async_copy(gain_ref, gain, small_sem.at[1]),
        pltpu.make_async_copy(q_bias_ref, q_flat, small_sem.at[2]),
        pltpu.make_async_copy(k_bias_ref, k_bias, small_sem.at[3]),
        pltpu.make_async_copy(v_bias_ref, v_bias, small_sem.at[4]),
        pltpu.make_async_copy(base_cos_ref, base_cos, small_sem.at[5]),
        pltpu.make_async_copy(base_sin_ref, base_sin, small_sem.at[6]),
    ]
    for one in small:
        one.start()

    barrier = pltpu.get_barrier_semaphore()
    friends = [core_peer, x_peer, y_peer, diagonal]
    for d in range(1, nz):
        for f in range(2):
            friends.append(dev((z + d) % nz, y, (c + f) % 2, x))
    for friend in friends:
        pl.semaphore_signal(barrier, inc=1, device_id=friend, device_id_type=MESH)

    mine = y * 2 + c

    def block(xx, j, s):
        return w.at[
            j,
            pl.ds(pl.multiple_of(s * each, 16), each),
            pl.ds(pl.multiple_of(xx * 2 * HD, HD), 2 * HD),
        ]

    def blocks_like(n):
        return w.at[0, pl.ds(0, n * each), pl.ds(0, 2 * HD)]

    def load(f, j):
        place = stage.at[j] if f else block(x, j, mine)
        cc = (c + f) % 2
        sem = load_sem.at[j]
        if j == 0:
            at = pl.ds(pl.multiple_of(2 * x * HD, HD), 2 * HD)
            pl.when(cc == 0)(pltpu.make_async_copy(w_key_ref.at[:, at], place, sem).start)
            pl.when(cc == 1)(pltpu.make_async_copy(w_value_ref.at[:, at], place, sem).start)
        else:
            for gl in range(2):
                at = pl.ds(pl.multiple_of((gl * G + cc * per_core + j - 1) * HD, HD), HD)
                pltpu.make_async_copy(
                    w_query_ref.at[:, at], place.at[:, pl.ds(gl * HD, HD)], sem
                ).start()

    def loaded(j):
        pltpu.make_async_copy(blocks_like(2), blocks_like(2), load_sem.at[j]).wait()

    for j in range(chunks):
        for f in range(2):
            load(f, j)

    wo_cols = 2 * 2 * HD
    half_rows = each // 2

    def wo_block(h, xx, s, half):
        first = pl.multiple_of(s * each + half * half_rows, 16)
        return wo.at[h, pl.ds(first, half_rows), pl.ds(pl.multiple_of(xx * wo_cols, HD), wo_cols)]

    def wo_like(n):
        return wo.at[0, pl.ds(0, n * half_rows), pl.ds(0, wo_cols)]

    for h in range(per_core):
        for gl in range(2):
            for cc in range(2):
                zz = 2 * x + gl
                pltpu.make_async_copy(
                    w_out_ref.at[:, pl.ds((gl * G + cc * per_core + h) * HD, HD)],
                    wo.at[
                        h,
                        pl.ds(pl.multiple_of((y * 2 + c) * each, 16), each),
                        pl.ds(pl.multiple_of((zz * 2 + cc) * HD, HD), HD),
                    ],
                    wo_load_sem.at[h],
                ).start()

    small[0].wait()
    small[1].wait()
    floats = tokens[...].astype(f32)
    values = (
        floats
        * lax.rsqrt(jnp.mean(floats * floats, axis=1, keepdims=True) + eps_norm)
        * gain[...].reshape(1, width)
    ).astype(bf16)
    for n in range(nz):
        normed[n] = values[:, n * depth : (n + 1) * depth]
    at_me = pl.ds(pl.multiple_of((spot(z) * 2 + c) * rows, rows), rows)
    xs[at_me, :] = normed[z]
    small[2].wait()
    flat = q_flat[...]
    for n in range(q_flat.shape[0] // HD):
        biases[x, n] = flat[n * HD : (n + 1) * HD].reshape(1, HD)
    small[3].wait()
    small[4].wait()
    small[5].wait()
    small[6].wait()

    pl.semaphore_wait(barrier, len(friends))

    def home_send(j, s, cc):
        here = block(x, j, s)
        for to, ssem, relayed in ((x_peer, w_send.at[0], cc == 1), (y_peer, w_send.at[1], cc == 0)):
            go(here, here, ssem, w_relay.at[j, 1 if to is x_peer else 0], to, relayed)
            go(here, here, ssem, w_rest.at[j], to, jnp.logical_not(relayed))

    def own_block(j):
        loaded(j)
        go(stage.at[j], block(x, j, mine), w_send.at[2], w_home.at[j], core_peer)
        home_send(j, mine, c)

    def home(j):
        got(blocks_like(1), w_home.at[j])
        home_send(j, y * 2 + 1 - c, 1 - c)

    def relay_weights(j, k):
        def from_y():
            got(blocks_like(1), w_relay.at[j, 0])
            here = block(x, j, (1 - y) * 2)
            go(here, here, w_send.at[0], w_rest.at[j], x_peer)

        def from_x():
            got(blocks_like(1), w_relay.at[j, 1])
            here = block(1 - x, j, y * 2 + 1)
            go(here, here, w_send.at[1], w_rest.at[j], y_peer)

        pl.when(c == k)(from_y)
        pl.when(c != k)(from_x)

    at_end(w.at[pl.ds(0, 3), :, pl.ds(0, 2 * HD)], w_send.at[0])
    at_end(w.at[pl.ds(0, 3), :, pl.ds(0, 2 * HD)], w_send.at[1])
    at_end(blocks_like(chunks), w_send.at[2])

    def token_block(zz, cc):
        return xs.at[pl.ds(pl.multiple_of((spot(zz) * 2 + cc) * rows, rows), rows)]

    def tokens_like(n):
        return xs.at[pl.ds(0, n * rows)]

    def send_tokens():
        for to in (far, near, pair):
            go(normed.at[to], token_block(z, c), x_send.at[0], x_recv.at[z], dev(to, y, c, x))
        go(normed.at[z], token_block(z, c), x_send.at[1], x_recv.at[nz], core_peer)

    def pass_tokens(zz):
        here = token_block(zz, c)
        got(here, x_recv.at[zz])
        go(here, here, x_send.at[1], x_recv.at[nz], core_peer)

    def wait_tokens():
        got(tokens_like(nz), x_recv.at[nz])

    at_end(tokens_like(nz - 1), x_send.at[0])
    at_end(tokens_like(nz), x_send.at[1])

    def send_biases():
        go(biases.at[x], biases.at[x], b_sem.at[0], b_sem.at[1], x_peer)

    def shard(s):
        return pl.ds(pl.multiple_of(s * HD, HD), HD)

    def half_at(n):
        return pl.ds(n * span, span)

    def part_go(j, n, k, to, there):
        go(
            part_out.at[j, k, half_at(n)],
            part_in.at[j, there, half_at(n)],
            p_send.at[0],
            p_recv.at[j, there, n],
            dev(to, y, c, x),
        )

    def part_got(j, n, k):
        got(part_in.at[j, k, half_at(n)], p_recv.at[j, k, n])

    def multiply(j):
        got(blocks_like(4), w_rest.at[j])
        full[j] = jnp.dot(xs[...], w[j], preferred_element_type=f32)

        def send():
            for n in range(halves):
                for k, s in enumerate((far, near, pair)):
                    part_out[j, k, half_at(n)] = full[j, half_at(n), shard(s)].astype(bf16)
                    part_go(j, n, k, pair, k)

        pl.when(outer)(send)

    def chain(j, n, steps):
        def act():
            for k, s, source, to, there in steps:
                part_got(j, n, source)
                part_out[j, k, half_at(n)] = (
                    full[j, half_at(n), shard(s)] + part_in[j, source, half_at(n)].astype(f32)
                ).astype(bf16)
                part_go(j, n, k, to, there)

        pl.when(inner)(act)

    def inward(j, n):
        chain(j, n, ((0, far, 0, near, 3), (1, near, 1, near, 4)))

    def outward(j, n):
        chain(j, n, ((2, pair, 3, pair, 2),))

    def summed(j, n):
        def more():
            part_got(j, n, 4)
            full[j, half_at(n), shard(z)] = (
                full[j, half_at(n), shard(z)] + part_in[j, 4, half_at(n)].astype(f32)
            )

        pl.when(inner)(more)
        part_got(j, n, 2)
        return full[j, half_at(n), shard(z)] + part_in[j, 2, half_at(n)].astype(f32)

    at_end(part_out, p_send.at[0])

    def turn(values, n):
        return values * cosine[half_at(n)] + pltpu.roll(values, HD // 2, 1) * sine[half_at(n)]

    here_src = y * 2 + x
    others = [(1 - y) * 2 + x, y * 2 + 1 - x, (1 - y) * 2 + 1 - x]

    def make_tables():
        signs = jnp.where(lax.broadcasted_iota(jnp.int32, (1, HD), 1) < HD // 2, -1.0, 1.0)
        starts = base_cos.shape[0] - rows
        cos_in, sin_in = base_cos[starts:], base_sin[starts:]
        for n in range(2 * nz):
            row = pl.ds((order[n // 2] * 4 + y * 2 + n % 2) * 2 + x, 1)
            cos_at, sin_at = base_cos[row], base_sin[row]
            cosine[n * rows : (n + 1) * rows] = cos_at * cos_in - sin_at * sin_in
            sine[n * rows : (n + 1) * rows] = (sin_at * cos_in + cos_at * sin_in) * signs
        at = lax.broadcasted_iota(jnp.int32, (2 * rows, 8 * rows), 1)
        within = at % (2 * rows)
        key_at = (
            (at // (4 * rows)) * 4 + (within // rows) * 2 + (at // (2 * rows)) % 2
        ) * rows + within % rows
        at = lax.broadcasted_iota(jnp.int32, (2 * rows, 8 * rows), 0)
        query_at = (y * 4 + (at // rows) * 2 + x) * rows + at % rows
        hidden[...] = jnp.where(key_at <= query_at, 0.0, masked_score)

    def kv_half(kind, s, n):
        return kv.at[kind, s, half_at(n)]

    def make_kv(n):
        at_group = pl.ds(pl.multiple_of(z * HD, HD), HD)
        total = summed(0, n)
        kv[c, here_src, half_at(n)] = jnp.where(
            c == 0, turn(total + k_bias[:, at_group], n), total + v_bias[:, at_group]
        ).astype(bf16)
        here = kv_half(c, here_src, n)
        go(here, here, kv_send.at[0], kv_recv.at[n], x_peer)
        go(here, here, kv_send.at[0], kv_recv.at[2 + n], y_peer)
        go(here, here, kv_send.at[0], kv_recv.at[4 + n], diagonal)
        go(here, here, kv_send.at[1], kv_recv.at[6], core_peer)

    def kv_pass(n):
        for k, s in ((0, others[1]), (2, others[0]), (4, others[2])):
            here = kv_half(c, s, n)
            got(here, kv_recv.at[k + n])
            go(here, here, kv_send.at[1], kv_recv.at[6], core_peer)

    def kv_peer():
        got(kv.at[0], kv_recv.at[6])
        got(biases.at[1 - x], b_sem.at[1])

    at_end(kv.at[0, pl.ds(0, 3)], kv_send.at[0])
    at_end(kv.at[0], kv_send.at[1])
    at_end(biases.at[0], b_sem.at[0])

    factor = math.log2(math.e) / math.sqrt(HD)

    att_rows = nz // halves * rows

    def att_piece(h, n, zz, cc):
        return att.at[
            h,
            pl.ds(n * att_rows, att_rows),
            pl.ds(pl.multiple_of((zz * 2 + cc) * HD, HD), HD),
        ]

    def att_like(count):
        return att.at[0, pl.ds(0, att_rows), pl.ds(0, count * HD)]

    def attend(h, n):
        total = summed(h + 1, n) + biases[zh, (z % 2) * G + c * per_core + h]
        query = turn(total, n).astype(bf16)
        cols_of_me = pl.ds(pl.multiple_of((z * 2 + c) * HD, HD), HD)
        for k in range(nz // halves):
            t = order[n * (nz // halves) + k]
            q = query[k * 2 * rows : (k + 1) * 2 * rows]
            tiles = [pl.ds(order.index(u) * 2 * rows, 2 * rows) for u in range(t + 1)]
            scores = []
            for tile in tiles:
                keys = kv[0, :, tile].reshape(8 * rows, HD)
                scores.append(
                    lax.dot_general(
                        q, keys, (((1,), (1,)), ((), ())), preferred_element_type=f32
                    )
                )
            scores[t] = scores[t] + hidden[...]
            top = jnp.max(functools.reduce(jnp.maximum, scores), axis=1, keepdims=True)
            mixed, sums = None, None
            for tile, one in zip(tiles, scores):
                weights = jnp.exp2((one - top) * factor)
                sums = weights if sums is None else sums + weights
                vals = kv[1, :, tile].reshape(8 * rows, HD)
                one = jnp.dot(weights.astype(bf16), vals, preferred_element_type=f32)
                mixed = one if mixed is None else mixed + one
            mixed = (mixed / jnp.sum(sums, axis=1, keepdims=True)).astype(bf16)
            low, high = mixed[:rows], mixed[rows:]
            at = pl.ds(n * att_rows + k * rows, rows)
            att[h, at, cols_of_me] = jnp.where(c == 0, low, high)
            att_other[h, at, :] = jnp.where(c == 0, high, low)
        here, there = att_piece(h, n, z, c), att_other.at[h, pl.ds(n * att_rows, att_rows)]
        rsem = a_recv.at[h, n, z]
        direct = (h, n) == (per_core - 1, halves - 1)

        def att_go(k, to, when=None):
            go(here, here, a_send.at[k], rsem, dev(to, y, c, x), when)
            go(there, here, a_send.at[k], rsem, dev(to, y, 1 - c, x), when)

        if direct:
            att_go(4, far)
            att_go(4, near)
        else:
            att_go(0, near, inner)
        att_go(1, pair)
        go(there, here, a_send.at[2], rsem, core_peer)

    def relay_attended(h, n, zz, to):
        def act():
            got(att_like(2), a_recv.at[h, n, zz])
            for cc in range(2):
                here = att_piece(h, n, zz, cc)
                go(here, here, a_send.at[3], a_recv.at[h, n, zz], dev(to, y, c, x))

        pl.when(inner)(act)

    def from_near(h, n):
        relay_attended(h, n, near, pair)

    def from_pair(h, n):
        relay_attended(h, n, pair, near)

    def from_far(h, n):
        relay_attended(h, n, far, pair)

    def gathered(h, n):
        def act():
            for zz in (pair, near, far):
                got(att_like(2), a_recv.at[h, n, zz])

        if (h, n) == (per_core - 1, halves - 1):
            act()
        else:
            pl.when(outer)(act)
        got(att_like(1), a_recv.at[h, n, z])

    steps = per_core * halves

    def att_sent(pieces):
        return att.at[pl.ds(0, 2), pl.ds(0, pieces * att_rows // (4 * nz)), :]

    at_end(att_sent(2 * (steps - 1)), a_send.at[0], inner)
    at_end(att_sent(4), a_send.at[4])
    at_end(att.at[:, :, pl.ds(0, 2 * HD)], a_send.at[1])
    at_end(att.at[:, :, pl.ds(0, HD)], a_send.at[2])
    at_end(att_sent(6 * (steps - 1)), a_send.at[3], inner)

    def wo_go(h, xx, s, half, n, rsem, to):
        here = wo_block(h, xx, s, half)
        go(here, here, wo_send.at[n], rsem, to)

    def wo_begin(h):
        like = wo.at[h, pl.ds(0, each), pl.ds(0, wo_cols)]
        pltpu.make_async_copy(like, like, wo_load_sem.at[h]).wait()
        for half in range(2):
            for n, to in enumerate((x_peer, y_peer, core_peer)):
                wo_go(h, x, y * 2 + c, half, n, wo_recv.at[h, n], to)

    def wo_relay(h):
        got(wo_like(2), wo_recv.at[h, 1])
        wo_go(h, x, (1 - y) * 2 + c, 0, 0, wo_recv.at[h, 3], x_peer)
        got(wo_like(2), wo_recv.at[h, 0])
        wo_go(h, 1 - x, y * 2 + c, 1, 1, wo_recv.at[h, 3], y_peer)
        for half in range(2):
            wo_go(h, x, (1 - y) * 2 + c, half, 2, wo_recv.at[h, 2], core_peer)
            wo_go(h, 1 - x, y * 2 + c, half, 2, wo_recv.at[h, 2], core_peer)

    def wo_finish(h):
        got(wo_like(2), wo_recv.at[h, 3])
        for half in range(2):
            wo_go(h, 1 - x, (1 - y) * 2 + c, half, 2, wo_recv.at[h, 2], core_peer)

    def wo_wait(h):
        got(wo_like(8), wo_recv.at[h, 2])

    at_end(wo.at[:, pl.ds(0, 3 * half_rows), pl.ds(0, wo_cols)], wo_send.at[0])
    at_end(wo.at[:, pl.ds(0, 3 * half_rows), pl.ds(0, wo_cols)], wo_send.at[1])
    at_end(wo.at[:, pl.ds(0, 8 * half_rows), pl.ds(0, wo_cols)], wo_send.at[2])

    def produce(h, n):
        gathered(h, n)
        at = slice(n * att_rows, (n + 1) * att_rows)
        for first in range(0, columns, 512):
            cols = slice(first, min(first + 512, columns))
            part = lax.dot_general(
                att[h, at], wo[h, cols, :], (((1,), (1,)), ((), ())), preferred_element_type=f32
            )
            if h:
                part = part + acc[at, cols]
            if h < per_core - 1:
                acc[at, cols] = part
            else:
                for k in range(nz // halves):
                    t = order[n * (nz // halves) + k]
                    outs[t, :, cols] = part[k * rows : (k + 1) * rows].astype(bf16)

    def result_cols(zz):
        return pl.ds(pl.multiple_of(zz * columns, HD), columns)

    def last(n):
        for k in range(nz // halves):
            t = order[n * (nz // halves) + k]
            go(
                outs.at[t],
                result.at[:, result_cols(z)],
                o_sem.at[0],
                o_sem.at[1],
                dev(t, y, c, x),
                z != t,
            )

    at_end(outs.at[pl.ds(0, nz - 1)], o_sem.at[0])

    send_tokens()
    own_block(0)
    send_biases()
    home(0)
    make_tables()
    relay_weights(0, 0)
    relay_weights(0, 1)
    own_block(1)
    home(1)
    pass_tokens(pair)
    pass_tokens(near)
    pass_tokens(far)
    wait_tokens()
    multiply(0)
    relay_weights(1, 0)
    relay_weights(1, 1)
    own_block(2)
    home(2)
    inward(0, 0)
    multiply(1)
    outward(0, 0)
    inward(0, 1)
    relay_weights(2, 0)
    relay_weights(2, 1)
    own_block(3)
    make_kv(0)
    outward(0, 1)
    make_kv(1)
    home(3)
    inward(1, 0)
    multiply(2)
    outward(1, 0)
    inward(1, 1)
    outward(1, 1)
    kv_pass(0)
    inward(2, 0)
    kv_pass(1)
    kv_peer()
    attend(0, 0)
    relay_weights(3, 0)
    relay_weights(3, 1)
    attend(0, 1)
    wo_begin(0)
    inward(2, 1)
    from_near(0, 0)
    outward(2, 0)
    from_near(0, 1)
    multiply(3)
    wo_begin(1)
    outward(2, 1)
    from_pair(0, 0)
    from_pair(0, 1)
    attend(1, 0)
    wo_relay(0)
    wo_begin(2)
    attend(1, 1)
    inward(3, 0)
    from_near(1, 0)
    from_far(0, 0)
    from_near(1, 1)
    outward(3, 0)
    inward(3, 1)
    from_far(0, 1)
    wo_relay(1)
    from_pair(1, 0)
    from_pair(1, 1)
    outward(3, 1)
    attend(2, 0)
    attend(2, 1)
    wo_finish(0)
    from_far(1, 0)
    wo_relay(2)
    from_near(2, 0)
    wo_finish(1)
    from_far(1, 1)
    from_pair(2, 0)
    wo_wait(0)
    produce(0, 0)
    produce(0, 1)
    wo_wait(1)
    produce(1, 0)
    produce(1, 1)
    wo_finish(2)
    wo_wait(2)
    from_far(2, 0)
    produce(2, 0)
    last(0)
    produce(2, 1)
    last(1)
    out_ref[:, result_cols(z)] = outs[z]
    for done in final_waits:
        done()
    got(outs.at[pl.ds(0, nz - 1)], o_sem.at[1])
    for d in range(1, nz):
        zz = (z + d) % nz
        out_ref[:, result_cols(zz)] = result[:, result_cols(zz)]


def in_planes(tokens, norm_gain, w_query, w_key, w_value, q_bias, k_bias, v_bias, w_out):
    blocks = lax.axis_size("blk")
    nz = blocks // 4
    rows, width = tokens.shape
    inner, each, per_core = w_query.shape[1], w_query.shape[0], G // 2
    chunks, held, columns = per_core + 1, 2 * nz * rows, width // nz
    positions = np.concatenate([np.arange(2 * blocks) * rows, np.arange(rows)])
    lanes = np.arange(HD) % (HD // 2)
    angles = positions[:, None] * theta_base ** (-2.0 * lanes / HD)[None, :]
    base_cos = jnp.asarray(np.cos(angles), jnp.float32)
    base_sin = jnp.asarray(np.sin(angles), jnp.float32)
    vmem = pl.BlockSpec(memory_space=pltpu.VMEM)
    hbm = pl.BlockSpec(memory_space=pltpu.HBM)
    bf16, f32 = jnp.bfloat16, jnp.float32
    dma = pltpu.SemaphoreType.DMA
    return pl.pallas_call(
        functools.partial(plane_kernel, nz),
        out_shape=jax.ShapeDtypeStruct((rows, width), bf16),
        in_specs=[hbm] * 11,
        out_specs=vmem,
        scratch_shapes=[
            pltpu.VMEM((rows, width), bf16),
            pltpu.VMEM(base_cos.shape, f32),
            pltpu.VMEM(base_sin.shape, f32),
            pltpu.VMEM((width,), f32),
            pltpu.VMEM((inner,), f32),
            pltpu.VMEM((1, w_key.shape[1]), f32),
            pltpu.VMEM((1, w_key.shape[1]), f32),
            pltpu.VMEM((held, HD), f32),
            pltpu.VMEM((held, HD), f32),
            pltpu.VMEM((chunks, each, 2 * HD), bf16),
            pltpu.VMEM((chunks, 4 * each, 4 * HD), bf16),
            pltpu.VMEM((nz, rows, width // nz), bf16),
            pltpu.VMEM((held, width // nz), bf16),
            pltpu.VMEM((chunks, 3, held, HD), bf16),
            pltpu.VMEM((chunks, 5, held, HD), bf16),
            pltpu.VMEM((chunks, held, 4 * HD), f32),
            pltpu.VMEM((2, inner // HD, 1, HD), f32),
            pltpu.VMEM((2, 4, held, HD), bf16),
            pltpu.VMEM((2 * rows, 8 * rows), f32),
            pltpu.VMEM((per_core, nz * rows, 2 * nz * HD), bf16),
            pltpu.VMEM((per_core, nz * rows, HD), bf16),
            pltpu.VMEM((per_core, columns, 2 * nz * HD), bf16),
            pltpu.VMEM((nz * rows, columns), f32),
            pltpu.VMEM((nz, rows, columns), bf16),
            pltpu.VMEM((rows, width), bf16),
            dma((7,)),
            dma((chunks,)),
            dma((per_core,)),
            dma((3,)),
            dma((chunks,)),
            dma((chunks, 2)),
            dma((chunks,)),
            dma((2,)),
            dma((nz + 1,)),
            dma((2,)),
            dma((1,)),
            dma((chunks, 5, 2)),
            dma((2,)),
            dma((7,)),
            dma((5,)),
            dma((per_core, 2, nz)),
            dma((3,)),
            dma((per_core, 4)),
            dma((2,)),
        ],
        compiler_params=pltpu.CompilerParams(
            collective_id=1, has_side_effects=True, vmem_limit_bytes=63 * 1024 * 1024
        ),
    )(
        tokens,
        norm_gain,
        w_query,
        w_key,
        w_value,
        q_bias,
        k_bias[None, :],
        v_bias[None, :],
        w_out.T,
        base_cos,
        base_sin,
    )


def by_mesh(tokens, norm_gain, w_query, w_key, *rest):
    blocks, heads = lax.axis_size("blk"), lax.axis_size("head")
    groups = w_key.shape[1] // HD
    fits = blocks == 16 and heads == 2 and groups == 4 and w_query.shape[1] == 2 * G * HD
    run = in_planes if fits else on_device
    return run(tokens, norm_gain, w_query, w_key, *rest)


def solution(mesh):
    placed = (
        P(("blk", "head"), None),
        P(),
        P("blk", "head"),
        P("blk", None),
        P("blk", None),
        P("head"),
        P(),
        P(),
        P("head", "blk"),
    )
    return jax.shard_map(
        by_mesh, mesh=mesh, in_specs=placed, out_specs=P(("blk", "head"), None), check_vma=False
    )
```

```python
import functools
import math

import jax
import jax.numpy as jnp
import numpy as np
from jax import lax
from jax.experimental import pallas as pl
from jax.experimental.pallas import tpu as pltpu
from jax.sharding import PartitionSpec as P

HD = 128
G = 6
MESH = pl.DeviceIdType.MESH

theta_base = 1000000.0
eps_norm = 1e-06
masked_score = -1e30

WQ, WKV, WO, KV, WQ_TAIL, WO_TAIL = range(6)
UP, DOWN, ACROSS, CORE = range(4)


def block_width(rows, limit):
    width = min(rows, limit)
    while rows % width:
        width -= 1
    return width


def kernel(
    sizes,
    tokens_ref,
    gain_ref,
    w_query_ref,
    w_key_ref,
    w_value_ref,
    q_bias_ref,
    k_bias_ref,
    v_bias_ref,
    w_out_ref,
    cos_ref,
    sin_ref,
    out_ref,
    wq,
    wkv,
    wo,
    kv,
    normed,
    query,
    attended,
    partial,
    outgoing,
    incoming,
    local_sem,
    send_sem,
    recv_sem,
    norm_send,
    norm_recv,
    sum_send,
    sum_recv,
):
    blocks, heads = sizes
    nz = blocks // 4
    me = lax.axis_index("blk")
    head = lax.axis_index("head")
    z, y, c = me // 4, (me // 2) % 2, me % 2
    local_rows, width = tokens_ref.shape
    group_rows = local_rows * heads
    heads_here = wq.shape[1] // HD
    kv_here = wkv.shape[1] // (2 * HD)
    per_kv = heads_here // kv_here
    kv_cols = kv_here * HD
    kv_start = pl.multiple_of((head * heads_here // G) * HD, HD)
    buffers = {WQ: wq, WKV: wkv, WO: wo, KV: kv, WQ_TAIL: wq, WO_TAIL: wo}
    queries, outs = (WQ, WQ_TAIL), (WO, WO_TAIL)
    scale = 1.0 / math.sqrt(HD)

    def slot_of(zz, yy, cc):
        return (zz * 2 + yy) * 2 + cc

    def rows_of(item, slot):
        each = buffers[item].shape[0] // blocks
        first, size = 0, each
        if item in queries + outs:
            cut = each // 2 // 16 * 16
            first, size = (0, cut) if item in (WQ, WO) else (cut, each - cut)
        return buffers[item].at[pl.ds(pl.multiple_of(slot * each + first, 16), size)]

    def whole_rows(ref):
        each = ref.shape[0] // blocks
        return ref.at[pl.ds(pl.multiple_of(me * each, each), each)]

    def target(route):
        step = {UP: 4, DOWN: -4, ACROSS: 2 - 4 * y, CORE: 1 - 2 * c}[route]
        return (me + step, head)

    def copy(item, slot, route):
        part = rows_of(item, slot)
        return pltpu.make_async_remote_copy(
            src_ref=part,
            dst_ref=part,
            send_sem=send_sem.at[item, slot, route],
            recv_sem=recv_sem.at[item, slot],
            device_id=target(route),
            device_id_type=MESH,
        )

    def send(item, slot, route):
        if route == UP:
            pl.when(z < nz - 1)(lambda: copy(item, slot, route).start())
        elif route == DOWN:
            pl.when(z > 0)(lambda: copy(item, slot, route).start())
        else:
            copy(item, slot, route).start()

    def sent(item, slot, route):
        if route == UP:
            pl.when(z < nz - 1)(lambda: copy(item, slot, route).wait_send())
        elif route == DOWN:
            pl.when(z > 0)(lambda: copy(item, slot, route).wait_send())
        else:
            copy(item, slot, route).wait_send()

    def arrived(item, slot):
        copy(item, slot, CORE).wait_recv()

    def below(k, act):
        pl.when(z >= k)(lambda: act(z - k))

    def above(k, act):
        pl.when(z + k < nz)(lambda: act(z + k))

    def z_step(item, k, yy, then=()):
        def from_below(zz):
            slot = slot_of(zz, yy, c)
            arrived(item, slot)
            for route in (UP,) + then:
                send(item, slot, route)

        def from_above(zz):
            slot = slot_of(zz, yy, c)
            arrived(item, slot)
            for route in (DOWN,) + then:
                send(item, slot, route)

        below(k, from_below)
        above(k, from_above)

    def at_distance(k, act):
        if k == 0:
            act(z)
        else:
            below(k, act)
            above(k, act)

    def across(item, k):
        def act(zz):
            slot = slot_of(zz, 1 - y, c)
            arrived(item, slot)
            send(item, slot, CORE)

        at_distance(k, act)

    def finish(item):
        for zz in range(nz):
            for yy in range(2):
                arrived(item, slot_of(zz, yy, 1 - c))

    def drain(item, both):
        for yy in (y, 1 - y) if both else (y,):
            for route in (UP, DOWN):
                sent(item, slot_of(z, yy, c), route)
            for k in range(1, nz):
                below(k, lambda zz, yy=yy: sent(item, slot_of(zz, yy, c), UP))
                above(k, lambda zz, yy=yy: sent(item, slot_of(zz, yy, c), DOWN))
        if both:
            sent(item, me, ACROSS)
        for zz in range(nz):
            if not both:
                sent(item, slot_of(zz, y, c), ACROSS)
            for yy in range(2):
                sent(item, slot_of(zz, yy, c), CORE)

    own = [
        pltpu.make_async_copy(w_query_ref, whole_rows(wq), local_sem.at[0]),
        pltpu.make_async_copy(
            w_key_ref.at[:, pl.ds(kv_start, kv_cols)],
            rows_of(WKV, me).at[:, pl.ds(0, kv_cols)],
            local_sem.at[1],
        ),
        pltpu.make_async_copy(
            w_value_ref.at[:, pl.ds(kv_start, kv_cols)],
            rows_of(WKV, me).at[:, pl.ds(kv_cols, kv_cols)],
            local_sem.at[2],
        ),
        pltpu.make_async_copy(w_out_ref, whole_rows(wo), local_sem.at[3]),
    ]
    for one in own:
        one.start()

    barrier = pltpu.get_barrier_semaphore()

    def greet(blk, hd):
        pl.semaphore_signal(barrier, inc=1, device_id=(blk, hd), device_id_type=MESH)

    pl.when(z < nz - 1)(lambda: greet(me + 4, head))
    pl.when(z > 0)(lambda: greet(me - 4, head))
    greet(target(ACROSS)[0], head)
    greet(target(CORE)[0], head)
    peers = [lax.rem(head + d, heads) for d in range(1, heads)]
    for peer in peers:
        greet(me, peer)
    ends = jnp.where(z < nz - 1, 1, 0) + jnp.where(z > 0, 1, 0)
    pl.semaphore_wait(barrier, ends + 2 + len(peers))

    own[1].wait()
    own[2].wait()
    for route in (ACROSS, UP, DOWN, CORE):
        send(WKV, me, route)
    own[0].wait()
    own[3].wait()
    for item in queries + outs:
        for route in (ACROSS, CORE):
            send(item, me, route)

    my_rows = pl.ds(pl.multiple_of(head * local_rows, local_rows), local_rows)
    floats = tokens_ref[...].astype(jnp.float32)
    normed[my_rows, :] = (
        floats
        * lax.rsqrt(jnp.mean(floats * floats, axis=1, keepdims=True) + eps_norm)
        * gain_ref[...]
    ).astype(jnp.bfloat16)

    there = slot_of(z, 1 - y, c)
    arrived(WKV, there)
    for route in (UP, DOWN, CORE):
        send(WKV, there, route)

    def norm_copy(d):
        return pltpu.make_async_remote_copy(
            src_ref=normed.at[my_rows],
            dst_ref=normed.at[my_rows],
            send_sem=norm_send.at[d],
            recv_sem=norm_recv.at[d],
            device_id=(me, peers[d]),
            device_id_type=MESH,
        )

    for d in range(len(peers)):
        norm_copy(d).start()

    for k in range(1, nz):
        z_step(WKV, k, y, (CORE,))
        z_step(WKV, k, 1 - y, (CORE,))
        if k == max(1, nz - 2):
            for item in queries:
                for route in (UP, DOWN):
                    send(item, me, route)
    for d in range(len(peers)):
        norm_copy(d).wait_recv()
    finish(WKV)

    cosine, sine = cos_ref[...], sin_ref[...]

    def turn(values):
        return values * cosine + pltpu.roll(values, HD // 2, 1) * sine

    kv_rows = pl.ds(pl.multiple_of(me * group_rows, group_rows), group_rows)
    sums = jnp.dot(normed[...], wkv[...], preferred_element_type=jnp.float32)
    for g in range(kv_here):
        bias = k_bias_ref[:, pl.ds(pl.multiple_of(kv_start + g * HD, HD), HD)]
        kv[kv_rows, pl.ds(g * HD, HD)] = turn(sums[:, g * HD : (g + 1) * HD] + bias).astype(
            jnp.bfloat16
        )
        bias = v_bias_ref[:, pl.ds(pl.multiple_of(kv_start + g * HD, HD), HD)]
        at = kv_cols + g * HD
        kv[kv_rows, pl.ds(at, HD)] = (sums[:, at : at + HD] + bias).astype(jnp.bfloat16)

    for item in queries:
        across(item, 0)
    for route in (UP, DOWN, ACROSS, CORE):
        send(KV, me, route)

    for k in range(1, nz):
        for item in queries:
            z_step(item, k, y, (ACROSS, CORE))
        z_step(KV, k, y, (ACROSS, CORE))
        if k == max(1, nz - 2):
            for item in outs:
                for route in (UP, DOWN):
                    send(item, me, route)
    for k in range(1, nz):
        if k == nz - 1:
            for item in outs:
                z_step(item, 1, y, (ACROSS, CORE))
        for item in queries:
            across(item, k)
    for k in range(nz):
        across(KV, k)
    for item in queries + (KV,):
        finish(item)

    joined = 2 if heads_here % 2 == 0 else 1

    def project(n, carry):
        cols = pl.ds(pl.multiple_of(n * joined * HD, joined * HD), joined * HD)
        total = jnp.dot(normed[...], wq[:, cols], preferred_element_type=jnp.float32)
        total = total + q_bias_ref[:, cols]
        for j in range(joined):
            query[n * joined + j] = turn(total[:, j * HD : (j + 1) * HD]).astype(jnp.bfloat16)
        return carry

    lax.fori_loop(0, heads_here // joined, project, 0)

    if nz > 2:
        for item in outs:
            z_step(item, 2, y, (ACROSS, CORE))

    keys = kv.shape[0]
    span = block_width(keys, 512)
    stacked = per_kv * group_rows
    last_query = me * group_rows + group_rows - 1
    steps = last_query // span + 1

    for g in range(kv_here):
        q = query[g * per_kv : (g + 1) * per_kv].reshape(stacked, HD)

        def attend(j, state, q=q, g=g):
            top, total, acc = state
            at = pl.ds(pl.multiple_of(j * span, span), span)
            scores = (
                lax.dot_general(
                    q,
                    kv[at, pl.ds(g * HD, HD)],
                    (((1,), (1,)), ((), ())),
                    preferred_element_type=jnp.float32,
                )
                * scale
            )
            shape = (per_kv, group_rows, span)
            rows = lax.broadcasted_iota(jnp.int32, shape, 1).reshape(stacked, span)
            columns = lax.broadcasted_iota(jnp.int32, (stacked, span), 1)
            visible = columns + j * span <= rows + me * group_rows
            scores = jnp.where(visible, scores, masked_score)
            new_top = jnp.maximum(top, jnp.max(scores, axis=1, keepdims=True))
            weights = jnp.where(visible, jnp.exp(scores - new_top), 0.0)
            fade = jnp.exp(top - new_top)
            total = total * fade + jnp.sum(weights, axis=1, keepdims=True)
            acc = acc * fade + jnp.dot(
                weights.astype(jnp.bfloat16),
                kv[at, pl.ds(kv_cols + g * HD, HD)],
                preferred_element_type=jnp.float32,
            )
            return (new_top, total, acc)

        start = (
            jnp.full((stacked, 1), masked_score, jnp.float32),
            jnp.zeros((stacked, 1), jnp.float32),
            jnp.zeros((stacked, HD), jnp.float32),
        )
        top, total, acc = lax.fori_loop(0, steps, attend, start)
        result = (acc / total).astype(jnp.bfloat16)
        for r in range(per_kv):
            attended[:, pl.ds((g * per_kv + r) * HD, HD)] = result[
                r * group_rows : (r + 1) * group_rows
            ]
        for k in range(3, nz):
            if g == 0:
                z_step(WO, k, y, (ACROSS, CORE))
    for k in range(3, nz):
        z_step(WO_TAIL, k, y, (ACROSS, CORE))

    each = wo.shape[0] // blocks
    grouped = (4 * each) % HD == 0
    groups = nz if grouped else 1
    chunk = width // groups

    def sum_copy(d, i, start):
        rows = pl.ds(pl.multiple_of(peers[d] * local_rows, local_rows), local_rows)
        cols = pl.ds(pl.multiple_of(start, HD), chunk)
        return pltpu.make_async_remote_copy(
            src_ref=outgoing.at[rows, cols],
            dst_ref=incoming.at[d, :, cols],
            send_sem=sum_send.at[d, i],
            recv_sem=sum_recv.at[d, i],
            device_id=(me, peers[d]),
            device_id_type=MESH,
        )

    def produce(start, size):
        cols = pl.ds(pl.multiple_of(start, HD), size)
        result = lax.dot_general(
            attended[...],
            wo[cols, :],
            (((1,), (1,)), ((), ())),
            preferred_element_type=jnp.float32,
        )
        partial[:, cols] = result
        outgoing[:, cols] = result.astype(jnp.bfloat16)

    def place(i):
        way = 1 - 2 * (z // max(1, nz // 2)) if nz > 1 else 1
        return lax.rem(z + way * i + nz, nz)

    if grouped:

        def produce_group(i, carry):
            zz = place(i)
            slot = slot_of(zz, 1 - y, c)
            for item in outs:
                arrived(item, slot)
                send(item, slot, CORE)
            for item in outs:
                for yy in range(2):
                    arrived(item, slot_of(zz, yy, 1 - c))
            produce(zz * 4 * each, chunk)
            for d in range(len(peers)):
                sum_copy(d, i, zz * chunk).start()
            return carry

        lax.fori_loop(0, nz, produce_group, 0)
    else:
        for item in outs:
            for k in range(nz):
                across(item, k)
            finish(item)
        part = 256
        lax.fori_loop(0, width // part, lambda n, carry: (produce(n * part, part), carry)[1], 0)
        for d in range(len(peers)):
            sum_copy(d, 0, 0).start()

    for item in queries + outs + (WKV, KV):
        drain(item, item == WKV)
    for d in range(len(peers)):
        norm_copy(d).wait_send()

    def collect(i, carry):
        start = place(i) * chunk if grouped else 0
        cols = pl.ds(pl.multiple_of(start, HD), chunk)
        for d in range(len(peers)):
            sum_copy(d, i, start).wait_recv()
        result = partial[my_rows, cols]
        for d in range(len(peers)):
            result = result + incoming[d, :, cols].astype(jnp.float32)
        out_ref[:, cols] = result.astype(jnp.bfloat16)
        for d in range(len(peers)):
            sum_copy(d, i, start).wait_send()
        return carry

    lax.fori_loop(0, groups, collect, 0)


def on_device(tokens, norm_gain, w_query, w_key, w_value, q_bias, k_bias, v_bias, w_out):
    blocks, heads = lax.axis_size("blk"), lax.axis_size("head")
    local_rows, width = tokens.shape
    group_rows = local_rows * heads
    heads_here = w_query.shape[1] // HD
    kv_here = max(1, heads_here // G)
    positions = lax.axis_index("blk") * group_rows + jnp.arange(group_rows, dtype=jnp.int32)
    half = HD // 2
    freq = theta_base ** (-(jnp.arange(half, dtype=jnp.float32) * 2.0 / HD))
    angles = positions.astype(jnp.float32)[:, None] * freq[None, :]
    cosine, sine = jnp.cos(angles), jnp.sin(angles)
    cosine = jnp.concatenate([cosine, cosine], axis=1)
    sine = jnp.concatenate([-sine, sine], axis=1)
    inner = heads_here * HD
    vmem = pl.BlockSpec(memory_space=pltpu.VMEM)
    hbm = pl.BlockSpec(memory_space=pl.ANY)
    others = max(1, heads - 1)
    bf16, f32 = jnp.bfloat16, jnp.float32
    return pl.pallas_call(
        functools.partial(kernel, (blocks, heads)),
        out_shape=jax.ShapeDtypeStruct((local_rows, width), bf16),
        in_specs=[vmem, vmem, hbm, hbm, hbm, vmem, vmem, vmem, hbm, vmem, vmem],
        out_specs=vmem,
        scratch_shapes=[
            pltpu.VMEM((width, inner), bf16),
            pltpu.VMEM((width, 2 * kv_here * HD), bf16),
            pltpu.VMEM((width, inner), bf16),
            pltpu.VMEM((blocks * group_rows, 2 * kv_here * HD), bf16),
            pltpu.VMEM((group_rows, width), bf16),
            pltpu.VMEM((heads_here, group_rows, HD), bf16),
            pltpu.VMEM((group_rows, inner), bf16),
            pltpu.VMEM((group_rows, width), f32),
            pltpu.VMEM((group_rows, width), bf16),
            pltpu.VMEM((others, local_rows, width), bf16),
            pltpu.SemaphoreType.DMA((4,)),
            pltpu.SemaphoreType.DMA((6, blocks, 4)),
            pltpu.SemaphoreType.DMA((6, blocks)),
            pltpu.SemaphoreType.DMA((others,)),
            pltpu.SemaphoreType.DMA((others,)),
            pltpu.SemaphoreType.DMA((others, blocks // 4)),
            pltpu.SemaphoreType.DMA((others, blocks // 4)),
        ],
        compiler_params=pltpu.CompilerParams(
            collective_id=0, has_side_effects=True, vmem_limit_bytes=60 * 1024 * 1024
        ),
    )(
        tokens,
        norm_gain[None, :],
        w_query,
        w_key,
        w_value,
        q_bias[None, :],
        k_bias[None, :],
        v_bias[None, :],
        w_out.T,
        cosine,
        sine,
    )


def plane_kernel(
    nz,
    tokens_ref,
    gain_ref,
    w_query_ref,
    w_key_ref,
    w_value_ref,
    q_bias_ref,
    k_bias_ref,
    v_bias_ref,
    w_out_ref,
    base_cos_ref,
    base_sin_ref,
    out_ref,
    tokens,
    base_cos,
    base_sin,
    gain,
    q_flat,
    k_bias,
    v_bias,
    cosine,
    sine,
    stage,
    w,
    normed,
    xs,
    part_out,
    part_in,
    full,
    biases,
    kv,
    hidden,
    att,
    att_other,
    wo,
    acc,
    outs,
    result,
    small_sem,
    load_sem,
    wo_load_sem,
    w_send,
    w_home,
    w_relay,
    w_rest,
    x_send,
    x_recv,
    b_sem,
    p_send,
    p_recv,
    kv_send,
    kv_recv,
    a_send,
    a_recv,
    wo_send,
    wo_recv,
    o_sem,
):
    f32, bf16 = jnp.float32, jnp.bfloat16
    me = lax.axis_index("blk")
    x = lax.axis_index("head")
    z, y, c = me // 4, (me // 2) % 2, me % 2
    rows, width = tokens_ref.shape
    each = w_query_ref.shape[0]
    depth = width // nz
    per_core = G // 2
    chunks = per_core + 1
    columns = width // nz
    zh = z // 2
    inner = ((z + 1) // 2) % 2 == 1
    outer = jnp.logical_not(inner)
    pair = z + 1 - 2 * (z % 2)
    near, far = 2 - zh, 3 - 3 * zh
    final_waits = []
    order = (0, nz - 1) + tuple(range(1, nz - 1))
    halves = 2
    span = nz // halves * 2 * rows

    def spot(zz):
        return jnp.where(((zz + 1) // 2) % 2 == 1, zz + 1, zz // 3)

    def dev(zz, yy, cc, xx):
        return ((zz * 2 + yy) * 2 + cc, xx)

    core_peer = dev(z, y, 1 - c, x)
    x_peer = dev(z, y, c, 1 - x)
    y_peer = dev(z, 1 - y, c, x)
    diagonal = dev(z, 1 - y, c, 1 - x)

    def go(src, dst, ssem, rsem, to, when=None):
        one = pltpu.make_async_remote_copy(
            src_ref=src, dst_ref=dst, send_sem=ssem, recv_sem=rsem, device_id=to, device_id_type=MESH
        )
        if when is None:
            one.start()
        else:
            pl.when(when)(one.start)

    def got(like, rsem):
        pltpu.make_async_remote_copy(
            src_ref=like, dst_ref=like, send_sem=b_sem.at[0], recv_sem=rsem, device_id=x_peer, device_id_type=MESH
        ).wait_recv()

    def at_end(like, ssem, when=None):
        one = pltpu.make_async_remote_copy(
            src_ref=like, dst_ref=like, send_sem=ssem, recv_sem=b_sem.at[1], device_id=x_peer, device_id_type=MESH
        )
        if when is None:
            final_waits.append(one.wait_send)
        else:
            final_waits.append(lambda: pl.when(when)(one.wait_send))

    small = [
        pltpu.make_async_copy(tokens_ref, tokens, small_sem.at[0]),
        pltpu.make_async_copy(gain_ref, gain, small_sem.at[1]),
        pltpu.make_async_copy(q_bias_ref, q_flat, small_sem.at[2]),
        pltpu.make_async_copy(k_bias_ref, k_bias, small_sem.at[3]),
        pltpu.make_async_copy(v_bias_ref, v_bias, small_sem.at[4]),
        pltpu.make_async_copy(base_cos_ref, base_cos, small_sem.at[5]),
        pltpu.make_async_copy(base_sin_ref, base_sin, small_sem.at[6]),
    ]
    for one in small:
        one.start()

    barrier = pltpu.get_barrier_semaphore()
    friends = [core_peer, x_peer, y_peer, diagonal]
    for d in range(1, nz):
        for f in range(2):
            friends.append(dev((z + d) % nz, y, (c + f) % 2, x))
    for friend in friends:
        pl.semaphore_signal(barrier, inc=1, device_id=friend, device_id_type=MESH)

    mine = y * 2 + c

    def block(xx, j, s):
        return w.at[
            j,
            pl.ds(pl.multiple_of(s * each, 16), each),
            pl.ds(pl.multiple_of(xx * 2 * HD, HD), 2 * HD),
        ]

    def blocks_like(n):
        return w.at[0, pl.ds(0, n * each), pl.ds(0, 2 * HD)]

    def load(f, j):
        place = stage.at[j] if f else block(x, j, mine)
        cc = (c + f) % 2
        sem = load_sem.at[j]
        if j == 0:
            at = pl.ds(pl.multiple_of(2 * x * HD, HD), 2 * HD)
            pl.when(cc == 0)(pltpu.make_async_copy(w_key_ref.at[:, at], place, sem).start)
            pl.when(cc == 1)(pltpu.make_async_copy(w_value_ref.at[:, at], place, sem).start)
        else:
            for gl in range(2):
                at = pl.ds(pl.multiple_of((gl * G + cc * per_core + j - 1) * HD, HD), HD)
                pltpu.make_async_copy(
                    w_query_ref.at[:, at], place.at[:, pl.ds(gl * HD, HD)], sem
                ).start()

    def loaded(j):
        pltpu.make_async_copy(blocks_like(2), blocks_like(2), load_sem.at[j]).wait()

    for j in range(chunks):
        for f in range(2):
            load(f, j)

    wo_cols = 2 * 2 * HD
    half_rows = each // 2

    def wo_block(h, xx, s, half):
        first = pl.multiple_of(s * each + half * half_rows, 16)
        return wo.at[h, pl.ds(first, half_rows), pl.ds(pl.multiple_of(xx * wo_cols, HD), wo_cols)]

    def wo_like(n):
        return wo.at[0, pl.ds(0, n * half_rows), pl.ds(0, wo_cols)]

    for h in range(per_core):
        for gl in range(2):
            for cc in range(2):
                zz = 2 * x + gl
                pltpu.make_async_copy(
                    w_out_ref.at[:, pl.ds((gl * G + cc * per_core + h) * HD, HD)],
                    wo.at[
                        h,
                        pl.ds(pl.multiple_of((y * 2 + c) * each, 16), each),
                        pl.ds(pl.multiple_of((zz * 2 + cc) * HD, HD), HD),
                    ],
                    wo_load_sem.at[h],
                ).start()

    small[0].wait()
    small[1].wait()
    floats = tokens[...].astype(f32)
    values = (
        floats
        * lax.rsqrt(jnp.mean(floats * floats, axis=1, keepdims=True) + eps_norm)
        * gain[...].reshape(1, width)
    ).astype(bf16)
    for n in range(nz):
        normed[n] = values[:, n * depth : (n + 1) * depth]
    at_me = pl.ds(pl.multiple_of((spot(z) * 2 + c) * rows, rows), rows)
    xs[at_me, :] = normed[z]
    small[2].wait()
    flat = q_flat[...]
    for n in range(q_flat.shape[0] // HD):
        biases[x, n] = flat[n * HD : (n + 1) * HD].reshape(1, HD)
    small[3].wait()
    small[4].wait()
    small[5].wait()
    small[6].wait()

    pl.semaphore_wait(barrier, len(friends))

    def home_send(j, s, cc):
        here = block(x, j, s)
        for to, ssem, relayed in ((x_peer, w_send.at[0], cc == 1), (y_peer, w_send.at[1], cc == 0)):
            go(here, here, ssem, w_relay.at[j, 1 if to is x_peer else 0], to, relayed)
            go(here, here, ssem, w_rest.at[j], to, jnp.logical_not(relayed))

    def own_block(j):
        loaded(j)
        go(stage.at[j], block(x, j, mine), w_send.at[2], w_home.at[j], core_peer)
        home_send(j, mine, c)

    def home(j):
        got(blocks_like(1), w_home.at[j])
        home_send(j, y * 2 + 1 - c, 1 - c)

    def relay_weights(j, k):
        def from_y():
            got(blocks_like(1), w_relay.at[j, 0])
            here = block(x, j, (1 - y) * 2)
            go(here, here, w_send.at[0], w_rest.at[j], x_peer)

        def from_x():
            got(blocks_like(1), w_relay.at[j, 1])
            here = block(1 - x, j, y * 2 + 1)
            go(here, here, w_send.at[1], w_rest.at[j], y_peer)

        pl.when(c == k)(from_y)
        pl.when(c != k)(from_x)

    at_end(w.at[pl.ds(0, 3), :, pl.ds(0, 2 * HD)], w_send.at[0])
    at_end(w.at[pl.ds(0, 3), :, pl.ds(0, 2 * HD)], w_send.at[1])
    at_end(blocks_like(chunks), w_send.at[2])

    def token_block(zz, cc):
        return xs.at[pl.ds(pl.multiple_of((spot(zz) * 2 + cc) * rows, rows), rows)]

    def tokens_like(n):
        return xs.at[pl.ds(0, n * rows)]

    def send_tokens():
        for to in (far, near, pair):
            go(normed.at[to], token_block(z, c), x_send.at[0], x_recv.at[z], dev(to, y, c, x))
        go(normed.at[z], token_block(z, c), x_send.at[1], x_recv.at[nz], core_peer)

    def pass_tokens(zz):
        here = token_block(zz, c)
        got(here, x_recv.at[zz])
        go(here, here, x_send.at[1], x_recv.at[nz], core_peer)

    def wait_tokens():
        got(tokens_like(nz), x_recv.at[nz])

    at_end(tokens_like(nz - 1), x_send.at[0])
    at_end(tokens_like(nz), x_send.at[1])

    def send_biases():
        go(biases.at[x], biases.at[x], b_sem.at[0], b_sem.at[1], x_peer)

    def shard(s):
        return pl.ds(pl.multiple_of(s * HD, HD), HD)

    def half_at(n):
        return pl.ds(n * span, span)

    def part_go(j, n, k, to, there):
        go(
            part_out.at[j, k, half_at(n)],
            part_in.at[j, there, half_at(n)],
            p_send.at[0],
            p_recv.at[j, there, n],
            dev(to, y, c, x),
        )

    def part_got(j, n, k):
        got(part_in.at[j, k, half_at(n)], p_recv.at[j, k, n])

    def multiply(j):
        got(blocks_like(4), w_rest.at[j])
        full[j] = jnp.dot(xs[...], w[j], preferred_element_type=f32)

        def send():
            for n in range(halves):
                for k, s in enumerate((far, near, pair)):
                    part_out[j, k, half_at(n)] = full[j, half_at(n), shard(s)].astype(bf16)
                    part_go(j, n, k, pair, k)

        pl.when(outer)(send)

    def chain(j, n, steps):
        def act():
            for k, s, source, to, there in steps:
                part_got(j, n, source)
                part_out[j, k, half_at(n)] = (
                    full[j, half_at(n), shard(s)] + part_in[j, source, half_at(n)].astype(f32)
                ).astype(bf16)
                part_go(j, n, k, to, there)

        pl.when(inner)(act)

    def inward(j, n):
        chain(j, n, ((0, far, 0, near, 3), (1, near, 1, near, 4)))

    def outward(j, n):
        chain(j, n, ((2, pair, 3, pair, 2),))

    def summed(j, n):
        def more():
            part_got(j, n, 4)
            full[j, half_at(n), shard(z)] = (
                full[j, half_at(n), shard(z)] + part_in[j, 4, half_at(n)].astype(f32)
            )

        pl.when(inner)(more)
        part_got(j, n, 2)
        return full[j, half_at(n), shard(z)] + part_in[j, 2, half_at(n)].astype(f32)

    at_end(part_out, p_send.at[0])

    def turn(values, n):
        return values * cosine[half_at(n)] + pltpu.roll(values, HD // 2, 1) * sine[half_at(n)]

    here_src = y * 2 + x
    others = [(1 - y) * 2 + x, y * 2 + 1 - x, (1 - y) * 2 + 1 - x]

    def make_tables():
        signs = jnp.where(lax.broadcasted_iota(jnp.int32, (1, HD), 1) < HD // 2, -1.0, 1.0)
        starts = base_cos.shape[0] - rows
        cos_in, sin_in = base_cos[starts:], base_sin[starts:]
        for n in range(2 * nz):
            row = pl.ds((order[n // 2] * 4 + y * 2 + n % 2) * 2 + x, 1)
            cos_at, sin_at = base_cos[row], base_sin[row]
            cosine[n * rows : (n + 1) * rows] = cos_at * cos_in - sin_at * sin_in
            sine[n * rows : (n + 1) * rows] = (sin_at * cos_in + cos_at * sin_in) * signs
        at = lax.broadcasted_iota(jnp.int32, (2 * rows, 8 * rows), 1)
        within = at % (2 * rows)
        key_at = (
            (at // (4 * rows)) * 4 + (within // rows) * 2 + (at // (2 * rows)) % 2
        ) * rows + within % rows
        at = lax.broadcasted_iota(jnp.int32, (2 * rows, 8 * rows), 0)
        query_at = (y * 4 + (at // rows) * 2 + x) * rows + at % rows
        hidden[...] = jnp.where(key_at <= query_at, 0.0, masked_score)

    def kv_half(kind, s, n):
        return kv.at[kind, s, half_at(n)]

    def make_kv(n):
        at_group = pl.ds(pl.multiple_of(z * HD, HD), HD)
        total = summed(0, n)
        kv[c, here_src, half_at(n)] = jnp.where(
            c == 0, turn(total + k_bias[:, at_group], n), total + v_bias[:, at_group]
        ).astype(bf16)
        here = kv_half(c, here_src, n)
        go(here, here, kv_send.at[0], kv_recv.at[n], x_peer)
        go(here, here, kv_send.at[0], kv_recv.at[2 + n], y_peer)
        go(here, here, kv_send.at[0], kv_recv.at[4 + n], diagonal)
        go(here, here, kv_send.at[1], kv_recv.at[6], core_peer)

    def kv_pass(n):
        for k, s in ((0, others[1]), (2, others[0]), (4, others[2])):
            here = kv_half(c, s, n)
            got(here, kv_recv.at[k + n])
            go(here, here, kv_send.at[1], kv_recv.at[6], core_peer)

    def kv_peer():
        got(kv.at[0], kv_recv.at[6])
        got(biases.at[1 - x], b_sem.at[1])

    at_end(kv.at[0, pl.ds(0, 3)], kv_send.at[0])
    at_end(kv.at[0], kv_send.at[1])
    at_end(biases.at[0], b_sem.at[0])

    factor = math.log2(math.e) / math.sqrt(HD)

    att_rows = nz // halves * rows

    def att_piece(h, n, zz, cc):
        return att.at[
            h,
            pl.ds(n * att_rows, att_rows),
            pl.ds(pl.multiple_of((zz * 2 + cc) * HD, HD), HD),
        ]

    def att_like(count):
        return att.at[0, pl.ds(0, att_rows), pl.ds(0, count * HD)]

    def attend(h, n):
        total = summed(h + 1, n) + biases[zh, (z % 2) * G + c * per_core + h]
        query = turn(total, n).astype(bf16)
        cols_of_me = pl.ds(pl.multiple_of((z * 2 + c) * HD, HD), HD)
        for k in range(nz // halves):
            t = order[n * (nz // halves) + k]
            q = query[k * 2 * rows : (k + 1) * 2 * rows]
            tiles = [pl.ds(order.index(u) * 2 * rows, 2 * rows) for u in range(t + 1)]
            scores = []
            for tile in tiles:
                keys = kv[0, :, tile].reshape(8 * rows, HD)
                scores.append(
                    lax.dot_general(
                        q, keys, (((1,), (1,)), ((), ())), preferred_element_type=f32
                    )
                )
            scores[t] = scores[t] + hidden[...]
            top = jnp.max(functools.reduce(jnp.maximum, scores), axis=1, keepdims=True)
            mixed, sums = None, None
            for tile, one in zip(tiles, scores):
                weights = jnp.exp2((one - top) * factor)
                sums = weights if sums is None else sums + weights
                vals = kv[1, :, tile].reshape(8 * rows, HD)
                one = jnp.dot(weights.astype(bf16), vals, preferred_element_type=f32)
                mixed = one if mixed is None else mixed + one
            mixed = (mixed / jnp.sum(sums, axis=1, keepdims=True)).astype(bf16)
            low, high = mixed[:rows], mixed[rows:]
            at = pl.ds(n * att_rows + k * rows, rows)
            att[h, at, cols_of_me] = jnp.where(c == 0, low, high)
            att_other[h, at, :] = jnp.where(c == 0, high, low)
        here, there = att_piece(h, n, z, c), att_other.at[h, pl.ds(n * att_rows, att_rows)]
        rsem = a_recv.at[h, n, z]
        direct = (h, n) == (per_core - 1, halves - 1)

        def att_go(k, to, when=None):
            go(here, here, a_send.at[k], rsem, dev(to, y, c, x), when)
            go(there, here, a_send.at[k], rsem, dev(to, y, 1 - c, x), when)

        if direct:
            att_go(4, far)
            att_go(4, near)
        else:
            att_go(0, near, inner)
        att_go(1, pair)
        go(there, here, a_send.at[2], rsem, core_peer)

    def relay_attended(h, n, zz, to):
        def act():
            got(att_like(2), a_recv.at[h, n, zz])
            for cc in range(2):
                here = att_piece(h, n, zz, cc)
                go(here, here, a_send.at[3], a_recv.at[h, n, zz], dev(to, y, c, x))

        pl.when(inner)(act)

    def from_near(h, n):
        relay_attended(h, n, near, pair)

    def from_pair(h, n):
        relay_attended(h, n, pair, near)

    def from_far(h, n):
        relay_attended(h, n, far, pair)

    def gathered(h, n):
        def act():
            for zz in (pair, near, far):
                got(att_like(2), a_recv.at[h, n, zz])

        if (h, n) == (per_core - 1, halves - 1):
            act()
        else:
            pl.when(outer)(act)
        got(att_like(1), a_recv.at[h, n, z])

    steps = per_core * halves

    def att_sent(pieces):
        return att.at[pl.ds(0, 2), pl.ds(0, pieces * att_rows // (4 * nz)), :]

    at_end(att_sent(2 * (steps - 1)), a_send.at[0], inner)
    at_end(att_sent(4), a_send.at[4])
    at_end(att.at[:, :, pl.ds(0, 2 * HD)], a_send.at[1])
    at_end(att.at[:, :, pl.ds(0, HD)], a_send.at[2])
    at_end(att_sent(6 * (steps - 1)), a_send.at[3], inner)

    def wo_go(h, xx, s, half, n, rsem, to):
        here = wo_block(h, xx, s, half)
        go(here, here, wo_send.at[n], rsem, to)

    def wo_begin(h):
        like = wo.at[h, pl.ds(0, each), pl.ds(0, wo_cols)]
        pltpu.make_async_copy(like, like, wo_load_sem.at[h]).wait()
        for half in range(2):
            for n, to in enumerate((x_peer, y_peer, core_peer)):
                wo_go(h, x, y * 2 + c, half, n, wo_recv.at[h, n], to)

    def wo_relay(h):
        got(wo_like(2), wo_recv.at[h, 1])
        wo_go(h, x, (1 - y) * 2 + c, 0, 0, wo_recv.at[h, 3], x_peer)
        got(wo_like(2), wo_recv.at[h, 0])
        wo_go(h, 1 - x, y * 2 + c, 1, 1, wo_recv.at[h, 3], y_peer)
        for half in range(2):
            wo_go(h, x, (1 - y) * 2 + c, half, 2, wo_recv.at[h, 2], core_peer)
            wo_go(h, 1 - x, y * 2 + c, half, 2, wo_recv.at[h, 2], core_peer)

    def wo_finish(h):
        got(wo_like(2), wo_recv.at[h, 3])
        for half in range(2):
            wo_go(h, 1 - x, (1 - y) * 2 + c, half, 2, wo_recv.at[h, 2], core_peer)

    def wo_wait(h):
        got(wo_like(8), wo_recv.at[h, 2])

    at_end(wo.at[:, pl.ds(0, 3 * half_rows), pl.ds(0, wo_cols)], wo_send.at[0])
    at_end(wo.at[:, pl.ds(0, 3 * half_rows), pl.ds(0, wo_cols)], wo_send.at[1])
    at_end(wo.at[:, pl.ds(0, 8 * half_rows), pl.ds(0, wo_cols)], wo_send.at[2])

    def produce(h, n):
        gathered(h, n)
        at = slice(n * att_rows, (n + 1) * att_rows)
        for first in range(0, columns, 512):
            cols = slice(first, min(first + 512, columns))
            part = lax.dot_general(
                att[h, at], wo[h, cols, :], (((1,), (1,)), ((), ())), preferred_element_type=f32
            )
            if h:
                part = part + acc[at, cols]
            if h < per_core - 1:
                acc[at, cols] = part
            else:
                for k in range(nz // halves):
                    t = order[n * (nz // halves) + k]
                    outs[t, :, cols] = part[k * rows : (k + 1) * rows].astype(bf16)

    def result_cols(zz):
        return pl.ds(pl.multiple_of(zz * columns, HD), columns)

    def last(n):
        for k in range(nz // halves):
            t = order[n * (nz // halves) + k]
            go(
                outs.at[t],
                result.at[:, result_cols(z)],
                o_sem.at[0],
                o_sem.at[1],
                dev(t, y, c, x),
                z != t,
            )

    at_end(outs.at[pl.ds(0, nz - 1)], o_sem.at[0])

    send_tokens()
    own_block(0)
    send_biases()
    home(0)
    make_tables()
    relay_weights(0, 0)
    relay_weights(0, 1)
    own_block(1)
    home(1)
    pass_tokens(pair)
    pass_tokens(near)
    pass_tokens(far)
    wait_tokens()
    multiply(0)
    relay_weights(1, 0)
    relay_weights(1, 1)
    own_block(2)
    home(2)
    inward(0, 0)
    multiply(1)
    outward(0, 0)
    inward(0, 1)
    relay_weights(2, 0)
    relay_weights(2, 1)
    own_block(3)
    make_kv(0)
    outward(0, 1)
    make_kv(1)
    home(3)
    inward(1, 0)
    multiply(2)
    outward(1, 0)
    inward(1, 1)
    outward(1, 1)
    kv_pass(0)
    inward(2, 0)
    relay_weights(3, 0)
    kv_pass(1)
    relay_weights(3, 1)
    kv_peer()
    attend(0, 0)
    attend(0, 1)
    wo_begin(0)
    inward(2, 1)
    from_near(0, 0)
    outward(2, 0)
    from_near(0, 1)
    multiply(3)
    wo_begin(1)
    outward(2, 1)
    from_pair(0, 0)
    from_pair(0, 1)
    attend(1, 0)
    wo_relay(0)
    wo_begin(2)
    attend(1, 1)
    inward(3, 0)
    from_near(1, 0)
    from_far(0, 0)
    from_near(1, 1)
    outward(3, 0)
    inward(3, 1)
    from_far(0, 1)
    wo_relay(1)
    from_pair(1, 0)
    from_pair(1, 1)
    outward(3, 1)
    attend(2, 0)
    attend(2, 1)
    wo_finish(0)
    from_far(1, 0)
    wo_relay(2)
    from_near(2, 0)
    wo_finish(1)
    from_far(1, 1)
    from_pair(2, 0)
    wo_wait(0)
    produce(0, 0)
    produce(0, 1)
    wo_wait(1)
    produce(1, 0)
    produce(1, 1)
    wo_finish(2)
    wo_wait(2)
    from_far(2, 0)
    produce(2, 0)
    last(0)
    produce(2, 1)
    last(1)
    out_ref[:, result_cols(z)] = outs[z]
    for done in final_waits:
        done()
    got(outs.at[pl.ds(0, nz - 1)], o_sem.at[1])
    for d in range(1, nz):
        zz = (z + d) % nz
        out_ref[:, result_cols(zz)] = result[:, result_cols(zz)]


def in_planes(tokens, norm_gain, w_query, w_key, w_value, q_bias, k_bias, v_bias, w_out):
    blocks = lax.axis_size("blk")
    nz = blocks // 4
    rows, width = tokens.shape
    inner, each, per_core = w_query.shape[1], w_query.shape[0], G // 2
    chunks, held, columns = per_core + 1, 2 * nz * rows, width // nz
    positions = np.concatenate([np.arange(2 * blocks) * rows, np.arange(rows)])
    lanes = np.arange(HD) % (HD // 2)
    angles = positions[:, None] * theta_base ** (-2.0 * lanes / HD)[None, :]
    base_cos = jnp.asarray(np.cos(angles), jnp.float32)
    base_sin = jnp.asarray(np.sin(angles), jnp.float32)
    vmem = pl.BlockSpec(memory_space=pltpu.VMEM)
    hbm = pl.BlockSpec(memory_space=pltpu.HBM)
    bf16, f32 = jnp.bfloat16, jnp.float32
    dma = pltpu.SemaphoreType.DMA
    return pl.pallas_call(
        functools.partial(plane_kernel, nz),
        out_shape=jax.ShapeDtypeStruct((rows, width), bf16),
        in_specs=[hbm] * 11,
        out_specs=vmem,
        scratch_shapes=[
            pltpu.VMEM((rows, width), bf16),
            pltpu.VMEM(base_cos.shape, f32),
            pltpu.VMEM(base_sin.shape, f32),
            pltpu.VMEM((width,), f32),
            pltpu.VMEM((inner,), f32),
            pltpu.VMEM((1, w_key.shape[1]), f32),
            pltpu.VMEM((1, w_key.shape[1]), f32),
            pltpu.VMEM((held, HD), f32),
            pltpu.VMEM((held, HD), f32),
            pltpu.VMEM((chunks, each, 2 * HD), bf16),
            pltpu.VMEM((chunks, 4 * each, 4 * HD), bf16),
            pltpu.VMEM((nz, rows, width // nz), bf16),
            pltpu.VMEM((held, width // nz), bf16),
            pltpu.VMEM((chunks, 3, held, HD), bf16),
            pltpu.VMEM((chunks, 5, held, HD), bf16),
            pltpu.VMEM((chunks, held, 4 * HD), f32),
            pltpu.VMEM((2, inner // HD, 1, HD), f32),
            pltpu.VMEM((2, 4, held, HD), bf16),
            pltpu.VMEM((2 * rows, 8 * rows), f32),
            pltpu.VMEM((per_core, nz * rows, 2 * nz * HD), bf16),
            pltpu.VMEM((per_core, nz * rows, HD), bf16),
            pltpu.VMEM((per_core, columns, 2 * nz * HD), bf16),
            pltpu.VMEM((nz * rows, columns), f32),
            pltpu.VMEM((nz, rows, columns), bf16),
            pltpu.VMEM((rows, width), bf16),
            dma((7,)),
            dma((chunks,)),
            dma((per_core,)),
            dma((3,)),
            dma((chunks,)),
            dma((chunks, 2)),
            dma((chunks,)),
            dma((2,)),
            dma((nz + 1,)),
            dma((2,)),
            dma((1,)),
            dma((chunks, 5, 2)),
            dma((2,)),
            dma((7,)),
            dma((5,)),
            dma((per_core, 2, nz)),
            dma((3,)),
            dma((per_core, 4)),
            dma((2,)),
        ],
        compiler_params=pltpu.CompilerParams(
            collective_id=1, has_side_effects=True, vmem_limit_bytes=63 * 1024 * 1024
        ),
    )(
        tokens,
        norm_gain,
        w_query,
        w_key,
        w_value,
        q_bias,
        k_bias[None, :],
        v_bias[None, :],
        w_out.T,
        base_cos,
        base_sin,
    )


def by_mesh(tokens, norm_gain, w_query, w_key, *rest):
    blocks, heads = lax.axis_size("blk"), lax.axis_size("head")
    groups = w_key.shape[1] // HD
    fits = blocks == 16 and heads == 2 and groups == 4 and w_query.shape[1] == 2 * G * HD
    run = in_planes if fits else on_device
    return run(tokens, norm_gain, w_query, w_key, *rest)


def solution(mesh):
    placed = (
        P(("blk", "head"), None),
        P(),
        P("blk", "head"),
        P("blk", None),
        P("blk", None),
        P("head"),
        P(),
        P(),
        P("head", "blk"),
    )
    return jax.shard_map(
        by_mesh, mesh=mesh, in_specs=placed, out_specs=P(("blk", "head"), None), check_vma=False
    )
```
